128 devices in a mesh: patch: 32 (over y, z, core), level: 4 (over x).
Axes of the slice: x: 4, y: 4, z: 4, core: 2. Of those that a mesh axis runs over, the one named last changes fastest.
Arguments:
- forcing: bfloat16 [4, 256, 2, 128, 128], P('level', 'patch'), may hold values from -24 to 24
- velocity: bfloat16 [4, 256, 2, 128, 128], P('level', 'patch'), may hold values from -18 to 18
- viscosity: float32 [4, 256, 128, 128], P('level', 'patch'), may hold values from 0.3 to 3
- friction: bfloat16 [4, 256, 128, 128], P('level', 'patch'), may hold values from 0.049804688 to 1
- patch_rows: int32 [4, 32], replicated, may hold values from 0 to 8, as said below
Outputs:
- adjoint: float32 [4, 256, 2, 128, 128], P('level', 'patch')
- gradient: bfloat16 [4, 256, 128, 128], P('level', 'patch')
The draws below stay inside these ranges and needn't reach their ends.
Inputs may be any that keep to these rules, and one draw needn't show every extreme that they name: patch_rows[l, p] is the number of live rows of level l on patch index p: at most 8 // 2**l, patch_rows[0, p] >= 1 and patch_rows[l + 1, p] <= 2 * patch_rows[l, p]; in every draw some patch index holds the most rows on every level.
All inputs are finite; a program needn't handle non-finite values.
Results may differ from the reference program's by a relative error of at most 0.0005.
Values may be sent and summed in bfloat16 or wider, within the bound.
A program may use at most 128 MiB of HBM per device.

```python
import math
import jax
import jax.numpy as jnp

SIDE = 128
SLOTS = 8
SWEEPS = 1
LEVELS = 4
PATCHES = 32


def draw_patch_rows(key, part):
    first_key, chosen_key, tier_key = jax.random.split(key, 3)
    position = jnp.arange(PATCHES, dtype=jnp.int32)
    chosen = jax.random.randint(chosen_key, (), 0, PATCHES)
    current = jax.random.randint(first_key, (PATCHES,), SLOTS // 2, SLOTS + 1)
    current = jnp.where(position == chosen, SLOTS, current)
    stacked = [current]
    for tier_index in range(1, LEVELS):
        capacity = SLOTS // 2 ** tier_index
        upper_bound = jnp.minimum(2 * current, capacity)
        random_bits = jax.random.randint(jax.random.fold_in(tier_key, tier_index), (PATCHES,), 0, 1 << 20)
        current = random_bits * (upper_bound + 1) // (1 << 20)
        current = jnp.where(position == chosen, capacity, current)
        stacked.append(current)
    return jnp.stack(stacked).astype(jnp.int32)


def steps_of(own_key, extent, cuts, low, high):
    factor_of = 1.0
    for dim, parts in cuts:
        draws = jax.random.uniform(jax.random.fold_in(jax.random.fold_in(own_key, 6), dim), (parts,), jnp.float32, low / len(cuts), high / len(cuts))
        factor_of = factor_of * jnp.repeat(jnp.exp(draws), extent[dim] // parts).reshape((-1,) + (1,) * (len(extent) - 1 - dim))
    return factor_of


def bell_draw(rng, extent, spread, reach, cuts=(), held_as=jnp.bfloat16):
    drawn = spread * jax.random.normal(rng, extent, jnp.float32)
    if cuts:
        drawn = drawn * steps_of(rng, extent, cuts, -0.22, 0.18)
    return jnp.clip(drawn, -reach, reach).astype(held_as)


def setup_inputs(seed: int = 0) -> dict:
    key_of = jax.random.split(jax.random.key(seed), 6)
    return {
        "forcing": bell_draw(key_of[0], (LEVELS, PATCHES * SLOTS, 2, SIDE, SIDE), 4.0, 24.0, ((0, 4), (1, 32))),
        "velocity": bell_draw(key_of[1], (LEVELS, PATCHES * SLOTS, 2, SIDE, SIDE), 3.0, 18.0, ((0, 4), (1, 32))),
        "viscosity": jnp.clip(jnp.exp(math.log(3.0) - 2.3025851 * jax.random.uniform(key_of[2], (LEVELS, PATCHES * SLOTS, SIDE, SIDE), jnp.float32) ** steps_of(key_of[2], (LEVELS, PATCHES * SLOTS, SIDE, SIDE), ((0, 4), (1, 32)), -0.2, 0.2)), 0.3, 3.0),
        "friction": jnp.clip(jnp.exp(math.log(1.0) - 2.9996462 * jax.random.uniform(key_of[3], (LEVELS, PATCHES * SLOTS, SIDE, SIDE), jnp.float32) ** steps_of(key_of[3], (LEVELS, PATCHES * SLOTS, SIDE, SIDE), ((0, 4), (1, 32)), -0.2, 0.2)), 0.049804688, 1.0).astype(jnp.bfloat16),
        "patch_rows": draw_patch_rows(jax.random.fold_in(key_of[5], 71), 0),
    }


relaxation = 0.5


def cell_at(grid, row_step, col_step):
    row_total = grid.shape[-2]
    col_total = grid.shape[-1]
    return grid[..., 1 + row_step:row_total - 1 + row_step, 1 + col_step:col_total - 1 + col_step]


def viscosity_faces(visc_loop):
    centre = cell_at(visc_loop, 0, 0)
    east_cell = cell_at(visc_loop, 0, 1)
    west_cell = cell_at(visc_loop, 0, -1)
    north_cell = cell_at(visc_loop, 1, 0)
    south_cell = cell_at(visc_loop, -1, 0)
    return (east_cell, west_cell, north_cell, south_cell,
            0.5 * (centre + east_cell), 0.5 * (centre + west_cell),
            0.5 * (centre + north_cell), 0.5 * (centre + south_cell))


def diagonal_terms(face_values, friction_cells):
    east_cell, west_cell, north_cell, south_cell, face_east, face_west, face_north, face_south = face_values
    diag_u = 4.0 * (face_east + face_west) + face_north + face_south + friction_cells
    diag_v = 4.0 * (face_north + face_south) + face_east + face_west + friction_cells
    return jnp.stack([diag_u, diag_v], axis=1)


def operator_cells(loop_cells, face_values, friction_cells):
    east_cell, west_cell, north_cell, south_cell, face_east, face_west, face_north, face_south = face_values
    u_loop = loop_cells[:, 0]
    v_loop = loop_cells[:, 1]
    u_centre = cell_at(u_loop, 0, 0)
    u_east = cell_at(u_loop, 0, 1)
    u_west = cell_at(u_loop, 0, -1)
    u_north = cell_at(u_loop, 1, 0)
    u_south = cell_at(u_loop, -1, 0)
    u_northeast = cell_at(u_loop, 1, 1)
    u_northwest = cell_at(u_loop, 1, -1)
    u_southeast = cell_at(u_loop, -1, 1)
    u_southwest = cell_at(u_loop, -1, -1)
    v_centre = cell_at(v_loop, 0, 0)
    v_east = cell_at(v_loop, 0, 1)
    v_west = cell_at(v_loop, 0, -1)
    v_north = cell_at(v_loop, 1, 0)
    v_south = cell_at(v_loop, -1, 0)
    v_northeast = cell_at(v_loop, 1, 1)
    v_northwest = cell_at(v_loop, 1, -1)
    v_southeast = cell_at(v_loop, -1, 1)
    v_southwest = cell_at(v_loop, -1, -1)
    cross_u = (east_cell * (0.5 * (v_northeast - v_southeast)) - west_cell * (0.5 * (v_northwest - v_southwest))
               + 0.5 * (north_cell * (0.5 * (v_northeast - v_northwest)) - south_cell * (0.5 * (v_southeast - v_southwest))))
    cross_v = (north_cell * (0.5 * (u_northeast - u_northwest)) - south_cell * (0.5 * (u_southeast - u_southwest))
               + 0.5 * (east_cell * (0.5 * (u_northeast - u_southeast)) - west_cell * (0.5 * (u_northwest - u_southwest))))
    result_u = (-4.0 * (face_east * (u_east - u_centre) - face_west * (u_centre - u_west))
                - (face_north * (u_north - u_centre) - face_south * (u_centre - u_south))
                - cross_u + friction_cells * u_centre)
    result_v = (-4.0 * (face_north * (v_north - v_centre) - face_south * (v_centre - v_south))
                - (face_east * (v_east - v_centre) - face_west * (v_centre - v_west))
                - cross_v + friction_cells * v_centre)
    return jnp.stack([result_u, result_v], axis=1)


def assemble_loop(cells, edge_table, indices):
    south_index, north_index, west_index, east_index, northeast_index, southeast_index, northwest_index, southwest_index = indices
    side_cells = cells.shape[-1]
    south_row = edge_table[south_index]
    north_row = edge_table[north_index]
    west_col = edge_table[west_index]
    east_col = edge_table[east_index]
    corner_northeast = edge_table[northeast_index][:, :, 0]
    corner_southeast = edge_table[southeast_index][:, :, side_cells - 1]
    corner_northwest = edge_table[northwest_index][:, :, 0]
    corner_southwest = edge_table[southwest_index][:, :, side_cells - 1]
    middle = jnp.concatenate([west_col[..., None], cells, east_col[..., None]], axis=-1)
    bottom = jnp.concatenate([corner_southwest[..., None], south_row, corner_southeast[..., None]], axis=-1)
    top_row = jnp.concatenate([corner_northwest[..., None], north_row, corner_northeast[..., None]], axis=-1)
    return jnp.concatenate([bottom[:, :, None], middle, top_row[:, :, None]], axis=2)


def loop_global(cells, indices):
    comps = cells.shape[1]
    side_cells = cells.shape[-1]
    edge_table = jnp.concatenate([cells[:, :, 0, :], cells[:, :, side_cells - 1, :], cells[:, :, :, 0],
                                  cells[:, :, :, side_cells - 1], jnp.zeros((1, comps, side_cells), jnp.float32)], axis=0)
    return assemble_loop(cells, edge_table, indices)


def global_layout(level_rows, columns, slot_count):
    total = level_rows.shape[0] * slot_count
    global_ids = jnp.arange(total, dtype=jnp.int32)
    patch_of = global_ids // slot_count
    slot_of = global_ids % slot_count
    row_ids = slot_of // columns
    col_ids = slot_of % columns
    padded = jnp.concatenate([jnp.zeros((1,), jnp.int32), level_rows.astype(jnp.int32), jnp.zeros((1,), jnp.int32)])
    own_rows = padded[patch_of + 1]
    left_rows = padded[patch_of]
    right_rows = padded[patch_of + 2]
    alive = row_ids < own_rows
    blank = 4 * total
    inside_west = col_ids > 0
    inside_east = col_ids < columns - 1
    has_south = row_ids >= 1
    has_north = row_ids + 1 < own_rows
    left_base = (patch_of - 1) * slot_count
    right_base = (patch_of + 1) * slot_count

    def choose(condition, position):
        return jnp.where(condition & alive, position, blank)

    south_index = choose(has_south, total + global_ids - columns)
    north_index = choose(has_north, global_ids + columns)
    west_index = jnp.where(inside_west, choose(alive, 3 * total + global_ids - 1),
                           choose(row_ids < left_rows, 3 * total + left_base + row_ids * columns + columns - 1))
    east_index = jnp.where(inside_east, choose(alive, 2 * total + global_ids + 1),
                           choose(row_ids < right_rows, 2 * total + right_base + row_ids * columns))
    northeast_index = jnp.where(inside_east, choose(has_north, 2 * total + global_ids + columns + 1),
                                choose(row_ids + 1 < right_rows, 2 * total + right_base + (row_ids + 1) * columns))
    southeast_index = jnp.where(inside_east, choose(has_south, 2 * total + global_ids - columns + 1),
                                choose(has_south & (row_ids - 1 < right_rows), 2 * total + right_base + (row_ids - 1) * columns))
    northwest_index = jnp.where(inside_west, choose(has_north, 3 * total + global_ids + columns - 1),
                                choose(row_ids + 1 < left_rows, 3 * total + left_base + (row_ids + 1) * columns + columns - 1))
    southwest_index = jnp.where(inside_west, choose(has_south, 3 * total + global_ids - columns - 1),
                                choose(has_south & (row_ids - 1 < left_rows), 3 * total + left_base + (row_ids - 1) * columns + columns - 1))
    indices = (south_index, north_index, west_index, east_index, northeast_index, southeast_index, northwest_index, southwest_index)
    return indices, alive, patch_of, row_ids, col_ids


def join_quadrants(south_west, south_east, north_west, north_east):
    bottom = jnp.concatenate([south_west, south_east], axis=-1)
    top_half = jnp.concatenate([north_west, north_east], axis=-1)
    return jnp.concatenate([bottom, top_half], axis=-2)


def reference(forcing, velocity, viscosity, friction, patch_rows):
    slot_count = SLOTS
    total = PATCHES * SLOTS
    half_side = SIDE // 2
    layouts = []
    masks = []
    faces_all = []
    diagonals = []
    frictions = []
    forces = []
    for tier in range(LEVELS):
        layout = global_layout(patch_rows[tier], 2 ** tier, slot_count)
        layouts.append(layout)
        live_mask = layout[1].astype(jnp.float32)[:, None, None, None]
        masks.append(live_mask)
        visc_loop = loop_global(viscosity[tier][:, None], layout[0])[:, 0]
        face_values = viscosity_faces(visc_loop)
        friction_cells = friction[tier].astype(jnp.float32)
        faces_all.append(face_values)
        frictions.append(friction_cells)
        diagonals.append(diagonal_terms(face_values, friction_cells))
        forces.append(forcing[tier].astype(jnp.float32))

    def apply_level(tier, cells):
        return operator_cells(loop_global(cells, layouts[tier][0]), faces_all[tier], frictions[tier])

    def smooth(tier, right_side, start):
        current = start
        for sweep_index in range(SWEEPS):
            current = masks[tier] * (current + relaxation * (right_side - apply_level(tier, current)) / diagonals[tier])
        return current

    zero_cells = jnp.zeros((total, 2, SIDE, SIDE), jnp.float32)
    right_sides = [None] * LEVELS
    solutions = [None] * LEVELS
    right_sides[LEVELS - 1] = masks[LEVELS - 1] * forces[LEVELS - 1]
    for tier in range(LEVELS - 1, 0, -1):
        solutions[tier] = smooth(tier, right_sides[tier], zero_cells)
        residual = masks[tier] * (right_sides[tier] - apply_level(tier, solutions[tier]))
        quads = residual.reshape(total, 2, half_side, 2, half_side, 2).sum(axis=(3, 5))
        quad_table = jnp.concatenate([quads, jnp.zeros((1, 2, half_side, half_side), jnp.float32)], axis=0)
        coarse = tier - 1
        indices, alive, patch_of, row_ids, col_ids = layouts[coarse]
        coarse_columns = 2 ** coarse
        finer_rows = patch_rows[tier].astype(jnp.int32)[patch_of]
        placed = []
        covers = []
        for quad_row in range(2):
            for quad_col in range(2):
                fine_row = 2 * row_ids + quad_row
                valid = alive & (fine_row < finer_rows)
                child = jnp.where(valid, patch_of * slot_count + fine_row * (2 * coarse_columns) + 2 * col_ids + quad_col, total)
                placed.append(quad_table[child])
                covers.append(jnp.broadcast_to(valid.astype(jnp.float32)[:, None, None, None], (total, 1, half_side, half_side)))
        restricted = join_quadrants(placed[0], placed[1], placed[2], placed[3])
        covered = join_quadrants(covers[0], covers[1], covers[2], covers[3])
        right_sides[coarse] = masks[coarse] * ((1.0 - covered) * forces[coarse] + restricted)
    solutions[0] = smooth(0, right_sides[0], zero_cells)
    for tier in range(1, LEVELS):
        indices, alive, patch_of, row_ids, col_ids = layouts[tier]
        parent_ids = patch_of * slot_count + (row_ids // 2) * (2 ** (tier - 1)) + col_ids // 2
        parents = solutions[tier - 1][parent_ids]
        quad_row_of = (row_ids % 2)[:, None, None, None]
        quad_col_of = (col_ids % 2)[:, None, None, None]
        half_rows = jnp.where(quad_row_of == 0, parents[:, :, :half_side, :], parents[:, :, half_side:, :])
        quarter = jnp.where(quad_col_of == 0, half_rows[..., :half_side], half_rows[..., half_side:])
        correction = jnp.repeat(jnp.repeat(quarter, 2, axis=2), 2, axis=3)
        solutions[tier] = smooth(tier, right_sides[tier], solutions[tier] + masks[tier] * correction)
    gradients = []
    for tier in range(LEVELS):
        speed = velocity[tier].astype(jnp.float32)
        product = speed[:, 0] * solutions[tier][:, 0] + speed[:, 1] * solutions[tier][:, 1]
        gradients.append((-(frictions[tier] * product) * masks[tier][:, 0]).astype(jnp.bfloat16))
    return jnp.stack(solutions), jnp.stack(gradients)
```

```python
import functools

import jax
import jax.numpy as jnp
from jax import lax
from jax.experimental import pallas as pl
from jax.experimental.pallas import tpu as pltpu
from jax.sharding import PartitionSpec as P

MESH = pl.DeviceIdType.MESH
F32 = jnp.float32
BF16 = jnp.bfloat16
SIDE = 128
SLOTS = 8
PAD = 8
TALL = 3 * (SLOTS * SIDE + 2 * PAD)


def split_dot(x, matrix):
    high = x.astype(BF16)
    low = (x - high.astype(F32)).astype(BF16)
    return jnp.dot(high, matrix, preferred_element_type=F32) + jnp.dot(
        low, matrix, preferred_element_type=F32
    )


def kernel(
    levels,
    patches,
    rows_ref,
    forcing_hbm,
    velocity_hbm,
    viscosity_hbm,
    friction_hbm,
    out_ref,
    grad_ref,
    forcing,
    velocity,
    viscosity,
    friction,
    mu,
    fric,
    mu_e,
    mu_w,
    diag_u,
    diag_v,
    half_u,
    half_v,
    b_u,
    b_v,
    x_u,
    x_v,
    ue,
    uw,
    ve,
    vw,
    y_u,
    y_v,
    init_send,
    init_recv,
    down_send,
    down_recv,
    down_edge_send,
    down_edge_recv,
    up_send,
    up_recv,
    up_edge_send,
    up_edge_recv,
    load_sem,
    send_sem,
    recv_sem,
):
    level = lax.axis_index("level")
    patch = lax.axis_index("patch")
    cols = jnp.where(level == 0, 1, jnp.where(level == 1, 2, jnp.where(level == 2, 4, 8)))
    prows = jnp.where(level == 0, 8, jnp.where(level == 1, 4, jnp.where(level == 2, 2, 1)))
    height = prows * SIDE
    pitch = height + 2 * PAD
    has_west = patch > 0
    has_east = patch < patches - 1
    finer = jnp.minimum(level + 1, levels - 1)
    west = jnp.maximum(patch - 1, 0)
    east = jnp.minimum(patch + 1, patches - 1)
    own_rows = rows_ref[level, patch]
    west_rows = jnp.where(has_west, rows_ref[level, west], 0)
    east_rows = jnp.where(has_east, rows_ref[level, east], 0)
    fine_own = rows_ref[finer, patch]
    fine_west = jnp.where(has_west, rows_ref[finer, west], 0)
    fine_east = jnp.where(has_east, rows_ref[finer, east], 0)

    loads = [
        pltpu.make_async_copy(src, dst, load_sem.at[i])
        for i, (src, dst) in enumerate(
            (
                (viscosity_hbm, viscosity),
                (friction_hbm, friction),
                (forcing_hbm, forcing),
                (velocity_hbm, velocity),
            )
        )
    ]
    for load in loads:
        load.start()

    barrier = pltpu.get_barrier_semaphore()
    count = jnp.int32(0)
    for dl in (-1, 0, 1):
        for dp in (-1, 0, 1):
            if dl == 0 and dp == 0:
                continue
            there = (level + dl >= 0) & (level + dl < levels) & (patch + dp >= 0) & (patch + dp < patches)
            count = count + jnp.where(there, 1, 0)

            @pl.when(there)
            def _(dl=dl, dp=dp):
                pl.semaphore_signal(
                    barrier,
                    inc=1,
                    device_id={"level": level + dl, "patch": patch + dp},
                    device_id_type=MESH,
                )

    def base_of(col, row):
        return pl.multiple_of((col * pitch + PAD + row * SIDE).astype(jnp.int32), 8)

    def alive(row, total):
        return jnp.where(row < total, 1.0, 0.0).astype(F32)

    lane = lax.broadcasted_iota(jnp.int32, (SIDE, SIDE), 1)

    zeros = jnp.zeros((PAD, SIDE), F32)

    def clear(col, carry):
        first = pl.multiple_of(col * pitch, 8)
        last = pl.multiple_of(col * pitch + PAD + height, 8)
        for ref in (mu, x_u, x_v, ue, uw, ve, vw):
            ref[pl.ds(first, PAD), :] = zeros
            ref[pl.ds(last, PAD), :] = zeros
        return carry

    lax.fori_loop(0, cols + 2, clear, 0)

    for load in loads[:3]:
        load.wait()

    def unpack(slot_id, carry):
        col = slot_id // prows
        row = slot_id - col * prows
        base = base_of(col + 1, row)
        slot = row * cols + col
        live = alive(row, own_rows)
        mu[pl.ds(base, SIDE), :] = viscosity[slot] * live
        fric[pl.ds(base, SIDE), :] = friction[slot].astype(F32)
        b_u[pl.ds(base, SIDE), :] = forcing[slot, 0].astype(F32) * live
        b_v[pl.ds(base, SIDE), :] = forcing[slot, 1].astype(F32) * live
        return carry

    lax.fori_loop(0, SLOTS, unpack, 0)

    def pack(row, carry):
        for side in range(2):
            base = base_of(jnp.where(side == 0, 1, cols), row)
            near, far = (0, 1) if side == 0 else (SIDE - 1, SIDE - 2)
            mu_t = jnp.transpose(mu[pl.ds(base, SIDE), :])
            fr_t = jnp.transpose(fric[pl.ds(base, SIDE), :])
            bu_t = jnp.transpose(b_u[pl.ds(base, SIDE), :])
            bv_t = jnp.transpose(b_v[pl.ds(base, SIDE), :])
            parts = [
                mu_t[near : near + 1],
                mu_t[far : far + 1],
                fr_t[near : near + 1],
                bu_t[near : near + 1],
                bv_t[near : near + 1],
                jnp.zeros((3, SIDE), F32),
            ]
            init_send[side, row] = jnp.concatenate(parts, axis=0)
        return carry

    lax.fori_loop(0, prows, pack, 0)

    pl.semaphore_wait(barrier, count)

    def copy_to(src, dst, sem, dl, dp):
        return pltpu.make_async_remote_copy(
            src_ref=src,
            dst_ref=dst,
            send_sem=send_sem.at[sem],
            recv_sem=recv_sem.at[sem],
            device_id={"level": level + dl, "patch": patch + dp},
            device_id_type=MESH,
        )

    init_west = copy_to(init_send.at[0], init_recv.at[0], 0, 0, -1)
    init_east = copy_to(init_send.at[1], init_recv.at[1], 1, 0, 1)

    @pl.when(has_west)
    def _():
        init_west.start()

    @pl.when(has_east)
    def _():
        init_east.start()

    @pl.when(has_east)
    def _():
        init_west.wait_recv()

    @pl.when(jnp.logical_not(has_east))
    def _():
        init_recv[0] = jnp.ones((SLOTS, 8, SIDE), F32)

    @pl.when(has_west)
    def _():
        init_east.wait_recv()

    @pl.when(jnp.logical_not(has_west))
    def _():
        init_recv[1] = jnp.ones((SLOTS, 8, SIDE), F32)

    def spread(tile_t, index, first=0, count=SIDE):
        return jnp.broadcast_to(tile_t[first : first + count, index : index + 1], (count, SIDE))

    def unpack_halo(row, carry):
        for side in range(2):
            col = cols + 1 if side == 0 else 0
            base = base_of(jnp.int32(0) + col, row)
            near = 0 if side == 0 else SIDE - 1
            live = alive(row, east_rows if side == 0 else west_rows)
            tile_t = jnp.transpose(init_recv[side, row])
            mu[pl.ds(base, SIDE), :] = (
                jnp.where(lane == near, spread(tile_t, 0), spread(tile_t, 1)) * live
            )
            fric[pl.ds(base, SIDE), :] = spread(tile_t, 2)
            b_u[pl.ds(base, SIDE), :] = spread(tile_t, 3) * live
            b_v[pl.ds(base, SIDE), :] = spread(tile_t, 4) * live
        return carry

    lax.fori_loop(0, prows, unpack_halo, 0)

    def coefficients(index, carry):
        col = index // prows
        row = index - col * prows
        base = base_of(col, row)
        to_east = pl.multiple_of(base + jnp.where(col == cols + 1, 0, pitch), 8)
        to_west = pl.multiple_of(base - jnp.where(col == 0, 0, pitch), 8)
        total = jnp.where(col == 0, west_rows, jnp.where(col == cols + 1, east_rows, own_rows))
        live = 0.5 * alive(row, total)
        here = mu[pl.ds(base, SIDE), :]
        m_e = pltpu.roll(jnp.where(lane == 0, mu[pl.ds(to_east, SIDE), :], here), SIDE - 1, 1)
        m_w = pltpu.roll(jnp.where(lane == SIDE - 1, mu[pl.ds(to_west, SIDE), :], here), 1, 1)
        across = m_e + m_w + 2.0 * here
        along = mu[pl.ds(base + 1, SIDE), :] + mu[pl.ds(base - 1, SIDE), :] + 2.0 * here
        fr = fric[pl.ds(base, SIDE), :]
        d_u = 2.0 * across + 0.5 * along + fr
        d_v = 2.0 * along + 0.5 * across + fr
        mu_e[pl.ds(base, SIDE), :] = m_e
        mu_w[pl.ds(base, SIDE), :] = m_w
        diag_u[pl.ds(base, SIDE), :] = d_u
        diag_v[pl.ds(base, SIDE), :] = d_v
        half_u[pl.ds(base, SIDE), :] = live / d_u
        half_v[pl.ds(base, SIDE), :] = live / d_v
        return carry

    lax.fori_loop(0, (cols + 2) * prows, coefficients, 0)

    def shift_pass():
        def body(slot_id, carry):
            col = slot_id // prows
            row = slot_id - col * prows
            base = base_of(col + 1, row)
            to_east = pl.multiple_of(base + pitch, 8)
            to_west = pl.multiple_of(base - pitch, 8)
            for src, dst_e, dst_w in ((x_u, ue, uw), (x_v, ve, vw)):
                here = src[pl.ds(base, SIDE), :]
                dst_e[pl.ds(base, SIDE), :] = pltpu.roll(
                    jnp.where(lane == 0, src[pl.ds(to_east, SIDE), :], here), SIDE - 1, 1
                )
                dst_w[pl.ds(base, SIDE), :] = pltpu.roll(
                    jnp.where(lane == SIDE - 1, src[pl.ds(to_west, SIDE), :], here), 1, 1
                )
            return carry

        lax.fori_loop(0, SLOTS, body, 0)

    chunk = 64

    def residual_at(base):
        def at(ref, step=0):
            return ref[pl.ds(base + step, chunk), :]

        m, m_e, m_w, m_n, m_s = at(mu), at(mu_e), at(mu_w), at(mu, 1), at(mu, -1)
        p_e, p_w, p_n, p_s = m + m_e, m + m_w, m + m_n, m + m_s
        ue_n, ue_s, uw_n, uw_s = at(ue, 1), at(ue, -1), at(uw, 1), at(uw, -1)
        ve_n, ve_s, vw_n, vw_s = at(ve, 1), at(ve, -1), at(vw, 1), at(vw, -1)
        u, v = at(x_u), at(x_v)
        cross_u = 0.5 * (m_e * (ve_n - ve_s) - m_w * (vw_n - vw_s)) + 0.25 * (
            m_n * (ve_n - vw_n) - m_s * (ve_s - vw_s)
        )
        cross_v = 0.5 * (m_n * (ue_n - uw_n) - m_s * (ue_s - uw_s)) + 0.25 * (
            m_e * (ue_n - ue_s) - m_w * (uw_n - uw_s)
        )
        near_u = 2.0 * (p_e * at(ue) + p_w * at(uw)) + 0.5 * (p_n * at(x_u, 1) + p_s * at(x_u, -1))
        near_v = 2.0 * (p_n * at(x_v, 1) + p_s * at(x_v, -1)) + 0.5 * (p_e * at(ve) + p_w * at(vw))
        r_u = at(b_u) - (at(diag_u) * u - near_u - cross_u)
        r_v = at(b_v) - (at(diag_v) * v - near_v - cross_v)
        return u, v, r_u, r_v

    def chunk_base(index):
        slot_id = index // (SIDE // chunk)
        part = index - slot_id * (SIDE // chunk)
        col = slot_id // prows
        row = slot_id - col * prows
        return pl.multiple_of(base_of(col + 1, row) + part * chunk, 8), row

    fine_lane = lax.broadcasted_iota(jnp.int32, (SIDE, SIDE), 0)
    joins = [
        jnp.where(fine_lane // 2 + half * (SIDE // 2) == lane, 1.0, 0.0).astype(BF16)
        for half in range(2)
    ]
    spreads = [
        jnp.where(lane // 2 + half * (SIDE // 2) == fine_lane, 1.0, 0.0).astype(BF16)
        for half in range(2)
    ]
    quarter = SIDE // 2

    down_main = copy_to(down_send.at[:, pl.ds(0, 256), :], down_recv, 2, -1, 0)
    down_west = copy_to(down_edge_send.at[0], down_edge_recv.at[0], 3, -1, -1)
    down_east = copy_to(down_edge_send.at[1], down_edge_recv.at[1], 4, -1, 1)
    up_main = copy_to(up_send, up_recv, 5, 1, 0)
    up_west = copy_to(up_edge_send.at[0], up_edge_recv.at[0], 6, 1, -1)
    up_east = copy_to(up_edge_send.at[1], up_edge_recv.at[1], 7, 1, 1)
    half_rows = prows // 2

    @pl.when(level < levels - 1)
    def _():
        down_main.wait_recv()

        def place(block, carry):
            col = block // half_rows
            part = block - col * half_rows
            base = pl.multiple_of((col + 1) * pitch + PAD + part * quarter, 8)
            covered = part < fine_own
            got = pl.multiple_of(block * quarter, 8)
            for comp, ref in enumerate((b_u, b_v)):
                ref[pl.ds(base, quarter), :] = jnp.where(
                    covered,
                    down_recv[comp, pl.ds(got, quarter), :],
                    ref[pl.ds(base, quarter), :],
                )
            return carry

        lax.fori_loop(0, 4, place, 0)

    for side in range(2):
        there = has_east if side == 0 else has_west

        @pl.when((level >= 1) & (level < levels - 1) & there)
        def _(side=side):
            (down_west if side == 0 else down_east).wait_recv()
            col = cols + 1 if side == 0 else 0
            total = fine_east if side == 0 else fine_west
            tile_t = jnp.transpose(down_edge_recv[side])
            for part in range(2):
                base = pl.multiple_of(col * pitch + PAD + part * quarter, 8)
                covered = part < total
                for comp, ref in enumerate((b_u, b_v)):
                    ref[pl.ds(base, quarter), :] = jnp.where(
                        covered,
                        spread(tile_t, comp, part * quarter, quarter),
                        ref[pl.ds(base, quarter), :],
                    )

    def start_pass(index, carry):
        col = index // prows
        row = index - col * prows
        base = base_of(col, row)
        x_u[pl.ds(base, SIDE), :] = half_u[pl.ds(base, SIDE), :] * b_u[pl.ds(base, SIDE), :]
        x_v[pl.ds(base, SIDE), :] = half_v[pl.ds(base, SIDE), :] * b_v[pl.ds(base, SIDE), :]
        return carry

    lax.fori_loop(0, (cols + 2) * prows, start_pass, 0)

    @pl.when(level > 0)
    def _():
        shift_pass()

        def residual_pass(index, carry):
            base, row = chunk_base(index)
            live = alive(row, own_rows)
            u, v, r_u, r_v = residual_at(base)
            y_u[pl.ds(base, chunk), :] = r_u * live
            y_v[pl.ds(base, chunk), :] = r_v * live
            return carry

        lax.fori_loop(0, SLOTS * SIDE // chunk, residual_pass, 0)

        def restrict_pass(block, carry):
            pair = block // prows
            row = block - pair * prows
            for comp, ref in enumerate((y_u, y_v)):
                total = None
                for half in range(2):
                    base = base_of(2 * pair + half + 1, row)
                    rows = (
                        ref[pl.ds(base, quarter, stride=2), :]
                        + ref[pl.ds(base + 1, quarter, stride=2), :]
                    )
                    term = split_dot(rows, joins[half])
                    total = term if total is None else total + term
                down_send[comp, pl.ds(pl.multiple_of(block * quarter, 8), quarter), :] = total
            return carry

        lax.fori_loop(0, 4, restrict_pass, 0)
        down_main.start()

    @pl.when(level > 1)
    def _():
        last = pl.multiple_of((cols // 2 - 1) * prows * quarter, 8)
        for side in range(2):
            base = 0 if side == 0 else last
            near = 0 if side == 0 else SIDE - 1
            parts = []
            for comp in range(2):
                block_t = jnp.transpose(down_send[comp, pl.ds(base, SIDE), :])
                parts.append(block_t[near : near + 1])
            parts.append(jnp.zeros((6, SIDE), F32))
            down_edge_send[side] = jnp.concatenate(parts, axis=0)

        @pl.when(has_west)
        def _():
            down_west.start()

        @pl.when(has_east)
        def _():
            down_east.start()

    @pl.when(level > 0)
    def _():
        up_main.wait_recv()

        def prolong(block, carry):
            pair = block // prows
            row = block - pair * prows
            live = alive(row, own_rows)
            for comp, ref in enumerate((x_u, x_v)):
                coarse = up_recv[comp, pl.ds(pl.multiple_of(block * quarter, 8), quarter), :] * live
                for half in range(2):
                    base = base_of(2 * pair + half + 1, row)
                    wide = split_dot(coarse, spreads[half])
                    for step in range(2):
                        where = pl.ds(base + step, quarter, stride=2)
                        ref[where, :] = ref[where, :] + wide
            return carry

        lax.fori_loop(0, 4, prolong, 0)

        for side in range(2):
            there = has_east if side == 0 else has_west

            @pl.when(there)
            def _(side=side):
                (up_west if side == 0 else up_east).wait_recv()
                col = cols + 1 if side == 0 else 0
                total = east_rows if side == 0 else west_rows
                tile_t = jnp.transpose(up_edge_recv[side])
                for part in range(4):

                    @pl.when(part < prows)
                    def _():
                        base = base_of(jnp.int32(0) + col, part)
                        live = alive(part, total)
                        for comp, ref in enumerate((x_u, x_v)):
                            wide = spread(
                                tile_t, 2 * comp + part // 2, (part % 2) * quarter, quarter
                            )
                            for step in range(2):
                                where = pl.ds(base + step, quarter, stride=2)
                                ref[where, :] = ref[where, :] + wide * live

        shift_pass()

        def smooth_pass(index, carry):
            base, row = chunk_base(index)
            u, v, r_u, r_v = residual_at(base)
            y_u[pl.ds(base, chunk), :] = u + half_u[pl.ds(base, chunk), :] * r_u
            y_v[pl.ds(base, chunk), :] = v + half_v[pl.ds(base, chunk), :] * r_v
            return carry

        lax.fori_loop(0, SLOTS * SIDE // chunk, smooth_pass, 0)

    @pl.when(level == 0)
    def _():
        def keep(row, carry):
            base = base_of(1, row)
            y_u[pl.ds(base, SIDE), :] = x_u[pl.ds(base, SIDE), :]
            y_v[pl.ds(base, SIDE), :] = x_v[pl.ds(base, SIDE), :]
            return carry

        lax.fori_loop(0, SLOTS, keep, 0)

    @pl.when(level < levels - 1)
    def _():
        def collect(block, carry):
            col = block // half_rows
            part = block - col * half_rows
            base = pl.multiple_of((col + 1) * pitch + PAD + part * quarter, 8)
            for comp, ref in enumerate((y_u, y_v)):
                up_send[comp, pl.ds(pl.multiple_of(block * quarter, 8), quarter), :] = ref[
                    pl.ds(base, quarter), :
                ]
            return carry

        lax.fori_loop(0, 4, collect, 0)
        up_main.start()
        for side in range(2):
            col = 1 if side == 0 else cols
            near = 0 if side == 0 else SIDE - 1
            parts = []
            for ref in (y_u, y_v):
                for part in range(2):
                    base = base_of(jnp.int32(0) + col, part)
                    block_t = jnp.transpose(ref[pl.ds(base, SIDE), :])
                    parts.append(block_t[near : near + 1])
            parts.append(jnp.zeros((4, SIDE), F32))
            up_edge_send[side] = jnp.concatenate(parts, axis=0)

        @pl.when(has_west)
        def _():
            up_west.start()

        @pl.when(has_east)
        def _():
            up_east.start()

    loads[3].wait()

    def finish(slot_id, carry):
        col = slot_id // prows
        row = slot_id - col * prows
        base = base_of(col + 1, row)
        slot = row * cols + col
        live = alive(row, own_rows)
        u = y_u[pl.ds(base, SIDE), :]
        v = y_v[pl.ds(base, SIDE), :]
        out_ref[slot, 0] = u
        out_ref[slot, 1] = v
        product = velocity[slot, 0].astype(F32) * u + velocity[slot, 1].astype(F32) * v
        grad_ref[slot] = (-(friction[slot].astype(F32) * product) * live).astype(BF16)
        return carry

    lax.fori_loop(0, SLOTS, finish, 0)

    @pl.when(has_west)
    def _():
        init_west.wait_send()

    @pl.when(has_east)
    def _():
        init_east.wait_send()

    @pl.when(level > 0)
    def _():
        down_main.wait_send()

    @pl.when((level > 1) & has_west)
    def _():
        down_west.wait_send()

    @pl.when((level > 1) & has_east)
    def _():
        down_east.wait_send()

    @pl.when(level < levels - 1)
    def _():
        up_main.wait_send()

    @pl.when((level < levels - 1) & has_west)
    def _():
        up_west.wait_send()

    @pl.when((level < levels - 1) & has_east)
    def _():
        up_east.wait_send()


def per_device(levels, patches, forcing, velocity, viscosity, friction, patch_rows):
    tall = pltpu.VMEM((TALL, SIDE), F32)
    any_space = pl.BlockSpec(memory_space=pl.ANY)
    vmem = pl.BlockSpec(memory_space=pltpu.VMEM)
    adjoint, gradient = pl.pallas_call(
        functools.partial(kernel, levels, patches),
        out_shape=(
            jax.ShapeDtypeStruct((SLOTS, 2, SIDE, SIDE), F32),
            jax.ShapeDtypeStruct((SLOTS, SIDE, SIDE), BF16),
        ),
        in_specs=[pl.BlockSpec(memory_space=pltpu.SMEM)] + [any_space] * 4,
        out_specs=(vmem, vmem),
        scratch_shapes=[
            pltpu.VMEM((SLOTS, 2, SIDE, SIDE), BF16),
            pltpu.VMEM((SLOTS, 2, SIDE, SIDE), BF16),
            pltpu.VMEM((SLOTS, SIDE, SIDE), F32),
            pltpu.VMEM((SLOTS, SIDE, SIDE), BF16),
        ]
        + [tall] * 18
        + [
            pltpu.VMEM((2, SLOTS, 8, SIDE), F32),
            pltpu.VMEM((2, SLOTS, 8, SIDE), F32),
            pltpu.VMEM((2, 384, SIDE), F32),
            pltpu.VMEM((2, 256, SIDE), F32),
            pltpu.VMEM((2, 8, SIDE), F32),
            pltpu.VMEM((2, 8, SIDE), F32),
            pltpu.VMEM((2, 256, SIDE), F32),
            pltpu.VMEM((2, 256, SIDE), F32),
            pltpu.VMEM((2, 8, SIDE), F32),
            pltpu.VMEM((2, 8, SIDE), F32),
            pltpu.SemaphoreType.DMA((4,)),
            pltpu.SemaphoreType.DMA((8,)),
            pltpu.SemaphoreType.DMA((8,)),
        ],
        compiler_params=pltpu.CompilerParams(
            collective_id=0, has_side_effects=True, vmem_limit_bytes=56 << 20
        ),
    )(patch_rows, forcing[0], velocity[0], viscosity[0], friction[0])
    return adjoint[None], gradient[None]


def solution(mesh):
    in_specs = (
        P("level", "patch", None, None, None),
        P("level", "patch", None, None, None),
        P("level", "patch", None, None),
        P("level", "patch", None, None),
        P(),
    )
    out_specs = (P("level", "patch", None, None, None), P("level", "patch", None, None))
    return jax.shard_map(
        functools.partial(per_device, mesh.shape["level"], mesh.shape["patch"]),
        mesh=mesh,
        in_specs=in_specs,
        out_specs=out_specs,
        check_vma=False,
    )
```

```python
import functools

import jax
import jax.numpy as jnp
from jax import lax
from jax.experimental import pallas as pl
from jax.experimental.pallas import tpu as pltpu
from jax.sharding import PartitionSpec as P

MESH = pl.DeviceIdType.MESH
F32 = jnp.float32
BF16 = jnp.bfloat16
SIDE = 128
SLOTS = 8
PAD = 8
TALL = 3 * (SLOTS * SIDE + 2 * PAD)


def split_dot(x, matrix):
    high = x.astype(BF16)
    low = (x - high.astype(F32)).astype(BF16)
    return jnp.dot(high, matrix, preferred_element_type=F32) + jnp.dot(
        low, matrix, preferred_element_type=F32
    )


START_ROWS = {
    0: {0: (256, 1024), 1: (72, 256), 2: (24, 72), 3: (0, 24)},
    1: {1: (128, 512), 2: (40, 128), 3: (0, 40)},
    2: {2: (64, 256), 3: (0, 64)},
    3: {3: (0, 128)},
}
RESIDUAL_ROWS = {
    1: {1: (144, 512), 2: (48, 144), 3: (0, 48)},
    2: {2: (80, 256), 3: (0, 80)},
    3: {3: (0, 128)},
}
SMOOTH_ROWS = {
    1: {1: (152, 512), 2: (56, 152), 3: (0, 56)},
    2: {2: (120, 256), 3: (0, 120)},
    3: {3: (0, 128)},
}
SENT_UP = {
    0: {1: (72, 256), 2: (24, 72), 3: (0, 24)},
    1: {2: (56, 128), 3: (0, 56)},
    2: {3: (0, 64)},
}
ORDER = {
    0: (("down", 0), ("down", 1), ("down", 2), ("down", 3)),
    1: (("down", 1), ("down", 2), ("down", 3), ("up", 1), ("up", 2), ("up", 3)),
    2: (("down", 2), ("down", 3), ("up", 2), ("up", 3)),
    3: (("down", 3), ("up", 3)),
}


def over(first_col, col_count, rows, most, body):
    low, high = rows
    pieces = -(-(high - low) // most)
    size = -(-(high - low) // (8 * pieces)) * 8

    def step(index, carry):
        col = index // pieces
        part = index - col * pieces
        start = low if pieces == 1 else jnp.minimum(low + part * size, high - size)
        body(first_col + col, start, size)
        return carry

    lax.fori_loop(0, col_count * pieces, step, 0)


def kernel(
    levels,
    patches,
    rows_ref,
    forcing,
    velocity,
    viscosity,
    friction,
    out_ref,
    grad_ref,
    mu,
    fric,
    mu_e,
    mu_w,
    diag_u,
    diag_v,
    half_u,
    half_v,
    b_u,
    b_v,
    x_u,
    x_v,
    z_u,
    z_v,
    ue,
    uw,
    ve,
    vw,
    y_u,
    y_v,
    init_send,
    init_recv,
    down_send_1,
    down_send_2,
    down_send_3,
    down_recv_0,
    down_recv_1,
    down_recv_2,
    up_recv_1,
    up_recv_2,
    up_recv_3,
    down_edge_send,
    down_edge_recv,
    up_edge_send,
    up_edge_recv,
    init_sem,
    down_sem,
    down_edge_sem,
    up_sem,
    up_edge_sem,
):
    down_send = {1: down_send_1, 2: down_send_2, 3: down_send_3}
    down_recv = {0: down_recv_0, 1: down_recv_1, 2: down_recv_2}
    up_recv = {1: up_recv_1, 2: up_recv_2, 3: up_recv_3}
    level = lax.axis_index("level")
    patch = lax.axis_index("patch")
    cols = jnp.where(level == 0, 1, jnp.where(level == 1, 2, jnp.where(level == 2, 4, 8)))
    prows = jnp.where(level == 0, 8, jnp.where(level == 1, 4, jnp.where(level == 2, 2, 1)))
    height = prows * SIDE
    pitch = height + 2 * PAD
    has_west = patch > 0
    has_east = patch < patches - 1
    finer = jnp.minimum(level + 1, levels - 1)
    west = jnp.maximum(patch - 1, 0)
    east = jnp.minimum(patch + 1, patches - 1)
    own_rows = rows_ref[level, patch]
    west_rows = jnp.where(has_west, rows_ref[level, west], 0)
    east_rows = jnp.where(has_east, rows_ref[level, east], 0)
    fine_own = rows_ref[finer, patch]
    fine_west = jnp.where(has_west, rows_ref[finer, west], 0)
    fine_east = jnp.where(has_east, rows_ref[finer, east], 0)

    barrier = pltpu.get_barrier_semaphore()
    count = jnp.int32(0)
    for dl in (-1, 0, 1):
        for dp in (-1, 0, 1):
            if dl == 0 and dp == 0:
                continue
            there = (level + dl >= 0) & (level + dl < levels) & (patch + dp >= 0) & (patch + dp < patches)
            count = count + jnp.where(there, 1, 0)

            @pl.when(there)
            def _(dl=dl, dp=dp):
                pl.semaphore_signal(
                    barrier,
                    inc=1,
                    device_id={"level": level + dl, "patch": patch + dp},
                    device_id_type=MESH,
                )

    def base_of(col, row):
        return pl.multiple_of((col * pitch + PAD + row * SIDE).astype(jnp.int32), 8)

    def alive(row, total):
        return jnp.where(row < total, 1.0, 0.0).astype(F32)

    lane = lax.broadcasted_iota(jnp.int32, (SIDE, SIDE), 1)

    zeros = jnp.zeros((PAD, SIDE), F32)

    def clear(col, carry):
        first = pl.multiple_of(col * pitch, 8)
        last = pl.multiple_of(col * pitch + PAD + height, 8)
        for ref in (mu, x_u, x_v, z_u, z_v, ue, uw, ve, vw):
            ref[pl.ds(first, PAD), :] = zeros
            ref[pl.ds(last, PAD), :] = zeros
        return carry

    lax.fori_loop(0, cols + 2, clear, 0)

    def unpack(slot_id, carry):
        col = slot_id // prows
        row = slot_id - col * prows
        base = base_of(col + 1, row)
        slot = row * cols + col
        live = alive(row, own_rows)
        mu[pl.ds(base, SIDE), :] = viscosity[slot] * live
        fric[pl.ds(base, SIDE), :] = friction[slot].astype(F32)
        b_u[pl.ds(base, SIDE), :] = forcing[slot, 0].astype(F32) * live
        b_v[pl.ds(base, SIDE), :] = forcing[slot, 1].astype(F32) * live
        return carry

    lax.fori_loop(0, SLOTS, unpack, 0)

    def pack(row, carry):
        for side in range(2):
            base = base_of(jnp.where(side == 0, 1, cols), row)
            near, far = (0, 1) if side == 0 else (SIDE - 1, SIDE - 2)
            mu_t = jnp.transpose(mu[pl.ds(base, SIDE), :])
            fr_t = jnp.transpose(fric[pl.ds(base, SIDE), :])
            bu_t = jnp.transpose(b_u[pl.ds(base, SIDE), :])
            bv_t = jnp.transpose(b_v[pl.ds(base, SIDE), :])
            parts = [
                mu_t[near : near + 1],
                mu_t[far : far + 1],
                fr_t[near : near + 1],
                bu_t[near : near + 1],
                bv_t[near : near + 1],
                jnp.zeros((3, SIDE), F32),
            ]
            init_send[side, row] = jnp.concatenate(parts, axis=0)
        return carry

    lax.fori_loop(0, prows, pack, 0)

    pl.semaphore_wait(barrier, count)

    def copy_to(src, dst, send, recv, there, dp):
        return pltpu.make_async_remote_copy(
            src_ref=src,
            dst_ref=dst,
            send_sem=send,
            recv_sem=recv,
            device_id={"level": there, "patch": patch + dp},
            device_id_type=MESH,
        )

    init_west = copy_to(
        init_send.at[0], init_recv.at[0], init_sem.at[0], init_sem.at[2], level, -1
    )
    init_east = copy_to(
        init_send.at[1], init_recv.at[1], init_sem.at[1], init_sem.at[3], level, 1
    )

    @pl.when(has_west)
    def _():
        init_west.start()

    @pl.when(has_east)
    def _():
        init_east.start()

    @pl.when(has_east)
    def _():
        init_west.wait_recv()

    @pl.when(jnp.logical_not(has_east))
    def _():
        init_recv[0] = jnp.ones((SLOTS, 8, SIDE), F32)

    @pl.when(has_west)
    def _():
        init_east.wait_recv()

    @pl.when(jnp.logical_not(has_west))
    def _():
        init_recv[1] = jnp.ones((SLOTS, 8, SIDE), F32)

    def spread(tile_t, index, first=0, count=SIDE):
        return jnp.broadcast_to(tile_t[first : first + count, index : index + 1], (count, SIDE))

    def unpack_halo(row, carry):
        for side in range(2):
            col = cols + 1 if side == 0 else 0
            base = base_of(jnp.int32(0) + col, row)
            near = 0 if side == 0 else SIDE - 1
            live = alive(row, east_rows if side == 0 else west_rows)
            tile_t = jnp.transpose(init_recv[side, row])
            mu[pl.ds(base, SIDE), :] = (
                jnp.where(lane == near, spread(tile_t, 0), spread(tile_t, 1)) * live
            )
            fric[pl.ds(base, SIDE), :] = spread(tile_t, 2)
            b_u[pl.ds(base, SIDE), :] = spread(tile_t, 3) * live
            b_v[pl.ds(base, SIDE), :] = spread(tile_t, 4) * live
        return carry

    lax.fori_loop(0, prows, unpack_halo, 0)

    def coefficients(index, carry):
        col = index // prows
        row = index - col * prows
        base = base_of(col, row)
        to_east = pl.multiple_of(base + jnp.where(col == cols + 1, 0, pitch), 8)
        to_west = pl.multiple_of(base - jnp.where(col == 0, 0, pitch), 8)
        total = jnp.where(col == 0, west_rows, jnp.where(col == cols + 1, east_rows, own_rows))
        live = 0.5 * alive(row, total)
        here = mu[pl.ds(base, SIDE), :]
        m_e = pltpu.roll(jnp.where(lane == 0, mu[pl.ds(to_east, SIDE), :], here), SIDE - 1, 1)
        m_w = pltpu.roll(jnp.where(lane == SIDE - 1, mu[pl.ds(to_west, SIDE), :], here), 1, 1)
        across = m_e + m_w + 2.0 * here
        along = mu[pl.ds(base + 1, SIDE), :] + mu[pl.ds(base - 1, SIDE), :] + 2.0 * here
        fr = fric[pl.ds(base, SIDE), :]
        d_u = 2.0 * across + 0.5 * along + fr
        d_v = 2.0 * along + 0.5 * across + fr
        mu_e[pl.ds(base, SIDE), :] = m_e
        mu_w[pl.ds(base, SIDE), :] = m_w
        diag_u[pl.ds(base, SIDE), :] = d_u
        diag_v[pl.ds(base, SIDE), :] = d_v
        half_u[pl.ds(base, SIDE), :] = live / d_u
        half_v[pl.ds(base, SIDE), :] = live / d_v
        return carry

    first = jnp.where(level == 0, prows, 0)
    last = jnp.where(level == 0, 2 * prows, (cols + 2) * prows)
    lax.fori_loop(first, last, coefficients, 0)

    quarter = SIDE // 2
    lane_row = lax.broadcasted_iota(jnp.int32, (SIDE, SIDE), 0)
    joins = [
        jnp.where(lane_row // 2 + half * quarter == lane, 1.0, 0.0).astype(BF16)
        for half in range(2)
    ]
    spreads = [
        jnp.where(lane // 2 + half * quarter == lane_row, 1.0, 0.0).astype(BF16)
        for half in range(2)
    ]

    def program(lv):
        columns = 2**lv
        tall = SLOTS // columns * SIDE
        step_col = tall + 2 * PAD
        pending = []

        def at_row(col, row):
            return pl.multiple_of(col * step_col + PAD + row, 8)

        def below(start, size, limit):
            rows = lax.broadcasted_iota(jnp.int32, (size, SIDE), 0) + start
            return rows < limit

        def shift(src_u, src_v, rows):
            def body(col, start, size):
                base = at_row(col, start)
                to_east = pl.multiple_of(base + step_col, 8)
                to_west = pl.multiple_of(base - step_col, 8)
                here_lane = lane[:size]
                for src, dst_e, dst_w in ((src_u, ue, uw), (src_v, ve, vw)):
                    here = src[pl.ds(base, size), :]
                    dst_e[pl.ds(base, size), :] = pltpu.roll(
                        jnp.where(here_lane == 0, src[pl.ds(to_east, size), :], here), SIDE - 1, 1
                    )
                    dst_w[pl.ds(base, size), :] = pltpu.roll(
                        jnp.where(here_lane == SIDE - 1, src[pl.ds(to_west, size), :], here), 1, 1
                    )

            over(1, columns, rows, SIDE, body)

        def residual_at(src_u, src_v, base, size):
            def at(ref, step=0):
                return ref[pl.ds(base + step, size), :]

            m, m_e, m_w, m_n, m_s = at(mu), at(mu_e), at(mu_w), at(mu, 1), at(mu, -1)
            p_e, p_w, p_n, p_s = m + m_e, m + m_w, m + m_n, m + m_s
            ue_n, ue_s, uw_n, uw_s = at(ue, 1), at(ue, -1), at(uw, 1), at(uw, -1)
            ve_n, ve_s, vw_n, vw_s = at(ve, 1), at(ve, -1), at(vw, 1), at(vw, -1)
            u, v = at(src_u), at(src_v)
            cross_u = 0.5 * (m_e * (ve_n - ve_s) - m_w * (vw_n - vw_s)) + 0.25 * (
                m_n * (ve_n - vw_n) - m_s * (ve_s - vw_s)
            )
            cross_v = 0.5 * (m_n * (ue_n - uw_n) - m_s * (ue_s - uw_s)) + 0.25 * (
                m_e * (ue_n - ue_s) - m_w * (uw_n - uw_s)
            )
            near_u = 2.0 * (p_e * at(ue) + p_w * at(uw)) + 0.5 * (
                p_n * at(src_u, 1) + p_s * at(src_u, -1)
            )
            near_v = 2.0 * (p_n * at(src_v, 1) + p_s * at(src_v, -1)) + 0.5 * (
                p_e * at(ve) + p_w * at(vw)
            )
            r_u = at(b_u) - (at(diag_u) * u - near_u - cross_u)
            r_v = at(b_v) - (at(diag_v) * v - near_v - cross_v)
            return u, v, r_u, r_v

        def sides():
            return ((0, has_west, has_east, -1), (1, has_east, has_west, 1))

        def down_copies(sender, tier):
            low, high = RESIDUAL_ROWS[sender][tier]
            low, high = low // 2, high // 2
            copies = []
            for k in range(2**sender // 2):
                part = (slice(None), k, pl.ds(low, high - low))
                copies.append(
                    copy_to(
                        down_send[sender].at[part],
                        down_recv[sender - 1].at[part],
                        down_sem.at[0, tier * 4 + k],
                        down_sem.at[1, tier * 4 + k],
                        sender - 1,
                        0,
                    )
                )
            return copies

        def down_edge(sender, tier, side, dp):
            return copy_to(
                down_edge_send.at[tier, side],
                down_edge_recv.at[tier, side],
                down_edge_sem.at[0, tier * 2 + side],
                down_edge_sem.at[1, tier * 2 + side],
                sender - 1,
                dp,
            )

        def up_copies(sender, tier):
            low, high = SENT_UP[sender][tier]
            sources = (x_u, x_v) if sender == 0 else (y_u, y_v)
            pitch_here = SLOTS // 2**sender * SIDE + 2 * PAD
            copies = []
            for k in range(2**sender):
                for comp in range(2):
                    index = tier * 8 + k * 2 + comp
                    copies.append(
                        copy_to(
                            sources[comp].at[pl.ds((k + 1) * pitch_here + PAD + low, high - low)],
                            up_recv[sender + 1].at[comp, k, pl.ds(low, high - low)],
                            up_sem.at[0, index],
                            up_sem.at[1, index],
                            sender + 1,
                            0,
                        )
                    )
            return copies

        def up_edge(sender, tier, side, dp):
            return copy_to(
                up_edge_send.at[tier, side],
                up_edge_recv.at[tier, side],
                up_edge_sem.at[0, tier * 2 + side],
                up_edge_sem.at[1, tier * 2 + side],
                sender + 1,
                dp,
            )

        def start_edges(make, sender, tier):
            for side, there, _, dp in sides():
                copy = make(sender, tier, side, dp)

                @pl.when(there)
                def _(copy=copy):
                    copy.start()

                pending.append((copy, there))

        def wait_edges(make, sender, tier):
            for side, _, there, dp in sides():
                copy = make(sender, tier, side, dp)

                @pl.when(there)
                def _(copy=copy):
                    copy.wait_recv()

        def send_up(tier):
            low, high = SENT_UP[lv][tier]
            sources = (x_u, x_v) if lv == 0 else (y_u, y_v)
            for side in range(2):
                col = 1 if side == 0 else columns
                near = 0 if side == 0 else SIDE - 1
                parts = []
                for ref in sources:
                    for part in range(2):
                        if part * SIDE < high and low < (part + 1) * SIDE:
                            block_t = jnp.transpose(ref[pl.ds(at_row(col, part * SIDE), SIDE), :])
                            parts.append(block_t[near : near + 1])
                        else:
                            parts.append(jnp.zeros((1, SIDE), F32))
                parts.append(jnp.zeros((4, SIDE), F32))
                up_edge_send[tier, side] = jnp.concatenate(parts, axis=0)
            start_edges(up_edge, lv, tier)
            for copy in up_copies(lv, tier):
                copy.start()
                pending.append((copy, None))

        def down(tier):
            rows = START_ROWS[lv][tier]
            low, high = rows
            if tier == lv:

                def start_body(col, start, size):
                    where = pl.ds(at_row(col, start), size)
                    x_u[where, :] = half_u[where, :] * b_u[where, :]
                    x_v[where, :] = half_v[where, :] * b_v[where, :]

                if lv == 0:
                    over(1, 1, rows, SIDE, start_body)
                else:
                    over(0, columns + 2, rows, SIDE, start_body)
            else:
                if lv > 0:
                    wait_edges(down_edge, lv + 1, tier)
                    for side in range(2):
                        col = columns + 1 if side == 0 else 0
                        limit = quarter * (fine_east if side == 0 else fine_west)
                        tile_t = jnp.transpose(down_edge_recv[tier, side])
                        where = pl.ds(at_row(col, low), high - low)
                        keep = below(low, high - low, limit)
                        for comp, (ref, half, to) in enumerate(
                            ((b_u, half_u, x_u), (b_v, half_v, x_v))
                        ):
                            got = spread(tile_t, comp, low, high - low)
                            to[where, :] = half[where, :] * jnp.where(keep, got, ref[where, :])
                for copy in down_copies(lv + 1, tier):
                    copy.wait_recv()

                def place_body(col, start, size):
                    where = pl.ds(at_row(col, start), size)
                    keep = below(start, size, quarter * fine_own)
                    for comp, (ref, half, to) in enumerate(
                        ((b_u, half_u, x_u), (b_v, half_v, x_v))
                    ):
                        got = down_recv[lv][comp, col - 1, pl.ds(start, size), :]
                        new = jnp.where(keep, got, ref[where, :])
                        ref[where, :] = new
                        to[where, :] = half[where, :] * new

                over(1, columns, rows, SIDE, place_body)
            if lv == 0:
                if tier > 0:
                    send_up(tier)
                return
            shift(x_u, x_v, rows)

            def residual_body(col, start, size):
                base = at_row(col, start)
                _, _, r_u, r_v = residual_at(x_u, x_v, base, size)
                y_u[pl.ds(base, size), :] = r_u
                y_v[pl.ds(base, size), :] = r_v

            over(1, columns, RESIDUAL_ROWS[lv][tier], 64, residual_body)
            low, high = RESIDUAL_ROWS[lv][tier]
            low, high = low // 2, high // 2
            pairs = columns // 2
            copies = down_copies(lv, tier)

            def join_pair(k):
                def join_body(_, start, size):
                    for comp, ref in enumerate((y_u, y_v)):
                        total = None
                        for half in range(2):
                            base = at_row(2 * k + half + 1, 2 * start)
                            lines = (
                                ref[pl.ds(base, size, stride=2), :]
                                + ref[pl.ds(base + 1, size, stride=2), :]
                            )
                            term = split_dot(lines, joins[half])
                            total = term if total is None else total + term
                        down_send[lv][comp, k, pl.ds(start, size), :] = total

                over(0, 1, (low, high), 64, join_body)
                copies[k].start()
                pending.append((copies[k], None))

            for k in sorted({0, pairs - 1}):
                join_pair(k)
            if lv > 1:
                for side in range(2):
                    k = 0 if side == 0 else pairs - 1
                    near = 0 if side == 0 else SIDE - 1
                    lines = min(SIDE, tall // 2)
                    parts = []
                    for comp in range(2):
                        block_t = jnp.transpose(down_send[lv][comp, k, pl.ds(0, lines), :])
                        line = block_t[near : near + 1]
                        if lines < SIDE:
                            line = jnp.concatenate([line, line], axis=1)
                        parts.append(line)
                    parts.append(jnp.zeros((6, SIDE), F32))
                    down_edge_send[tier, side] = jnp.concatenate(parts, axis=0)
                start_edges(down_edge, lv, tier)
            for k in range(1, pairs - 1):
                join_pair(k)

        def up(tier):
            low, high = SENT_UP[lv - 1][tier]
            wait_edges(up_edge, lv - 1, tier)
            for side in range(2):
                col = columns + 1 if side == 0 else 0
                limit = quarter * (east_rows if side == 0 else west_rows)
                tile_t = jnp.transpose(up_edge_recv[tier, side])
                for part in range(2):
                    first, last = max(low, part * SIDE), min(high, (part + 1) * SIDE)
                    if first >= last:
                        continue
                    size = last - first
                    keep = below(first, size, limit)
                    for comp, (ref, to) in enumerate(((x_u, z_u), (x_v, z_v))):
                        wide = spread(tile_t, 2 * comp + part, first - part * SIDE, size)
                        wide = jnp.where(keep, wide, 0.0)
                        for step in range(2):
                            where = pl.ds(at_row(col, 2 * first) + step, size, stride=2)
                            to[where, :] = ref[where, :] + wide
            for copy in up_copies(lv - 1, tier):
                copy.wait_recv()

            def prolong_body(k, start, size):
                keep = below(start, size, quarter * own_rows)
                for comp, (ref, to) in enumerate(((x_u, z_u), (x_v, z_v))):
                    coarse = up_recv[lv][comp, k, pl.ds(start, size), :]
                    coarse = jnp.where(keep, coarse, 0.0)
                    for half in range(2):
                        base = at_row(2 * k + half + 1, 2 * start)
                        wide = split_dot(coarse, spreads[half])
                        for step in range(2):
                            where = pl.ds(base + step, size, stride=2)
                            to[where, :] = ref[where, :] + wide

            over(0, columns // 2, (low, high), 64, prolong_body)
            shift(z_u, z_v, (2 * low, 2 * high))

            def smooth_body(col, start, size):
                base = at_row(col, start)
                where = pl.ds(base, size)
                u, v, r_u, r_v = residual_at(z_u, z_v, base, size)
                y_u[where, :] = u + half_u[where, :] * r_u
                y_v[where, :] = v + half_v[where, :] * r_v

            over(1, columns, SMOOTH_ROWS[lv][tier], 64, smooth_body)
            if lv < levels - 1 and tier > lv:
                send_up(tier)

        for stage, tier in ORDER[lv]:
            (down if stage == "down" else up)(tier)

        finals = (x_u, x_v) if lv == 0 else (y_u, y_v)

        def finish(col, start, size):
            base = at_row(col, start)
            row = start // SIDE
            slot = row * columns + col - 1
            live = alive(row, own_rows)
            u = finals[0][pl.ds(base, size), :]
            v = finals[1][pl.ds(base, size), :]
            out_ref[slot, 0] = u
            out_ref[slot, 1] = v
            product = velocity[slot, 0].astype(F32) * u + velocity[slot, 1].astype(F32) * v
            grad_ref[slot] = (-(friction[slot].astype(F32) * product) * live).astype(BF16)

        over(1, columns, (0, tall), SIDE, finish)
        for copy, there in pending:
            if there is None:
                copy.wait_send()
            else:

                @pl.when(there)
                def _(copy=copy):
                    copy.wait_send()

    for lv in range(levels):

        @pl.when(level == lv)
        def _(lv=lv):
            program(lv)

    @pl.when(has_west)
    def _():
        init_west.wait_send()

    @pl.when(has_east)
    def _():
        init_east.wait_send()


def per_device(levels, patches, forcing, velocity, viscosity, friction, patch_rows):
    tall = pltpu.VMEM((TALL, SIDE), F32)
    vmem = pl.BlockSpec(memory_space=pltpu.VMEM)
    coarse = {
        sender: pltpu.VMEM((2, 2**sender // 2, SLOTS // 2**sender * SIDE // 2, SIDE), F32)
        for sender in range(1, levels)
    }
    adjoint, gradient = pl.pallas_call(
        functools.partial(kernel, levels, patches),
        out_shape=(
            jax.ShapeDtypeStruct((SLOTS, 2, SIDE, SIDE), F32),
            jax.ShapeDtypeStruct((SLOTS, SIDE, SIDE), BF16),
        ),
        in_specs=[pl.BlockSpec(memory_space=pltpu.SMEM)] + [vmem] * 4,
        out_specs=(vmem, vmem),
        scratch_shapes=[tall] * 20
        + [
            pltpu.VMEM((2, SLOTS, 8, SIDE), F32),
            pltpu.VMEM((2, SLOTS, 8, SIDE), F32),
        ]
        + [coarse[sender] for sender in range(1, levels)] * 3
        + [pltpu.VMEM((4, 2, 8, SIDE), F32)] * 4
        + [
            pltpu.SemaphoreType.DMA((4,)),
            pltpu.SemaphoreType.DMA((2, 16)),
            pltpu.SemaphoreType.DMA((2, 8)),
            pltpu.SemaphoreType.DMA((2, 32)),
            pltpu.SemaphoreType.DMA((2, 8)),
        ],
        compiler_params=pltpu.CompilerParams(
            collective_id=0, has_side_effects=True, vmem_limit_bytes=44 << 20
        ),
    )(patch_rows, forcing[0], velocity[0], viscosity[0], friction[0])
    return adjoint[None], gradient[None]


def solution(mesh):
    in_specs = (
        P("level", "patch", None, None, None),
        P("level", "patch", None, None, None),
        P("level", "patch", None, None),
        P("level", "patch", None, None),
        P(),
    )
    out_specs = (P("level", "patch", None, None, None), P("level", "patch", None, None))
    return jax.shard_map(
        functools.partial(per_device, mesh.shape["level"], mesh.shape["patch"]),
        mesh=mesh,
        in_specs=in_specs,
        out_specs=out_specs,
        check_vma=False,
    )
```

```python
import functools

import jax
import jax.numpy as jnp
from jax import lax
from jax.experimental import pallas as pl
from jax.experimental.pallas import tpu as pltpu
from jax.sharding import PartitionSpec as P

MESH = pl.DeviceIdType.MESH
F32 = jnp.float32
BF16 = jnp.bfloat16
SIDE = 128
SLOTS = 8
PAD = 8
TALL = 3 * (SLOTS * SIDE + 2 * PAD)


def split_dot(x, matrix):
    high = x.astype(BF16)
    low = (x - high.astype(F32)).astype(BF16)
    return jnp.dot(high, matrix, preferred_element_type=F32) + jnp.dot(
        low, matrix, preferred_element_type=F32
    )


START_ROWS = {
    0: {0: (256, 1024), 1: (72, 256), 2: (24, 72), 3: (0, 24)},
    1: {1: (128, 512), 2: (40, 128), 3: (0, 40)},
    2: {2: (64, 256), 3: (0, 64)},
    3: {3: (0, 128)},
}
RESIDUAL_ROWS = {
    1: {1: (144, 512), 2: (48, 144), 3: (0, 48)},
    2: {2: (80, 256), 3: (0, 80)},
    3: {3: (0, 128)},
}
SMOOTH_ROWS = {
    1: {1: (136, 512), 2: (56, 136), 3: (0, 56)},
    2: {2: (64, 256), 3: (0, 64)},
    3: {3: (0, 128)},
}
SENT_UP = {
    0: {1: (72, 256), 2: (24, 72), 3: (0, 24)},
    1: {2: (40, 128), 3: (0, 40)},
    2: {3: (0, 64)},
}
ORDER = {
    0: "down0 down1 send1 down2 send2 down3 send3",
    1: "down1 down2 down3 up2 up3 send3 send2 up1",
    2: "down2 down3 up3 up2",
    3: "down3 up3",
}


def over(col_at, col_count, rows, most, body):
    low, high = rows
    pieces = -(-(high - low) // most)
    size = -(-(high - low) // (8 * pieces)) * 8

    def step(index, carry):
        col = index // pieces
        part = index - col * pieces
        start = low if pieces == 1 else jnp.minimum(low + part * size, high - size)
        body(col_at + col if isinstance(col_at, int) else col_at(col), start, size)
        return carry

    lax.fori_loop(0, col_count * pieces, step, 0)


def kernel(
    levels,
    patches,
    rows_ref,
    forcing_hbm,
    velocity_hbm,
    viscosity_hbm,
    friction_hbm,
    out_ref,
    grad_ref,
    forcing,
    velocity,
    viscosity,
    friction,
    mu,
    fric,
    mu_e,
    mu_w,
    diag_u,
    diag_v,
    half_u,
    half_v,
    b_u,
    b_v,
    x_u,
    x_v,
    z_u,
    z_v,
    ue,
    uw,
    ve,
    vw,
    y_u,
    y_v,
    init_send,
    init_recv,
    down_send_1,
    down_send_2,
    down_send_3,
    down_recv_0,
    down_recv_1,
    down_recv_2,
    up_recv_1,
    up_recv_2,
    up_recv_3,
    down_edge_send,
    down_edge_recv,
    up_edge_send,
    up_edge_recv,
    load_sem,
    init_sem,
    down_sem,
    down_edge_sem,
    up_sem,
    up_edge_sem,
):
    down_send = {1: down_send_1, 2: down_send_2, 3: down_send_3}
    down_recv = {0: down_recv_0, 1: down_recv_1, 2: down_recv_2}
    up_recv = {1: up_recv_1, 2: up_recv_2, 3: up_recv_3}
    level = lax.axis_index("level")
    patch = lax.axis_index("patch")
    cols = jnp.where(level == 0, 1, jnp.where(level == 1, 2, jnp.where(level == 2, 4, 8)))
    prows = jnp.where(level == 0, 8, jnp.where(level == 1, 4, jnp.where(level == 2, 2, 1)))
    height = prows * SIDE
    pitch = height + 2 * PAD
    has_west = patch > 0
    has_east = patch < patches - 1
    finer = jnp.minimum(level + 1, levels - 1)
    west = jnp.maximum(patch - 1, 0)
    east = jnp.minimum(patch + 1, patches - 1)
    own_rows = rows_ref[level, patch]
    west_rows = jnp.where(has_west, rows_ref[level, west], 0)
    east_rows = jnp.where(has_east, rows_ref[level, east], 0)
    fine_own = rows_ref[finer, patch]
    fine_west = jnp.where(has_west, rows_ref[finer, west], 0)
    fine_east = jnp.where(has_east, rows_ref[finer, east], 0)

    loads = [
        pltpu.make_async_copy(src, dst, load_sem.at[i])
        for i, (src, dst) in enumerate(
            (
                (viscosity_hbm, viscosity),
                (friction_hbm, friction),
                (forcing_hbm, forcing),
                (velocity_hbm, velocity),
            )
        )
    ]
    for load in loads:
        load.start()

    barrier = pltpu.get_barrier_semaphore()
    count = jnp.int32(0)
    for dl in (-1, 0, 1):
        for dp in (-1, 0, 1):
            if (dl == 0) == (dp == 0):
                continue
            there = (level + dl >= 0) & (level + dl < levels) & (patch + dp >= 0) & (patch + dp < patches)
            count = count + jnp.where(there, 1, 0)

            @pl.when(there)
            def _(dl=dl, dp=dp):
                pl.semaphore_signal(
                    barrier,
                    inc=1,
                    device_id={"level": level + dl, "patch": patch + dp},
                    device_id_type=MESH,
                )

    def base_of(col, row):
        return pl.multiple_of((col * pitch + PAD + row * SIDE).astype(jnp.int32), 8)

    def alive(row, total):
        return jnp.where(row < total, 1.0, 0.0).astype(F32)

    lane = lax.broadcasted_iota(jnp.int32, (SIDE, SIDE), 1)

    zeros = jnp.zeros((PAD, SIDE), F32)

    def clear(col, carry):
        first = pl.multiple_of(col * pitch, 8)
        last = pl.multiple_of(col * pitch + PAD + height, 8)
        for ref in (mu, x_u, x_v, z_u, z_v, ue, uw, ve, vw):
            ref[pl.ds(first, PAD), :] = zeros
            ref[pl.ds(last, PAD), :] = zeros
        return carry

    lax.fori_loop(0, cols + 2, clear, 0)

    for load in loads[:3]:
        load.wait()

    def unpack(slot_id, carry):
        col = slot_id // prows
        row = slot_id - col * prows
        base = base_of(col + 1, row)
        slot = row * cols + col
        live = alive(row, own_rows)
        mu[pl.ds(base, SIDE), :] = viscosity[slot] * live
        fric[pl.ds(base, SIDE), :] = friction[slot].astype(F32)
        b_u[pl.ds(base, SIDE), :] = forcing[slot, 0].astype(F32) * live
        b_v[pl.ds(base, SIDE), :] = forcing[slot, 1].astype(F32) * live
        return carry

    lax.fori_loop(0, SLOTS, unpack, 0)

    def pack(row, carry):
        for side in range(2):
            base = base_of(jnp.where(side == 0, 1, cols), row)
            near, far = (0, 1) if side == 0 else (SIDE - 1, SIDE - 2)
            mu_t = jnp.transpose(mu[pl.ds(base, SIDE), :])
            fr_t = jnp.transpose(fric[pl.ds(base, SIDE), :])
            bu_t = jnp.transpose(b_u[pl.ds(base, SIDE), :])
            bv_t = jnp.transpose(b_v[pl.ds(base, SIDE), :])
            parts = [
                mu_t[near : near + 1],
                mu_t[far : far + 1],
                fr_t[near : near + 1],
                bu_t[near : near + 1],
                bv_t[near : near + 1],
                jnp.zeros((3, SIDE), F32),
            ]
            init_send[side, row] = jnp.concatenate(parts, axis=0)
        return carry

    lax.fori_loop(0, prows, pack, 0)

    pl.semaphore_wait(barrier, count)

    def copy_to(src, dst, send, recv, there, dp):
        return pltpu.make_async_remote_copy(
            src_ref=src,
            dst_ref=dst,
            send_sem=send,
            recv_sem=recv,
            device_id={"level": there, "patch": patch + dp},
            device_id_type=MESH,
        )

    def init_copies(lv, side):
        used = pl.ds(0, SLOTS // 2**lv)
        return copy_to(
            init_send.at[side, used],
            init_recv.at[side, used],
            init_sem.at[side],
            init_sem.at[2 + side],
            lv,
            -1 if side == 0 else 1,
        )

    def init_each(act, flip):
        for lv in range(levels):
            for side in range(2):
                there = has_west if (side == 0) != flip else has_east

                @pl.when((level == lv) & there)
                def _(lv=lv, side=side):
                    act(init_copies(lv, side))

    init_each(lambda copy: copy.start(), False)

    def spread(tile_t, index, first=0, count=SIDE):
        return jnp.broadcast_to(tile_t[first : first + count, index : index + 1], (count, SIDE))

    def coefficients(index, carry):
        col = index // prows
        row = index - col * prows
        base = base_of(col, row)
        to_east = pl.multiple_of(base + jnp.where(col == cols + 1, 0, pitch), 8)
        to_west = pl.multiple_of(base - jnp.where(col == 0, 0, pitch), 8)
        total = jnp.where(col == 0, west_rows, jnp.where(col == cols + 1, east_rows, own_rows))
        live = 0.5 * alive(row, total)
        here = mu[pl.ds(base, SIDE), :]
        m_e = pltpu.roll(jnp.where(lane == 0, mu[pl.ds(to_east, SIDE), :], here), SIDE - 1, 1)
        m_w = pltpu.roll(jnp.where(lane == SIDE - 1, mu[pl.ds(to_west, SIDE), :], here), 1, 1)
        across = m_e + m_w + 2.0 * here
        along = mu[pl.ds(base + 1, SIDE), :] + mu[pl.ds(base - 1, SIDE), :] + 2.0 * here
        fr = fric[pl.ds(base, SIDE), :]
        d_u = 2.0 * across + 0.5 * along + fr
        d_v = 2.0 * along + 0.5 * across + fr
        mu_e[pl.ds(base, SIDE), :] = m_e
        mu_w[pl.ds(base, SIDE), :] = m_w
        diag_u[pl.ds(base, SIDE), :] = d_u
        diag_v[pl.ds(base, SIDE), :] = d_v
        half_u[pl.ds(base, SIDE), :] = live / d_u
        half_v[pl.ds(base, SIDE), :] = live / d_v
        return carry

    quarter = SIDE // 2
    lane_row = lax.broadcasted_iota(jnp.int32, (SIDE, SIDE), 0)
    joins = [
        jnp.where(lane_row // 2 + half * quarter == lane, 1.0, 0.0).astype(BF16)
        for half in range(2)
    ]
    spreads = [
        jnp.where(lane // 2 + half * quarter == lane_row, 1.0, 0.0).astype(BF16)
        for half in range(2)
    ]

    def program(lv, early):
        columns = 2**lv
        tall = SLOTS // columns * SIDE
        step_col = tall + 2 * PAD
        pending = []

        def at_row(col, row):
            return pl.multiple_of(col * step_col + PAD + row, 8)

        def below(start, size, limit):
            rows = lax.broadcasted_iota(jnp.int32, (size, SIDE), 0) + start
            return rows < limit

        def shift(src_u, src_v, rows, first=1, count=columns):
            def body(col, start, size):
                base = at_row(col, start)
                to_east = pl.multiple_of(base + step_col, 8)
                to_west = pl.multiple_of(base - step_col, 8)
                here_lane = lane[:size]
                for src, dst_e, dst_w in ((src_u, ue, uw), (src_v, ve, vw)):
                    here = src[pl.ds(base, size), :]
                    dst_e[pl.ds(base, size), :] = pltpu.roll(
                        jnp.where(here_lane == 0, src[pl.ds(to_east, size), :], here), SIDE - 1, 1
                    )
                    dst_w[pl.ds(base, size), :] = pltpu.roll(
                        jnp.where(here_lane == SIDE - 1, src[pl.ds(to_west, size), :], here), 1, 1
                    )

            over(first, count, rows, SIDE, body)

        def residual_at(src_u, src_v, base, size):
            def at(ref, step=0):
                return ref[pl.ds(base + step, size), :]

            m, m_e, m_w, m_n, m_s = at(mu), at(mu_e), at(mu_w), at(mu, 1), at(mu, -1)
            p_e, p_w, p_n, p_s = m + m_e, m + m_w, m + m_n, m + m_s
            ue_n, ue_s, uw_n, uw_s = at(ue, 1), at(ue, -1), at(uw, 1), at(uw, -1)
            ve_n, ve_s, vw_n, vw_s = at(ve, 1), at(ve, -1), at(vw, 1), at(vw, -1)
            u, v = at(src_u), at(src_v)
            cross_u = 0.5 * (m_e * (ve_n - ve_s) - m_w * (vw_n - vw_s)) + 0.25 * (
                m_n * (ve_n - vw_n) - m_s * (ve_s - vw_s)
            )
            cross_v = 0.5 * (m_n * (ue_n - uw_n) - m_s * (ue_s - uw_s)) + 0.25 * (
                m_e * (ue_n - ue_s) - m_w * (uw_n - uw_s)
            )
            near_u = 2.0 * (p_e * at(ue) + p_w * at(uw)) + 0.5 * (
                p_n * at(src_u, 1) + p_s * at(src_u, -1)
            )
            near_v = 2.0 * (p_n * at(src_v, 1) + p_s * at(src_v, -1)) + 0.5 * (
                p_e * at(ve) + p_w * at(vw)
            )
            r_u = at(b_u) - (at(diag_u) * u - near_u - cross_u)
            r_v = at(b_v) - (at(diag_v) * v - near_v - cross_v)
            return u, v, r_u, r_v

        def sides():
            return ((0, has_west, has_east, -1), (1, has_east, has_west, 1))

        def down_copies(sender, tier, which=None):
            low, high = RESIDUAL_ROWS[sender][tier]
            low, high = low // 2, high // 2
            copies = []
            for k in range(2**sender // 2) if which is None else which:
                part = (slice(None), k, pl.ds(low, high - low))
                copies.append(
                    copy_to(
                        down_send[sender].at[part],
                        down_recv[sender - 1].at[part],
                        down_sem.at[0, tier * 4 + k],
                        down_sem.at[1, tier * 4 + k],
                        sender - 1,
                        0,
                    )
                )
            return copies

        def down_edge(sender, tier, side, dp):
            return copy_to(
                down_edge_send.at[tier, side],
                down_edge_recv.at[tier, side],
                down_edge_sem.at[0, tier * 2 + side],
                down_edge_sem.at[1, tier * 2 + side],
                sender - 1,
                dp,
            )

        def up_copies(sender, tier):
            low, high = SENT_UP[sender][tier]
            sources = (x_u, x_v) if sender == 0 else (y_u, y_v)
            pitch_here = SLOTS // 2**sender * SIDE + 2 * PAD
            copies = []
            for k in range(2**sender):
                for comp in range(2):
                    index = tier * 8 + k * 2 + comp
                    copies.append(
                        copy_to(
                            sources[comp].at[pl.ds((k + 1) * pitch_here + PAD + low, high - low)],
                            up_recv[sender + 1].at[comp, k, pl.ds(low, high - low)],
                            up_sem.at[0, index],
                            up_sem.at[1, index],
                            sender + 1,
                            0,
                        )
                    )
            return copies

        def up_edge(sender, tier, side, dp):
            return copy_to(
                up_edge_send.at[tier, side],
                up_edge_recv.at[tier, side],
                up_edge_sem.at[0, tier * 2 + side],
                up_edge_sem.at[1, tier * 2 + side],
                sender + 1,
                dp,
            )

        def start_edges(make, sender, tier, which=(0, 1)):
            for side, there, _, dp in sides():
                if side not in which:
                    continue
                copy = make(sender, tier, side, dp)

                @pl.when(there)
                def _(copy=copy):
                    copy.start()

                pending.append((copy, there))

        def wait_edges(make, sender, tier, which=(0, 1)):
            for side, _, there, dp in sides():
                if side not in which:
                    continue
                copy = make(sender, tier, side, dp)

                @pl.when(there)
                def _(copy=copy):
                    copy.wait_recv()

        def fill_up_edges(tier, which=(0, 1)):
            low, high = SENT_UP[lv][tier]
            sources = (x_u, x_v) if lv == 0 else (y_u, y_v)
            for side in which:
                col = 1 if side == 0 else columns
                near = 0 if side == 0 else SIDE - 1
                parts = []
                for ref in sources:
                    for part in range(2):
                        if part * SIDE < high and low < (part + 1) * SIDE:
                            block_t = jnp.transpose(ref[pl.ds(at_row(col, part * SIDE), SIDE), :])
                            parts.append(block_t[near : near + 1])
                        else:
                            parts.append(jnp.zeros((1, SIDE), F32))
                parts.append(jnp.zeros((4, SIDE), F32))
                up_edge_send[tier, side] = jnp.concatenate(parts, axis=0)

        def send_up(tier):
            fill_up_edges(tier)
            start_edges(up_edge, lv, tier)
            for copy in up_copies(lv, tier):
                copy.start()
                pending.append((copy, None))

        def start_body(col, start, size):
            where = pl.ds(at_row(col, start), size)
            x_u[where, :] = half_u[where, :] * b_u[where, :]
            x_v[where, :] = half_v[where, :] * b_v[where, :]

        def down(tier):
            rows = START_ROWS[lv][tier]
            low, high = rows
            if tier == lv:
                if lv == 0:
                    over(1, 1, rows, SIDE, start_body)
                else:
                    over(0, columns + 2, rows, SIDE, start_body)
            else:
                if lv > 0:
                    wait_edges(down_edge, lv + 1, tier)
                    for side in range(2):
                        col = columns + 1 if side == 0 else 0
                        limit = quarter * (fine_east if side == 0 else fine_west)
                        tile_t = jnp.transpose(down_edge_recv[tier, side])
                        where = pl.ds(at_row(col, low), high - low)
                        keep = below(low, high - low, limit)
                        for comp, (ref, half, to) in enumerate(
                            ((b_u, half_u, x_u), (b_v, half_v, x_v))
                        ):
                            got = spread(tile_t, comp, low, high - low)
                            to[where, :] = half[where, :] * jnp.where(keep, got, ref[where, :])
                for copy in down_copies(lv + 1, tier):
                    copy.wait_recv()

                def place_body(col, start, size):
                    where = pl.ds(at_row(col, start), size)
                    keep = below(start, size, quarter * fine_own)
                    for comp, (ref, half, to) in enumerate(
                        ((b_u, half_u, x_u), (b_v, half_v, x_v))
                    ):
                        got = down_recv[lv][comp, col - 1, pl.ds(start, size), :]
                        new = jnp.where(keep, got, ref[where, :])
                        ref[where, :] = new
                        to[where, :] = half[where, :] * new

                over(1, columns, rows, SIDE, place_body)
            if lv == 0:
                return
            shift(x_u, x_v, rows)
            over(1, columns, RESIDUAL_ROWS[lv][tier], 64, residual_body)
            send_down(tier, range(columns // 2))

        def residual_body(col, start, size):
            base = at_row(col, start)
            _, _, r_u, r_v = residual_at(x_u, x_v, base, size)
            y_u[pl.ds(base, size), :] = r_u
            y_v[pl.ds(base, size), :] = r_v

        def send_down(tier, which):
            low, high = RESIDUAL_ROWS[lv][tier]
            low, high = low // 2, high // 2
            pairs = columns // 2
            def join_pair(k):
                def join_body(_, start, size):
                    for comp, ref in enumerate((y_u, y_v)):
                        total = None
                        for half in range(2):
                            base = at_row(2 * k + half + 1, 2 * start)
                            lines = (
                                ref[pl.ds(base, size, stride=2), :]
                                + ref[pl.ds(base + 1, size, stride=2), :]
                            )
                            term = split_dot(lines, joins[half])
                            total = term if total is None else total + term
                        down_send[lv][comp, k, pl.ds(start, size), :] = total

                over(0, 1, (low, high), 64, join_body)
                copy = down_copies(lv, tier, (k,))[0]
                copy.start()
                pending.append((copy, None))

            for k in sorted({0, pairs - 1}):
                if k in which:
                    join_pair(k)
            if lv > 1 and 0 in which:
                for side in range(2):
                    k = 0 if side == 0 else pairs - 1
                    near = 0 if side == 0 else SIDE - 1
                    lines = min(SIDE, tall // 2)
                    parts = []
                    for comp in range(2):
                        block_t = jnp.transpose(down_send[lv][comp, k, pl.ds(0, lines), :])
                        line = block_t[near : near + 1]
                        if lines < SIDE:
                            line = jnp.concatenate([line, line], axis=1)
                        parts.append(line)
                    parts.append(jnp.zeros((6, SIDE), F32))
                    down_edge_send[tier, side] = jnp.concatenate(parts, axis=0)
                start_edges(down_edge, lv, tier)
            for k in range(1, pairs - 1):
                if k in which:
                    join_pair(k)

        def up(tier):
            low, high = SENT_UP[lv - 1][tier]
            halo_up(tier)
            for copy in up_copies(lv - 1, tier):
                copy.wait_recv()
            prolong(tier, 0, columns // 2)
            shift(z_u, z_v, (2 * low, 2 * high))
            rows = SMOOTH_ROWS[lv][tier]
            if lv == 2 and tier == 3:
                copies = up_copies(lv, tier)
                for col in range(1, columns + 1):
                    over(col, 1, rows, 64, smooth_body)
                    for copy in copies[2 * col - 2 : 2 * col]:
                        copy.start()
                        pending.append((copy, None))
                    if col in (1, columns):
                        side = 0 if col == 1 else 1
                        fill_up_edges(tier, (side,))
                        start_edges(up_edge, lv, tier, (side,))
            else:
                over(1, columns, rows, 64, smooth_body)

        def smooth_body(col, start, size):
            base = at_row(col, start)
            where = pl.ds(base, size)
            u, v, r_u, r_v = residual_at(z_u, z_v, base, size)
            u = u + half_u[where, :] * r_u
            v = v + half_v[where, :] * r_v
            if lv < levels - 1:
                y_u[where, :] = u
                y_v[where, :] = v
                return
            slot = col - 1
            lines = pl.ds(start, size)
            live = alive(0, own_rows)
            out_ref[slot, 0, lines, :] = u
            out_ref[slot, 1, lines, :] = v
            product = (
                velocity[slot, 0, lines, :].astype(F32) * u
                + velocity[slot, 1, lines, :].astype(F32) * v
            )
            grad_ref[slot, lines, :] = (
                -(friction[slot, lines, :].astype(F32) * product) * live
            ).astype(BF16)

        def up_last():
            tier = levels - 1
            rows = (0, tall)
            copies = up_copies(lv - 1, tier)
            for k in range(4):
                if k == 2:
                    halo_up(tier, (1,))
                if k == 3:
                    halo_up(tier, (0,))
                for copy in copies[2 * k : 2 * k + 2]:
                    copy.wait_recv()
                prolong(tier, k, 1)
                if k > 0:
                    first = 2 * k
                    count = 3 if k == 3 else 2
                    if k == 2:
                        columns_at = lambda i: jnp.where(i == 0, 1, i + 3)
                        first, count = columns_at, 3
                    shift(z_u, z_v, rows, first, count)
                    over(first, count, rows, 64, smooth_body)

        def halo_up(tier, which=(0, 1)):
            low, high = SENT_UP[lv - 1][tier]
            wait_edges(up_edge, lv - 1, tier, which)
            for side in which:
                col = columns + 1 if side == 0 else 0
                limit = quarter * (east_rows if side == 0 else west_rows)
                tile_t = jnp.transpose(up_edge_recv[tier, side])
                for part in range(2):
                    first, last = max(low, part * SIDE), min(high, (part + 1) * SIDE)
                    if first >= last:
                        continue
                    size = last - first
                    keep = below(first, size, limit)
                    for comp, (ref, to) in enumerate(((x_u, z_u), (x_v, z_v))):
                        wide = spread(tile_t, 2 * comp + part, first - part * SIDE, size)
                        wide = jnp.where(keep, wide, 0.0)
                        for step in range(2):
                            where = pl.ds(at_row(col, 2 * first) + step, size, stride=2)
                            to[where, :] = ref[where, :] + wide

        def prolong(tier, first, count):
            low, high = SENT_UP[lv - 1][tier]

            def prolong_body(k, start, size):
                keep = below(start, size, quarter * own_rows)
                for comp, (ref, to) in enumerate(((x_u, z_u), (x_v, z_v))):
                    coarse = up_recv[lv][comp, k, pl.ds(start, size), :]
                    coarse = jnp.where(keep, coarse, 0.0)
                    for half in range(2):
                        base = at_row(2 * k + half + 1, 2 * start)
                        wide = split_dot(coarse, spreads[half])
                        for step in range(2):
                            where = pl.ds(base + step, size, stride=2)
                            to[where, :] = ref[where, :] + wide

            over(first, count, (low, high), 64, prolong_body)

        if lv == levels - 1:
            if early:
                lax.fori_loop(2, columns, coefficients, 0)
                over(2, columns - 2, (0, tall), SIDE, start_body)
                shift(x_u, x_v, (0, tall), 3, columns - 4)
                over(3, columns - 4, (0, tall), 64, residual_body)
                send_down(lv, (1, 2))
                return
            ends = lambda i: jnp.where(i < 2, i, i + 6)
            inner = lambda i: jnp.where(i < 2, i + 1, i + 5)
            lax.fori_loop(0, 4, lambda i, carry: coefficients(ends(i), carry), 0)
            over(ends, 4, (0, tall), SIDE, start_body)
            shift(x_u, x_v, (0, tall), inner, 4)
            over(inner, 4, (0, tall), 64, residual_body)
            send_down(lv, (0, 3))
            pending.extend((copy, None) for copy in down_copies(lv, lv, (1, 2)))
            loads[3].wait()
            up_last()
        else:
            for word in ORDER[lv].split():
                {"down": down, "up": up, "send": send_up}[word[:-1]](int(word[-1]))
            loads[3].wait()

        finals = (x_u, x_v) if lv == 0 else (y_u, y_v)

        def finish(col, start, size):
            base = at_row(col, start)
            row = start // SIDE
            slot = row * columns + col - 1
            live = alive(row, own_rows)
            u = finals[0][pl.ds(base, size), :]
            v = finals[1][pl.ds(base, size), :]
            out_ref[slot, 0] = u
            out_ref[slot, 1] = v
            product = velocity[slot, 0].astype(F32) * u + velocity[slot, 1].astype(F32) * v
            grad_ref[slot] = (-(friction[slot].astype(F32) * product) * live).astype(BF16)

        if lv < levels - 1:
            over(1, columns, (0, tall), SIDE, finish)
        for copy, there in pending:
            if there is None:
                copy.wait_send()
            else:

                @pl.when(there)
                def _(copy=copy):
                    copy.wait_send()

    @pl.when(level == levels - 1)
    def _():
        program(levels - 1, True)

    @pl.when(jnp.logical_not(has_east))
    def _():
        init_recv[0] = jnp.ones((SLOTS, 8, SIDE), F32)

    @pl.when(jnp.logical_not(has_west))
    def _():
        init_recv[1] = jnp.ones((SLOTS, 8, SIDE), F32)

    init_each(lambda copy: copy.wait_recv(), True)

    def unpack_halo(row, carry):
        for side in range(2):
            col = cols + 1 if side == 0 else 0
            base = base_of(jnp.int32(0) + col, row)
            near = 0 if side == 0 else SIDE - 1
            live = alive(row, east_rows if side == 0 else west_rows)
            tile_t = jnp.transpose(init_recv[side, row])
            mu[pl.ds(base, SIDE), :] = (
                jnp.where(lane == near, spread(tile_t, 0), spread(tile_t, 1)) * live
            )
            fric[pl.ds(base, SIDE), :] = spread(tile_t, 2)
            b_u[pl.ds(base, SIDE), :] = spread(tile_t, 3) * live
            b_v[pl.ds(base, SIDE), :] = spread(tile_t, 4) * live
        return carry

    lax.fori_loop(0, prows, unpack_halo, 0)

    @pl.when(level < levels - 1)
    def _():
        first = jnp.where(level == 0, prows, 0)
        last = jnp.where(level == 0, 2 * prows, (cols + 2) * prows)
        lax.fori_loop(first, last, coefficients, 0)

    for lv in range(levels):

        @pl.when(level == lv)
        def _(lv=lv):
            program(lv, False)

    init_each(lambda copy: copy.wait_send(), False)


def per_device(levels, patches, forcing, velocity, viscosity, friction, patch_rows):
    tall = pltpu.VMEM((TALL, SIDE), F32)
    vmem = pl.BlockSpec(memory_space=pltpu.VMEM)
    coarse = {
        sender: pltpu.VMEM((2, 2**sender // 2, SLOTS // 2**sender * SIDE // 2, SIDE), F32)
        for sender in range(1, levels)
    }
    adjoint, gradient = pl.pallas_call(
        functools.partial(kernel, levels, patches),
        out_shape=(
            jax.ShapeDtypeStruct((SLOTS, 2, SIDE, SIDE), F32),
            jax.ShapeDtypeStruct((SLOTS, SIDE, SIDE), BF16),
        ),
        in_specs=[pl.BlockSpec(memory_space=pltpu.SMEM)]
        + [pl.BlockSpec(memory_space=pltpu.HBM)] * 4,
        out_specs=(vmem, vmem),
        scratch_shapes=[
            pltpu.VMEM((SLOTS, 2, SIDE, SIDE), BF16),
            pltpu.VMEM((SLOTS, 2, SIDE, SIDE), BF16),
            pltpu.VMEM((SLOTS, SIDE, SIDE), F32),
            pltpu.VMEM((SLOTS, SIDE, SIDE), BF16),
        ]
        + [tall] * 20
        + [
            pltpu.VMEM((2, SLOTS, 8, SIDE), F32),
            pltpu.VMEM((2, SLOTS, 8, SIDE), F32),
        ]
        + [coarse[sender] for sender in range(1, levels)] * 3
        + [pltpu.VMEM((4, 2, 8, SIDE), F32)] * 4
        + [
            pltpu.SemaphoreType.DMA((4,)),
            pltpu.SemaphoreType.DMA((4,)),
            pltpu.SemaphoreType.DMA((2, 16)),
            pltpu.SemaphoreType.DMA((2, 8)),
            pltpu.SemaphoreType.DMA((2, 32)),
            pltpu.SemaphoreType.DMA((2, 8)),
        ],
        compiler_params=pltpu.CompilerParams(
            collective_id=0, has_side_effects=True, vmem_limit_bytes=44 << 20
        ),
    )(
        patch_rows,
        *(
            pltpu.with_memory_space_constraint(x[0], pltpu.HBM)
            for x in (forcing, velocity, viscosity, friction)
        ),
    )
    return adjoint[None], gradient[None]


def solution(mesh):
    in_specs = (
        P("level", "patch", None, None, None),
        P("level", "patch", None, None, None),
        P("level", "patch", None, None),
        P("level", "patch", None, None),
        P(),
    )
    out_specs = (P("level", "patch", None, None, None), P("level", "patch", None, None))
    return jax.shard_map(
        functools.partial(per_device, mesh.shape["level"], mesh.shape["patch"]),
        mesh=mesh,
        in_specs=in_specs,
        out_specs=out_specs,
        check_vma=False,
    )
```

```python
import functools

import jax
import jax.numpy as jnp
from jax import lax
from jax.experimental import pallas as pl
from jax.experimental.pallas import tpu as pltpu
from jax.sharding import PartitionSpec as P

MESH = pl.DeviceIdType.MESH
F32 = jnp.float32
BF16 = jnp.bfloat16
SIDE = 128
SLOTS = 8
PAD = 8
TALL = 3 * (SLOTS * SIDE + 2 * PAD)


def split_dot(x, matrix):
    high = x.astype(BF16)
    low = (x - high.astype(F32)).astype(BF16)
    return jnp.dot(high, matrix, preferred_element_type=F32) + jnp.dot(
        low, matrix, preferred_element_type=F32
    )


START_ROWS = {
    0: {0: (256, 1024), 1: (72, 256), 2: (24, 72), 3: (0, 24)},
    1: {1: (128, 512), 2: (40, 128), 3: (0, 40)},
    2: {2: (64, 256), 3: (0, 64)},
    3: {3: (0, 128)},
}
RESIDUAL_ROWS = {
    1: {1: (144, 512), 2: (48, 144), 3: (0, 48)},
    2: {2: (80, 256), 3: (0, 80)},
    3: {3: (0, 128)},
}
SMOOTH_ROWS = {
    1: {1: (136, 512), 2: (56, 136), 3: (0, 56)},
    2: {2: (64, 256), 3: (0, 64)},
    3: {3: (0, 128)},
}
SENT_UP = {
    0: {1: (72, 256), 2: (24, 72), 3: (0, 24)},
    1: {2: (40, 128), 3: (0, 40)},
    2: {3: (0, 64)},
}
ORDER = {
    0: ("down0", "down1", "send1", "down2", "send2", "down3", "send3"),
    1: ("down1", "down2", "down3", "up2", "up3", "send3", "send2", "up1"),
    2: ("down2", "down3", "up3", "up2"),
}


def over(col_at, col_count, rows, most, body):
    low, high = rows
    pieces = -(-(high - low) // most)
    size = -(-(high - low) // (8 * pieces)) * 8

    def step(index, carry):
        col = index // pieces
        part = index - col * pieces
        start = low if pieces == 1 else jnp.minimum(low + part * size, high - size)
        body(col_at + col if isinstance(col_at, int) else col_at(col), start, size)
        return carry

    lax.fori_loop(0, col_count * pieces, step, 0)


def kernel(
    levels,
    patches,
    rows_hbm,
    forcing_hbm,
    velocity_hbm,
    viscosity_hbm,
    friction_hbm,
    out_ref,
    grad_ref,
    rows_ref,
    forcing,
    velocity,
    viscosity,
    friction,
    mu,
    fric,
    mu_e,
    mu_w,
    diag_u,
    diag_v,
    half_u,
    half_v,
    b_u,
    b_v,
    x_u,
    x_v,
    z_u,
    z_v,
    ue,
    uw,
    ve,
    vw,
    y_u,
    y_v,
    init_send,
    init_recv,
    down_send_1,
    down_send_2,
    down_send_3,
    down_recv_0,
    down_recv_1,
    down_recv_2,
    up_recv_1,
    up_recv_2,
    up_recv_3,
    down_edge_send,
    down_edge_recv,
    up_edge_send,
    up_edge_recv,
    side_edge_send,
    side_edge_recv,
    base_edge_send,
    base_edge_recv,
    load_sem,
    init_sem,
    down_sem,
    down_edge_sem,
    up_sem,
    up_edge_sem,
    side_edge_sem,
    base_edge_sem,
):
    down_send = {1: down_send_1, 2: down_send_2, 3: down_send_3}
    down_recv = {0: down_recv_0, 1: down_recv_1, 2: down_recv_2}
    up_recv = {1: up_recv_1, 2: up_recv_2, 3: up_recv_3}
    level = lax.axis_index("level")
    patch = lax.axis_index("patch")
    cols = jnp.where(level == 0, 1, jnp.where(level == 1, 2, jnp.where(level == 2, 4, 8)))
    prows = jnp.where(level == 0, 8, jnp.where(level == 1, 4, jnp.where(level == 2, 2, 1)))
    height = prows * SIDE
    pitch = height + 2 * PAD
    has_west = patch > 0
    has_east = patch < patches - 1
    finer = jnp.minimum(level + 1, levels - 1)
    west = jnp.maximum(patch - 1, 0)
    east = jnp.minimum(patch + 1, patches - 1)
    loads = [
        pltpu.make_async_copy(src, dst, load_sem.at[i])
        for i, (src, dst) in enumerate(
            (
                (viscosity_hbm, viscosity),
                (friction_hbm, friction),
                (forcing_hbm, forcing),
                (velocity_hbm, velocity),
                (rows_hbm, rows_ref),
            )
        )
    ]
    for load in loads:
        load.start()

    barrier = pltpu.get_barrier_semaphore()
    count = jnp.int32(0)
    for dl in (-1, 0, 1):
        for dp in (-1, 0, 1):
            if (dl == 0) == (dp == 0):
                continue
            there = (level + dl >= 0) & (level + dl < levels) & (patch + dp >= 0) & (patch + dp < patches)
            count = count + jnp.where(there, 1, 0)

            @pl.when(there)
            def _(dl=dl, dp=dp):
                pl.semaphore_signal(
                    barrier,
                    inc=1,
                    device_id={"level": level + dl, "patch": patch + dp},
                    device_id_type=MESH,
                )

    def base_of(col, row):
        return pl.multiple_of((col * pitch + PAD + row * SIDE).astype(jnp.int32), 8)

    def alive(row, total):
        return jnp.where(row < total, 1.0, 0.0).astype(F32)

    lane = lax.broadcasted_iota(jnp.int32, (SIDE, SIDE), 1)

    zeros = jnp.zeros((PAD, SIDE), F32)

    def clear(col, carry):
        first = pl.multiple_of(col * pitch, 8)
        last = pl.multiple_of(col * pitch + PAD + height, 8)
        for ref in (mu, x_u, x_v, z_u, z_v, ue, uw, ve, vw):
            ref[pl.ds(first, PAD), :] = zeros
            ref[pl.ds(last, PAD), :] = zeros
        return carry

    lax.fori_loop(0, cols + 2, clear, 0)

    loads[4].wait()
    own_rows = rows_ref[level, patch]
    west_rows = jnp.where(has_west, rows_ref[level, west], 0)
    east_rows = jnp.where(has_east, rows_ref[level, east], 0)
    fine_own = rows_ref[finer, patch]
    fine_west = jnp.where(has_west, rows_ref[finer, west], 0)
    fine_east = jnp.where(has_east, rows_ref[finer, east], 0)

    for load in loads[:3]:
        load.wait()

    def unpack(slot_id, carry):
        col = slot_id // prows
        row = slot_id - col * prows
        base = base_of(col + 1, row)
        slot = row * cols + col
        live = alive(row, own_rows)
        mu[pl.ds(base, SIDE), :] = viscosity[slot] * live
        fric[pl.ds(base, SIDE), :] = friction[slot].astype(F32)
        b_u[pl.ds(base, SIDE), :] = forcing[slot, 0].astype(F32) * live
        b_v[pl.ds(base, SIDE), :] = forcing[slot, 1].astype(F32) * live
        return carry

    lax.fori_loop(0, SLOTS, unpack, 0)

    def pack(row, carry):
        for side in range(2):
            base = base_of(jnp.where(side == 0, 1, cols), row)
            near, far = (0, 1) if side == 0 else (SIDE - 1, SIDE - 2)
            mu_t = jnp.transpose(mu[pl.ds(base, SIDE), :])
            fr_t = jnp.transpose(fric[pl.ds(base, SIDE), :])
            bu_t = jnp.transpose(b_u[pl.ds(base, SIDE), :])
            bv_t = jnp.transpose(b_v[pl.ds(base, SIDE), :])
            parts = [
                mu_t[near : near + 1],
                mu_t[far : far + 1],
                fr_t[near : near + 1],
                bu_t[near : near + 1],
                bv_t[near : near + 1],
                jnp.zeros((3, SIDE), F32),
            ]
            init_send[side, row] = jnp.concatenate(parts, axis=0)
        return carry

    lax.fori_loop(0, prows, pack, 0)

    pl.semaphore_wait(barrier, count)

    def copy_to(src, dst, send, recv, there, dp):
        return pltpu.make_async_remote_copy(
            src_ref=src,
            dst_ref=dst,
            send_sem=send,
            recv_sem=recv,
            device_id={"level": there, "patch": patch + dp},
            device_id_type=MESH,
        )

    def init_copies(lv, side):
        used = pl.ds(0, SLOTS // 2**lv)
        return copy_to(
            init_send.at[side, used],
            init_recv.at[side, used],
            init_sem.at[side],
            init_sem.at[2 + side],
            lv,
            -1 if side == 0 else 1,
        )

    def init_each(act, flip):
        for lv in range(levels):
            for side in range(2):
                there = has_west if (side == 0) != flip else has_east

                @pl.when((level == lv) & there)
                def _(lv=lv, side=side):
                    act(init_copies(lv, side))

    init_each(lambda copy: copy.start(), False)

    def spread(tile_t, index, first=0, count=SIDE):
        return jnp.broadcast_to(tile_t[first : first + count, index : index + 1], (count, SIDE))

    def coefficients(index, carry):
        col = index // prows
        row = index - col * prows
        base = base_of(col, row)
        to_east = pl.multiple_of(base + jnp.where(col == cols + 1, 0, pitch), 8)
        to_west = pl.multiple_of(base - jnp.where(col == 0, 0, pitch), 8)
        total = jnp.where(col == 0, west_rows, jnp.where(col == cols + 1, east_rows, own_rows))
        live = 0.5 * alive(row, total)
        here = mu[pl.ds(base, SIDE), :]
        m_e = pltpu.roll(jnp.where(lane == 0, mu[pl.ds(to_east, SIDE), :], here), SIDE - 1, 1)
        m_w = pltpu.roll(jnp.where(lane == SIDE - 1, mu[pl.ds(to_west, SIDE), :], here), 1, 1)
        across = m_e + m_w + 2.0 * here
        along = mu[pl.ds(base + 1, SIDE), :] + mu[pl.ds(base - 1, SIDE), :] + 2.0 * here
        fr = fric[pl.ds(base, SIDE), :]
        d_u = 2.0 * across + 0.5 * along + fr
        d_v = 2.0 * along + 0.5 * across + fr
        mu_e[pl.ds(base, SIDE), :] = m_e
        mu_w[pl.ds(base, SIDE), :] = m_w
        diag_u[pl.ds(base, SIDE), :] = d_u
        diag_v[pl.ds(base, SIDE), :] = d_v
        half_u[pl.ds(base, SIDE), :] = live / d_u
        half_v[pl.ds(base, SIDE), :] = live / d_v
        return carry

    quarter = SIDE // 2
    lane_row = lax.broadcasted_iota(jnp.int32, (SIDE, SIDE), 0)
    joins = [
        jnp.where(lane_row // 2 + half * quarter == lane, 1.0, 0.0).astype(BF16)
        for half in range(2)
    ]
    spreads = [
        jnp.where(lane // 2 + half * quarter == lane_row, 1.0, 0.0).astype(BF16)
        for half in range(2)
    ]

    def program(lv, early):
        columns = 2**lv
        tall = SLOTS // columns * SIDE
        step_col = tall + 2 * PAD
        pending = []

        def at_row(col, row):
            return pl.multiple_of(col * step_col + PAD + row, 8)

        def below(start, size, limit):
            rows = lax.broadcasted_iota(jnp.int32, (size, SIDE), 0) + start
            return rows < limit

        def shift(src_u, src_v, rows, first=1, count=columns):
            def body(col, start, size):
                base = at_row(col, start)
                to_east = pl.multiple_of(base + step_col, 8)
                to_west = pl.multiple_of(base - step_col, 8)
                here_lane = lane[:size]
                for src, dst_e, dst_w in ((src_u, ue, uw), (src_v, ve, vw)):
                    here = src[pl.ds(base, size), :]
                    dst_e[pl.ds(base, size), :] = pltpu.roll(
                        jnp.where(here_lane == 0, src[pl.ds(to_east, size), :], here), SIDE - 1, 1
                    )
                    dst_w[pl.ds(base, size), :] = pltpu.roll(
                        jnp.where(here_lane == SIDE - 1, src[pl.ds(to_west, size), :], here), 1, 1
                    )

            over(first, count, rows, SIDE, body)

        def residual_at(src_u, src_v, base, size):
            def at(ref, step=0):
                return ref[pl.ds(base + step, size), :]

            m, m_e, m_w, m_n, m_s = at(mu), at(mu_e), at(mu_w), at(mu, 1), at(mu, -1)
            p_e, p_w, p_n, p_s = m + m_e, m + m_w, m + m_n, m + m_s
            ue_n, ue_s, uw_n, uw_s = at(ue, 1), at(ue, -1), at(uw, 1), at(uw, -1)
            ve_n, ve_s, vw_n, vw_s = at(ve, 1), at(ve, -1), at(vw, 1), at(vw, -1)
            u, v = at(src_u), at(src_v)
            cross_u = 0.5 * (m_e * (ve_n - ve_s) - m_w * (vw_n - vw_s)) + 0.25 * (
                m_n * (ve_n - vw_n) - m_s * (ve_s - vw_s)
            )
            cross_v = 0.5 * (m_n * (ue_n - uw_n) - m_s * (ue_s - uw_s)) + 0.25 * (
                m_e * (ue_n - ue_s) - m_w * (uw_n - uw_s)
            )
            near_u = 2.0 * (p_e * at(ue) + p_w * at(uw)) + 0.5 * (
                p_n * at(src_u, 1) + p_s * at(src_u, -1)
            )
            near_v = 2.0 * (p_n * at(src_v, 1) + p_s * at(src_v, -1)) + 0.5 * (
                p_e * at(ve) + p_w * at(vw)
            )
            r_u = at(b_u) - (at(diag_u) * u - near_u - cross_u)
            r_v = at(b_v) - (at(diag_v) * v - near_v - cross_v)
            return u, v, r_u, r_v

        def sides():
            return ((0, has_west, has_east, -1), (1, has_east, has_west, 1))

        def down_copies(sender, tier, which=None):
            low, high = RESIDUAL_ROWS[sender][tier]
            low, high = low // 2, high // 2
            copies = []
            for k in range(2**sender // 2) if which is None else which:
                part = (slice(None), k, pl.ds(low, high - low))
                copies.append(
                    copy_to(
                        down_send[sender].at[part],
                        down_recv[sender - 1].at[part],
                        down_sem.at[0, tier * 4 + k],
                        down_sem.at[1, tier * 4 + k],
                        sender - 1,
                        0,
                    )
                )
            return copies

        def down_edge(sender, tier, side, dp):
            return copy_to(
                down_edge_send.at[tier, side],
                down_edge_recv.at[tier, side],
                down_edge_sem.at[0, tier * 2 + side],
                down_edge_sem.at[1, tier * 2 + side],
                sender - 1,
                dp,
            )

        def up_copies(sender, tier):
            low, high = SENT_UP[sender][tier]
            sources = (x_u, x_v) if sender == 0 else (y_u, y_v)
            pitch_here = SLOTS // 2**sender * SIDE + 2 * PAD
            copies = []
            for k in range(2**sender):
                for comp in range(2):
                    index = tier * 8 + k * 2 + comp
                    copies.append(
                        copy_to(
                            sources[comp].at[pl.ds((k + 1) * pitch_here + PAD + low, high - low)],
                            up_recv[sender + 1].at[comp, k, pl.ds(low, high - low)],
                            up_sem.at[0, index],
                            up_sem.at[1, index],
                            sender + 1,
                            0,
                        )
                    )
            return copies

        def up_edge(sender, tier, side, dp):
            return copy_to(
                up_edge_send.at[tier, side],
                up_edge_recv.at[tier, side],
                up_edge_sem.at[0, tier * 2 + side],
                up_edge_sem.at[1, tier * 2 + side],
                sender + 1,
                dp,
            )

        def side_edge(sender, tier, side, dp):
            return copy_to(
                side_edge_send.at[tier, side],
                side_edge_recv.at[tier, side],
                side_edge_sem.at[0, tier * 2 + side],
                side_edge_sem.at[1, tier * 2 + side],
                1,
                dp,
            )

        def base_edge(sender, tier, side, dp):
            return copy_to(
                base_edge_send.at[side],
                base_edge_recv.at[side],
                base_edge_sem.at[side],
                base_edge_sem.at[2 + side],
                1,
                dp,
            )

        def edges_of(refs, low, high):
            blocks = []
            for ref in refs:
                for part in range(2):
                    if part * SIDE < high and low < (part + 1) * SIDE:
                        blocks.append(jnp.transpose(ref(part * SIDE)))
            return [
                [block[near : near + 1] for block in blocks] for near in (0, SIDE - 1)
            ]

        def start_edges(make, sender, tier, which=(0, 1)):
            for side, there, _, dp in sides():
                if side not in which:
                    continue
                copy = make(sender, tier, side, dp)

                @pl.when(there)
                def _(copy=copy):
                    copy.start()

                pending.append((copy, there))

        def wait_edges(make, sender, tier, which=(0, 1)):
            for side, _, there, dp in sides():
                if side not in which:
                    continue
                copy = make(sender, tier, side, dp)

                @pl.when(there)
                def _(copy=copy):
                    copy.wait_recv()

        def fill_up_edges(tier, which=(0, 1)):
            low, high = SENT_UP[lv][tier]
            sources = (x_u, x_v) if lv == 0 else (y_u, y_v)
            for side in which:
                col = 1 if side == 0 else columns
                near = 0 if side == 0 else SIDE - 1
                parts = []
                for ref in sources:
                    for part in range(2):
                        if part * SIDE < high and low < (part + 1) * SIDE:
                            block_t = jnp.transpose(ref[pl.ds(at_row(col, part * SIDE), SIDE), :])
                            parts.append(block_t[near : near + 1])
                        else:
                            parts.append(jnp.zeros((1, SIDE), F32))
                parts.append(jnp.zeros((4, SIDE), F32))
                up_edge_send[tier, side] = jnp.concatenate(parts, axis=0)

        def send_up(tier):
            if lv > 0:
                fill_up_edges(tier)
                start_edges(up_edge, lv, tier)
            for copy in up_copies(lv, tier):
                copy.start()
                pending.append((copy, None))

        def start_body(col, start, size):
            where = pl.ds(at_row(col, start), size)
            x_u[where, :] = half_u[where, :] * b_u[where, :]
            x_v[where, :] = half_v[where, :] * b_v[where, :]

        def down(tier):
            rows = START_ROWS[lv][tier]
            low, high = rows
            if tier == lv:
                if lv == 0:
                    over(1, 1, rows, SIDE, start_body)
                else:
                    over(0, columns + 2, rows, SIDE, start_body)
            else:
                def halos():
                    wait_edges(down_edge, lv + 1, tier)
                    for side in range(2):
                        col = columns + 1 if side == 0 else 0
                        limit = quarter * (fine_east if side == 0 else fine_west)
                        tile_t = jnp.transpose(down_edge_recv[tier, side])
                        where = pl.ds(at_row(col, low), high - low)
                        keep = below(low, high - low, limit)
                        for comp, (ref, half, to) in enumerate(
                            ((b_u, half_u, x_u), (b_v, half_v, x_v))
                        ):
                            got = spread(tile_t, comp, low, high - low)
                            to[where, :] = half[where, :] * jnp.where(keep, got, ref[where, :])

                if lv == 2:
                    halos()
                for copy in down_copies(lv + 1, tier):
                    copy.wait_recv()

                def place_body(col, start, size):
                    where = pl.ds(at_row(col, start), size)
                    keep = below(start, size, quarter * fine_own)
                    for comp, (ref, half, to) in enumerate(
                        ((b_u, half_u, x_u), (b_v, half_v, x_v))
                    ):
                        got = down_recv[lv][comp, col - 1, pl.ds(start, size), :]
                        new = jnp.where(keep, got, ref[where, :])
                        ref[where, :] = new
                        to[where, :] = half[where, :] * new

                over(1, columns, rows, SIDE, place_body)
                if lv == 1:
                    halos()
            if lv == 0:
                return
            shift(x_u, x_v, rows)
            over(1, columns, RESIDUAL_ROWS[lv][tier], 64, residual_body)
            send_down(tier, range(columns // 2))

        def residual_body(col, start, size):
            base = at_row(col, start)
            _, _, r_u, r_v = residual_at(x_u, x_v, base, size)
            y_u[pl.ds(base, size), :] = r_u
            y_v[pl.ds(base, size), :] = r_v

        def send_down(tier, which):
            low, high = RESIDUAL_ROWS[lv][tier]
            low, high = low // 2, high // 2
            pairs = columns // 2
            def join_pair(k):
                def join_body(_, start, size):
                    for comp, ref in enumerate((y_u, y_v)):
                        total = None
                        for half in range(2):
                            base = at_row(2 * k + half + 1, 2 * start)
                            lines = (
                                ref[pl.ds(base, size, stride=2), :]
                                + ref[pl.ds(base + 1, size, stride=2), :]
                            )
                            term = split_dot(lines, joins[half])
                            total = term if total is None else total + term
                        down_send[lv][comp, k, pl.ds(start, size), :] = total

                over(0, 1, (low, high), 64, join_body)
            def start_pairs(ks):
                for copy in down_copies(lv, tier, ks):
                    copy.start()
                    pending.append((copy, None))

            outer = tuple(k for k in sorted({0, pairs - 1}) if k in which)
            for k in outer:
                join_pair(k)
            if lv == 1:
                start_pairs(outer)
                refs = [
                    lambda row, comp=comp: down_send[1][comp, 0, pl.ds(row, SIDE), :]
                    for comp in range(2)
                ]
                for side, lines in enumerate(edges_of(refs, low, high)):
                    if len(lines) == 2:
                        blank = jnp.zeros((1, SIDE), F32)
                        lines = [lines[0], blank, lines[1], blank]
                    lines = lines + [jnp.zeros((4, SIDE), F32)]
                    side_edge_send[tier, side] = jnp.concatenate(lines, axis=0)
                start_edges(side_edge, lv, tier)
            if lv > 1 and 0 in which:
                for side in range(2):
                    k = 0 if side == 0 else pairs - 1
                    near = 0 if side == 0 else SIDE - 1
                    lines = min(SIDE, tall // 2)
                    parts = []
                    for comp in range(2):
                        block_t = jnp.transpose(down_send[lv][comp, k, pl.ds(0, lines), :])
                        line = block_t[near : near + 1]
                        if lines < SIDE:
                            line = jnp.concatenate([line, line], axis=1)
                        parts.append(line)
                    parts.append(jnp.zeros((6, SIDE), F32))
                    down_edge_send[tier, side] = jnp.concatenate(parts, axis=0)
                start_edges(down_edge, lv, tier)
            if lv > 1:
                start_pairs(outer)
            for k in range(1, pairs - 1):
                if k in which:
                    join_pair(k)
                    start_pairs((k,))

        def up(tier):
            low, high = SENT_UP[lv - 1][tier]
            if lv == 1:
                halo_up(tier)
            for copy in up_copies(lv - 1, tier):
                copy.wait_recv()
            prolong(tier, 0, columns // 2)
            if lv > 1:
                halo_up(tier)
            shift(z_u, z_v, (2 * low, 2 * high))
            rows = SMOOTH_ROWS[lv][tier]
            if lv == 2 and tier == 3:
                copies = up_copies(lv, tier)
                for col in (1, 4, 2, 3):
                    over(col, 1, rows, 64, smooth_body)
                    if col == 4:
                        fill_up_edges(tier)
                        start_edges(up_edge, lv, tier)
                        continue
                    for copy in copies[2 * col - 2 : 2 * col]:
                        copy.start()
                for copy in copies[6:8]:
                    copy.start()
                pending.extend((copy, None) for copy in copies)
            else:
                over(1, columns, rows, 64, smooth_body)

        def smooth_body(col, start, size):
            base = at_row(col, start)
            where = pl.ds(base, size)
            u, v, r_u, r_v = residual_at(z_u, z_v, base, size)
            u = u + half_u[where, :] * r_u
            v = v + half_v[where, :] * r_v
            if lv < levels - 1:
                y_u[where, :] = u
                y_v[where, :] = v
                return
            slot = col - 1
            lines = pl.ds(start, size)
            live = alive(0, own_rows)
            out_ref[slot, 0, lines, :] = u
            out_ref[slot, 1, lines, :] = v
            product = (
                velocity[slot, 0, lines, :].astype(F32) * u
                + velocity[slot, 1, lines, :].astype(F32) * v
            )
            grad_ref[slot, lines, :] = (
                -(friction[slot, lines, :].astype(F32) * product) * live
            ).astype(BF16)

        def up_last():
            tier = levels - 1
            rows = (0, tall)
            copies = up_copies(lv - 1, tier)
            def columns_done(first, count):
                shift(z_u, z_v, rows, first, count)
                over(first, count, rows, 64, smooth_body)

            for k in range(4):
                for copy in copies[2 * k : 2 * k + 2]:
                    copy.wait_recv()
                prolong(tier, k, 1)
                if k in (1, 2):
                    columns_done(2 * k, 2)
                if k == 2:
                    halo_up(tier)
                    columns_done(1, 1)
            columns_done(6, 3)

        def halo_up(tier, which=(0, 1)):
            low, high = SENT_UP[lv - 1][tier]
            wait_edges(side_edge if lv == 1 else up_edge, lv - 1, tier, which)
            for side in which:
                col = columns + 1 if side == 0 else 0
                limit = quarter * (east_rows if side == 0 else west_rows)
                tile = (side_edge_recv if lv == 1 else up_edge_recv)[tier, side]
                if lv == 1:
                    spot = lax.broadcasted_iota(jnp.int32, (8, SIDE), 0) % 2 * SIDE + lane[:8]
                    known = base_edge_recv[side]
                    factor = jnp.concatenate([known[:4], known[:4]], axis=0)
                    plain = jnp.concatenate([known[4:], known[4:]], axis=0)
                    tile = factor * jnp.where(spot < limit, tile, plain)
                tile_t = jnp.transpose(tile)
                for part in range(2):
                    first, last = max(low, part * SIDE), min(high, (part + 1) * SIDE)
                    if first >= last:
                        continue
                    size = last - first
                    keep = below(first, size, limit)
                    for comp, (ref, to) in enumerate(((x_u, z_u), (x_v, z_v))):
                        wide = spread(tile_t, 2 * comp + part, first - part * SIDE, size)
                        wide = jnp.where(keep, wide, 0.0)
                        for step in range(2):
                            where = pl.ds(at_row(col, 2 * first) + step, size, stride=2)
                            to[where, :] = ref[where, :] + wide

        def prolong(tier, first, count):
            low, high = SENT_UP[lv - 1][tier]

            def prolong_body(k, start, size):
                keep = below(start, size, quarter * own_rows)
                for comp, (ref, to) in enumerate(((x_u, z_u), (x_v, z_v))):
                    coarse = up_recv[lv][comp, k, pl.ds(start, size), :]
                    coarse = jnp.where(keep, coarse, 0.0)
                    for half in range(2):
                        base = at_row(2 * k + half + 1, 2 * start)
                        wide = split_dot(coarse, spreads[half])
                        for step in range(2):
                            where = pl.ds(base + step, size, stride=2)
                            to[where, :] = ref[where, :] + wide

            over(first, count, (low, high), 64, prolong_body)

        if lv == levels - 1:
            if early:
                lax.fori_loop(1, columns + 1, coefficients, 0)
                over(1, columns, (0, tall), SIDE, start_body)
                shift(x_u, x_v, (0, tall), 2, columns - 2)
                over(3, columns - 4, (0, tall), 64, residual_body)
                send_down(lv, (1, 2))
                over(lambda i: 2 + 5 * i, 2, (0, tall), 64, residual_body)
                return
            ends = lambda i: jnp.where(i < 2, i, i + 6)
            inner = lambda i: 1 + 7 * i
            lax.fori_loop(0, 4, lambda i, carry: coefficients(ends(i), carry), 0)
            over(ends, 4, (0, tall), SIDE, start_body)
            shift(x_u, x_v, (0, tall), inner, 2)
            over(inner, 2, (0, tall), 64, residual_body)
            send_down(lv, (0, 3))
            pending.extend((copy, None) for copy in down_copies(lv, lv, (1, 2)))
            loads[3].wait()
            up_last()
        else:
            if lv == 0:
                refs = [
                    lambda row, ref=ref: ref[pl.ds(at_row(1, row), SIDE), :]
                    for ref in (half_u, half_v, b_u, b_v)
                ]
                for side, lines in enumerate(edges_of(refs, 0, 2 * SIDE)):
                    base_edge_send[side] = jnp.concatenate(lines, axis=0)
                start_edges(base_edge, lv, 0)
            for word in ORDER[lv]:
                if lv == 1 and word == "up2":
                    wait_edges(base_edge, 0, 0)
                {"down": down, "up": up, "send": send_up}[word[:-1]](int(word[-1]))
            loads[3].wait()

        finals = (x_u, x_v) if lv == 0 else (y_u, y_v)

        def finish(col, start, size):
            base = at_row(col, start)
            row = start // SIDE
            slot = row * columns + col - 1
            live = alive(row, own_rows)
            u = finals[0][pl.ds(base, size), :]
            v = finals[1][pl.ds(base, size), :]
            out_ref[slot, 0] = u
            out_ref[slot, 1] = v
            product = velocity[slot, 0].astype(F32) * u + velocity[slot, 1].astype(F32) * v
            grad_ref[slot] = (-(friction[slot].astype(F32) * product) * live).astype(BF16)

        if lv < levels - 1:
            over(1, columns, (0, tall), SIDE, finish)
        for copy, there in pending:
            if there is None:
                copy.wait_send()
            else:

                @pl.when(there)
                def _(copy=copy):
                    copy.wait_send()

    @pl.when(level == levels - 1)
    def _():
        program(levels - 1, True)

    @pl.when(jnp.logical_not(has_east))
    def _():
        init_recv[0] = jnp.ones((SLOTS, 8, SIDE), F32)

    @pl.when(jnp.logical_not(has_west))
    def _():
        init_recv[1] = jnp.ones((SLOTS, 8, SIDE), F32)

    init_each(lambda copy: copy.wait_recv(), True)

    def unpack_halo(row, carry):
        for side in range(2):
            col = cols + 1 if side == 0 else 0
            base = base_of(jnp.int32(0) + col, row)
            near = 0 if side == 0 else SIDE - 1
            live = alive(row, east_rows if side == 0 else west_rows)
            tile_t = jnp.transpose(init_recv[side, row])
            mu[pl.ds(base, SIDE), :] = (
                jnp.where(lane == near, spread(tile_t, 0), spread(tile_t, 1)) * live
            )
            fric[pl.ds(base, SIDE), :] = spread(tile_t, 2)
            b_u[pl.ds(base, SIDE), :] = spread(tile_t, 3) * live
            b_v[pl.ds(base, SIDE), :] = spread(tile_t, 4) * live
        return carry

    lax.fori_loop(0, prows, unpack_halo, 0)

    @pl.when(level < levels - 1)
    def _():
        first = jnp.where(level == 0, prows, 0)
        last = jnp.where(level == 0, 2 * prows, (cols + 2) * prows)
        lax.fori_loop(first, last, coefficients, 0)

    for lv in range(levels):

        @pl.when(level == lv)
        def _(lv=lv):
            program(lv, False)

    init_each(lambda copy: copy.wait_send(), False)


def write_out(adjoint, gradient, adjoint_hbm, gradient_hbm, sem):
    copies = [
        pltpu.make_async_copy(adjoint, adjoint_hbm, sem.at[0]),
        pltpu.make_async_copy(gradient, gradient_hbm, sem.at[1]),
    ]
    for copy in copies:
        copy.start()
    for copy in copies:
        copy.wait()


def per_device(levels, patches, forcing, velocity, viscosity, friction, patch_rows):
    tall = pltpu.VMEM((TALL, SIDE), F32)
    vmem = pl.BlockSpec(memory_space=pltpu.VMEM)
    coarse = {
        sender: pltpu.VMEM((2, 2**sender // 2, SLOTS // 2**sender * SIDE // 2, SIDE), F32)
        for sender in range(1, levels)
    }
    adjoint, gradient = pl.pallas_call(
        functools.partial(kernel, levels, patches),
        out_shape=(
            jax.ShapeDtypeStruct((SLOTS, 2, SIDE, SIDE), F32),
            jax.ShapeDtypeStruct((SLOTS, SIDE, SIDE), BF16),
        ),
        in_specs=[pl.BlockSpec(memory_space=pltpu.HBM)] * 5,
        out_specs=(vmem, vmem),
        scratch_shapes=[
            pltpu.SMEM((levels, patches), jnp.int32),
            pltpu.VMEM((SLOTS, 2, SIDE, SIDE), BF16),
            pltpu.VMEM((SLOTS, 2, SIDE, SIDE), BF16),
            pltpu.VMEM((SLOTS, SIDE, SIDE), F32),
            pltpu.VMEM((SLOTS, SIDE, SIDE), BF16),
        ]
        + [tall] * 20
        + [
            pltpu.VMEM((2, SLOTS, 8, SIDE), F32),
            pltpu.VMEM((2, SLOTS, 8, SIDE), F32),
        ]
        + [coarse[sender] for sender in range(1, levels)] * 3
        + [pltpu.VMEM((4, 2, 8, SIDE), F32)] * 6
        + [pltpu.VMEM((2, 8, SIDE), F32)] * 2
        + [
            pltpu.SemaphoreType.DMA((5,)),
            pltpu.SemaphoreType.DMA((4,)),
            pltpu.SemaphoreType.DMA((2, 16)),
            pltpu.SemaphoreType.DMA((2, 8)),
            pltpu.SemaphoreType.DMA((2, 32)),
            pltpu.SemaphoreType.DMA((2, 8)),
            pltpu.SemaphoreType.DMA((2, 8)),
            pltpu.SemaphoreType.DMA((4,)),
        ],
        compiler_params=pltpu.CompilerParams(
            collective_id=0, has_side_effects=True, vmem_limit_bytes=44 << 20
        ),
    )(
        *(
            pltpu.with_memory_space_constraint(x, pltpu.HBM)
            for x in (patch_rows, forcing[0], velocity[0], viscosity[0], friction[0])
        )
    )
    adjoint, gradient = pl.pallas_call(
        write_out,
        out_shape=(
            jax.ShapeDtypeStruct(adjoint.shape, adjoint.dtype),
            jax.ShapeDtypeStruct(gradient.shape, gradient.dtype),
        ),
        in_specs=[vmem, vmem],
        out_specs=(pl.BlockSpec(memory_space=pltpu.HBM),) * 2,
        scratch_shapes=[pltpu.SemaphoreType.DMA((2,))],
        compiler_params=pltpu.CompilerParams(vmem_limit_bytes=4 << 20),
    )(adjoint, gradient)
    return adjoint[None], gradient[None]


def solution(mesh):
    in_specs = (
        P("level", "patch", None, None, None),
        P("level", "patch", None, None, None),
        P("level", "patch", None, None),
        P("level", "patch", None, None),
        P(),
    )
    out_specs = (P("level", "patch", None, None, None), P("level", "patch", None, None))
    return jax.shard_map(
        functools.partial(per_device, mesh.shape["level"], mesh.shape["patch"]),
        mesh=mesh,
        in_specs=in_specs,
        out_specs=out_specs,
        check_vma=False,
    )
```

```python
import functools

import jax
import jax.numpy as jnp
from jax import lax
from jax.experimental import pallas as pl
from jax.experimental.pallas import tpu as pltpu
from jax.sharding import PartitionSpec as P

MESH = pl.DeviceIdType.MESH
F32 = jnp.float32
BF16 = jnp.bfloat16
SIDE = 128
SLOTS = 8
PAD = 8
TALL = 3 * (SLOTS * SIDE + 2 * PAD)


def split_dot(x, matrix):
    high = x.astype(BF16)
    low = (x - high.astype(F32)).astype(BF16)
    return jnp.dot(high, matrix, preferred_element_type=F32) + jnp.dot(
        low, matrix, preferred_element_type=F32
    )


START_ROWS = {
    0: {0: (256, 1024), 1: (72, 256), 2: (24, 72), 3: (0, 24)},
    1: {1: (128, 512), 2: (40, 128), 3: (0, 40)},
    2: {2: (64, 256), 3: (0, 64)},
    3: {3: (0, 128)},
}
RESIDUAL_ROWS = {
    1: {1: (144, 512), 2: (48, 144), 3: (0, 48)},
    2: {2: (80, 256), 3: (0, 80)},
    3: {3: (0, 128)},
}
SMOOTH_ROWS = {
    1: {1: (136, 512), 2: (56, 136), 3: (0, 56)},
    2: {2: (64, 256), 3: (0, 64)},
    3: {3: (0, 128)},
}
SENT_UP = {
    0: {1: (72, 256), 2: (24, 72), 3: (0, 24)},
    1: {2: (40, 128), 3: (0, 40)},
    2: {3: (0, 64)},
}
ORDER = {
    0: ("down0", "down1", "down2", "down3"),
    1: ("down1", "known0", "down2", "down3", "up2", "up3", "send3", "send2", "up1"),
    2: ("down2", "down3", "up3", "up2"),
}


def over(col_at, col_count, rows, most, body):
    low, high = rows
    pieces = -(-(high - low) // most)
    size = -(-(high - low) // (8 * pieces)) * 8

    def step(index, carry):
        col = index // pieces
        part = index - col * pieces
        start = low if pieces == 1 else jnp.minimum(low + part * size, high - size)
        body(col_at + col if isinstance(col_at, int) else col_at(col), start, size)
        return carry

    lax.fori_loop(0, col_count * pieces, step, 0)


def kernel(
    levels,
    patches,
    rows_hbm,
    forcing_hbm,
    velocity_hbm,
    viscosity_hbm,
    friction_hbm,
    out_ref,
    grad_ref,
    rows_ref,
    forcing,
    velocity,
    viscosity,
    friction,
    mu,
    fric,
    mu_e,
    mu_w,
    diag_u,
    diag_v,
    half_u,
    half_v,
    b_u,
    b_v,
    x_u,
    x_v,
    z_u,
    z_v,
    ue,
    uw,
    ve,
    vw,
    y_u,
    y_v,
    init_send,
    init_recv,
    down_send_1,
    down_send_2,
    down_send_3,
    down_recv_0,
    down_recv_1,
    down_recv_2,
    up_recv_1,
    up_recv_2,
    up_recv_3,
    down_edge_send,
    down_edge_recv,
    up_edge_send,
    up_edge_recv,
    halo_sum,
    known_halo,
    base_edge_send,
    base_edge_recv,
    load_sem,
    init_sem,
    down_sem,
    down_edge_sem,
    up_sem,
    up_edge_sem,
    base_edge_sem,
):
    down_send = {1: down_send_1, 2: down_send_2, 3: down_send_3}
    down_recv = {0: down_recv_0, 1: down_recv_1, 2: down_recv_2}
    up_recv = {1: up_recv_1, 2: up_recv_2, 3: up_recv_3}
    level = lax.axis_index("level")
    patch = lax.axis_index("patch")
    cols = jnp.where(level == 0, 1, jnp.where(level == 1, 2, jnp.where(level == 2, 4, 8)))
    prows = jnp.where(level == 0, 8, jnp.where(level == 1, 4, jnp.where(level == 2, 2, 1)))
    height = prows * SIDE
    pitch = height + 2 * PAD
    has_west = patch > 0
    has_east = patch < patches - 1
    finer = jnp.minimum(level + 1, levels - 1)
    west = jnp.maximum(patch - 1, 0)
    east = jnp.minimum(patch + 1, patches - 1)
    loads = [
        pltpu.make_async_copy(src, dst, load_sem.at[i])
        for i, (src, dst) in enumerate(
            (
                (viscosity_hbm, viscosity),
                (friction_hbm, friction),
                (forcing_hbm, forcing),
                (velocity_hbm, velocity),
                (rows_hbm, rows_ref),
            )
        )
    ]
    for load in loads:
        load.start()

    barrier = pltpu.get_barrier_semaphore()
    count = jnp.int32(0)
    for dl in (-1, 0, 1):
        for dp in (-1, 0, 1):
            if (dl == 0) == (dp == 0):
                continue
            there = (level + dl >= 0) & (level + dl < levels) & (patch + dp >= 0) & (patch + dp < patches)
            count = count + jnp.where(there, 1, 0)

            @pl.when(there)
            def _(dl=dl, dp=dp):
                pl.semaphore_signal(
                    barrier,
                    inc=1,
                    device_id={"level": level + dl, "patch": patch + dp},
                    device_id_type=MESH,
                )

    def base_of(col, row):
        return pl.multiple_of((col * pitch + PAD + row * SIDE).astype(jnp.int32), 8)

    def alive(row, total):
        return jnp.where(row < total, 1.0, 0.0).astype(F32)

    lane = lax.broadcasted_iota(jnp.int32, (SIDE, SIDE), 1)

    zeros = jnp.zeros((PAD, SIDE), F32)

    def clear(col, carry):
        first = pl.multiple_of(col * pitch, 8)
        last = pl.multiple_of(col * pitch + PAD + height, 8)
        for ref in (mu, x_u, x_v, z_u, z_v, ue, uw, ve, vw):
            ref[pl.ds(first, PAD), :] = zeros
            ref[pl.ds(last, PAD), :] = zeros
        return carry

    lax.fori_loop(0, cols + 2, clear, 0)

    loads[4].wait()
    own_rows = rows_ref[level, patch]
    west_rows = jnp.where(has_west, rows_ref[level, west], 0)
    east_rows = jnp.where(has_east, rows_ref[level, east], 0)
    fine_own = rows_ref[finer, patch]
    fine_west = jnp.where(has_west, rows_ref[finer, west], 0)
    fine_east = jnp.where(has_east, rows_ref[finer, east], 0)

    for load in loads[:3]:
        load.wait()

    def unpack(slot_id, carry):
        col = slot_id // prows
        row = slot_id - col * prows
        base = base_of(col + 1, row)
        slot = row * cols + col
        live = alive(row, own_rows)
        mu[pl.ds(base, SIDE), :] = viscosity[slot] * live
        fric[pl.ds(base, SIDE), :] = friction[slot].astype(F32)
        b_u[pl.ds(base, SIDE), :] = forcing[slot, 0].astype(F32) * live
        b_v[pl.ds(base, SIDE), :] = forcing[slot, 1].astype(F32) * live
        return carry

    lax.fori_loop(0, SLOTS, unpack, 0)

    def pack(row, carry):
        for side in range(2):
            base = base_of(jnp.where(side == 0, 1, cols), row)
            four = slice(0, 4) if side == 0 else slice(SIDE - 4, SIDE)
            three = slice(0, 3) if side == 0 else slice(SIDE - 3, SIDE)
            mu_t = jnp.transpose(mu[pl.ds(base, SIDE), :])
            fr_t = jnp.transpose(fric[pl.ds(base, SIDE), :])
            bu_t = jnp.transpose(b_u[pl.ds(base, SIDE), :])
            bv_t = jnp.transpose(b_v[pl.ds(base, SIDE), :])
            parts = [
                mu_t[four],
                fr_t[three],
                bu_t[three],
                bv_t[three],
                jnp.zeros((3, SIDE), F32),
            ]
            init_send[side, row] = jnp.concatenate(parts, axis=0)
        return carry

    lax.fori_loop(0, prows, pack, 0)

    pl.semaphore_wait(barrier, count)

    def copy_to(src, dst, send, recv, there, dp):
        return pltpu.make_async_remote_copy(
            src_ref=src,
            dst_ref=dst,
            send_sem=send,
            recv_sem=recv,
            device_id={"level": there, "patch": patch + dp},
            device_id_type=MESH,
        )

    def init_copies(lv, side):
        used = pl.ds(0, SLOTS // 2**lv)
        return copy_to(
            init_send.at[side, used],
            init_recv.at[side, used],
            init_sem.at[side],
            init_sem.at[2 + side],
            lv,
            -1 if side == 0 else 1,
        )

    def init_each(act, flip):
        for lv in range(levels):
            for side in range(2):
                there = has_west if (side == 0) != flip else has_east

                @pl.when((level == lv) & there)
                def _(lv=lv, side=side):
                    act(init_copies(lv, side))

    init_each(lambda copy: copy.start(), False)

    def columns_of(tile):
        blank = jnp.zeros((SIDE - tile.shape[0], SIDE), F32)
        return jnp.transpose(jnp.concatenate([tile, blank], axis=0))

    def lanes_from(tile_t, side, first, width):
        steps = (-first if side == 0 else SIDE - width - first) % SIDE
        return tile_t if steps == 0 else pltpu.roll(tile_t, steps, 1)

    def spread(tile_t, index, first=0, count=SIDE):
        return jnp.broadcast_to(tile_t[first : first + count, index : index + 1], (count, SIDE))

    def coefficients(index, carry):
        col = index // prows
        row = index - col * prows
        base = base_of(col, row)
        to_east = pl.multiple_of(base + jnp.where(col == cols + 1, 0, pitch), 8)
        to_west = pl.multiple_of(base - jnp.where(col == 0, 0, pitch), 8)
        total = jnp.where(col == 0, west_rows, jnp.where(col == cols + 1, east_rows, own_rows))
        live = 0.5 * alive(row, total)
        here = mu[pl.ds(base, SIDE), :]
        m_e = pltpu.roll(jnp.where(lane == 0, mu[pl.ds(to_east, SIDE), :], here), SIDE - 1, 1)
        m_w = pltpu.roll(jnp.where(lane == SIDE - 1, mu[pl.ds(to_west, SIDE), :], here), 1, 1)
        across = m_e + m_w + 2.0 * here
        along = mu[pl.ds(base + 1, SIDE), :] + mu[pl.ds(base - 1, SIDE), :] + 2.0 * here
        fr = fric[pl.ds(base, SIDE), :]
        d_u = 2.0 * across + 0.5 * along + fr
        d_v = 2.0 * along + 0.5 * across + fr
        mu_e[pl.ds(base, SIDE), :] = m_e
        mu_w[pl.ds(base, SIDE), :] = m_w
        diag_u[pl.ds(base, SIDE), :] = d_u
        diag_v[pl.ds(base, SIDE), :] = d_v
        half_u[pl.ds(base, SIDE), :] = live / d_u
        half_v[pl.ds(base, SIDE), :] = live / d_v
        return carry

    quarter = SIDE // 2
    lane_row = lax.broadcasted_iota(jnp.int32, (SIDE, SIDE), 0)
    joins = [
        jnp.where(lane_row // 2 + half * quarter == lane, 1.0, 0.0).astype(BF16)
        for half in range(2)
    ]
    spreads = [
        jnp.where(lane // 2 + half * quarter == lane_row, 1.0, 0.0).astype(BF16)
        for half in range(2)
    ]

    def program(lv, early):
        columns = 2**lv
        tall = SLOTS // columns * SIDE
        step_col = tall + 2 * PAD
        pending = []

        def at_row(col, row):
            return pl.multiple_of(col * step_col + PAD + row, 8)

        def below(start, size, limit):
            rows = lax.broadcasted_iota(jnp.int32, (size, SIDE), 0) + start
            return rows < limit

        def shift(src_u, src_v, rows, first=1, count=columns):
            def body(col, start, size):
                base = at_row(col, start)
                to_east = pl.multiple_of(base + jnp.where(col == columns + 1, 0, step_col), 8)
                to_west = pl.multiple_of(base - jnp.where(col == 0, 0, step_col), 8)
                here_lane = lane[:size]
                for src, dst_e, dst_w in ((src_u, ue, uw), (src_v, ve, vw)):
                    here = src[pl.ds(base, size), :]
                    dst_e[pl.ds(base, size), :] = pltpu.roll(
                        jnp.where(here_lane == 0, src[pl.ds(to_east, size), :], here), SIDE - 1, 1
                    )
                    dst_w[pl.ds(base, size), :] = pltpu.roll(
                        jnp.where(here_lane == SIDE - 1, src[pl.ds(to_west, size), :], here), 1, 1
                    )

            over(first, count, rows, SIDE, body)

        def residual_at(src_u, src_v, base, size):
            def at(ref, step=0):
                return ref[pl.ds(base + step, size), :]

            m, m_e, m_w, m_n, m_s = at(mu), at(mu_e), at(mu_w), at(mu, 1), at(mu, -1)
            p_e, p_w, p_n, p_s = m + m_e, m + m_w, m + m_n, m + m_s
            ue_n, ue_s, uw_n, uw_s = at(ue, 1), at(ue, -1), at(uw, 1), at(uw, -1)
            ve_n, ve_s, vw_n, vw_s = at(ve, 1), at(ve, -1), at(vw, 1), at(vw, -1)
            u, v = at(src_u), at(src_v)
            cross_u = 0.5 * (m_e * (ve_n - ve_s) - m_w * (vw_n - vw_s)) + 0.25 * (
                m_n * (ve_n - vw_n) - m_s * (ve_s - vw_s)
            )
            cross_v = 0.5 * (m_n * (ue_n - uw_n) - m_s * (ue_s - uw_s)) + 0.25 * (
                m_e * (ue_n - ue_s) - m_w * (uw_n - uw_s)
            )
            near_u = 2.0 * (p_e * at(ue) + p_w * at(uw)) + 0.5 * (
                p_n * at(src_u, 1) + p_s * at(src_u, -1)
            )
            near_v = 2.0 * (p_n * at(src_v, 1) + p_s * at(src_v, -1)) + 0.5 * (
                p_e * at(ve) + p_w * at(vw)
            )
            r_u = at(b_u) - (at(diag_u) * u - near_u - cross_u)
            r_v = at(b_v) - (at(diag_v) * v - near_v - cross_v)
            return u, v, r_u, r_v

        def sides():
            return ((0, has_west, has_east, -1), (1, has_east, has_west, 1))

        def down_copies(sender, tier, which=None):
            low, high = RESIDUAL_ROWS[sender][tier]
            low, high = low // 2, high // 2
            copies = []
            for k in range(2**sender // 2) if which is None else which:
                part = (slice(None), k, pl.ds(low, high - low))
                copies.append(
                    copy_to(
                        down_send[sender].at[part],
                        down_recv[sender - 1].at[part],
                        down_sem.at[0, tier * 4 + k],
                        down_sem.at[1, tier * 4 + k],
                        sender - 1,
                        0,
                    )
                )
            return copies

        def down_edge(sender, tier, side, dp):
            return copy_to(
                down_edge_send.at[tier, side],
                down_edge_recv.at[tier, side],
                down_edge_sem.at[0, tier * 2 + side],
                down_edge_sem.at[1, tier * 2 + side],
                sender - 1,
                dp,
            )

        def up_copies(sender, tier):
            low, high = SENT_UP[sender][tier]
            sources = (x_u, x_v) if sender == 0 else (y_u, y_v)
            pitch_here = SLOTS // 2**sender * SIDE + 2 * PAD
            copies = []
            for k in range(2**sender):
                for comp in range(2):
                    index = tier * 8 + k * 2 + comp
                    copies.append(
                        copy_to(
                            sources[comp].at[pl.ds((k + 1) * pitch_here + PAD + low, high - low)],
                            up_recv[sender + 1].at[comp, k, pl.ds(low, high - low)],
                            up_sem.at[0, index],
                            up_sem.at[1, index],
                            sender + 1,
                            0,
                        )
                    )
            return copies

        def up_edge(sender, tier, side, dp):
            return copy_to(
                up_edge_send.at[tier, side],
                up_edge_recv.at[tier, side],
                up_edge_sem.at[0, tier * 2 + side],
                up_edge_sem.at[1, tier * 2 + side],
                sender + 1,
                dp,
            )

        def known_copies():
            rows = 2 * SIDE
            return [
                copy_to(
                    ref.at[pl.ds(SLOTS * SIDE + 2 * PAD + PAD, rows)],
                    up_recv[1].at[comp, 0, pl.ds(0, rows)],
                    up_sem.at[0, comp],
                    up_sem.at[1, comp],
                    1,
                    0,
                )
                for comp, ref in enumerate((half_u, half_v))
            ]

        def known():
            wait_edges(base_edge, 0, 0)
            tiles = [jnp.transpose(base_edge_recv[side]) for side in range(2)]
            for comp in range(2):
                for part in range(2):
                    index = 2 * comp + part
                    known_halo[comp, pl.ds(part * SIDE, SIDE), :] = jnp.where(
                        lane < quarter, spread(tiles[0], index), spread(tiles[1], index)
                    )
            for copy in known_copies():
                copy.wait_recv()

        def base_edge(sender, tier, side, dp):
            return copy_to(
                base_edge_send.at[side],
                base_edge_recv.at[side],
                base_edge_sem.at[side],
                base_edge_sem.at[2 + side],
                1,
                dp,
            )

        def edges_of(refs, low, high):
            blocks = []
            for ref in refs:
                for part in range(2):
                    if part * SIDE < high and low < (part + 1) * SIDE:
                        rows = pl.ds(at_row(1, part * SIDE), SIDE)
                        blocks.append(jnp.transpose(ref[rows, :]))
            return [
                [block[near : near + 1] for block in blocks] for near in (0, SIDE - 1)
            ]

        def start_edges(make, sender, tier, which=(0, 1)):
            for side, there, _, dp in sides():
                if side not in which:
                    continue
                copy = make(sender, tier, side, dp)

                @pl.when(there)
                def _(copy=copy):
                    copy.start()

                pending.append((copy, there))

        def wait_edges(make, sender, tier, which=(0, 1)):
            for side, _, there, dp in sides():
                if side not in which:
                    continue
                copy = make(sender, tier, side, dp)

                @pl.when(there)
                def _(copy=copy):
                    copy.wait_recv()

        def fill_up_edges(tier, which=(0, 1)):
            low, high = SENT_UP[lv][tier]
            sources = (x_u, x_v) if lv == 0 else (y_u, y_v)
            for side in which:
                col = 1 if side == 0 else columns
                near = 0 if side == 0 else SIDE - 1
                parts = []
                for ref in sources:
                    for part in range(2):
                        if part * SIDE < high and low < (part + 1) * SIDE:
                            block_t = jnp.transpose(ref[pl.ds(at_row(col, part * SIDE), SIDE), :])
                            parts.append(block_t[near : near + 1])
                        else:
                            parts.append(jnp.zeros((1, SIDE), F32))
                parts.append(jnp.zeros((4, SIDE), F32))
                up_edge_send[tier, side] = jnp.concatenate(parts, axis=0)

        def send_up(tier):
            fill_up_edges(tier)
            start_edges(up_edge, lv, tier)
            for copy in up_copies(lv, tier):
                copy.start()
                pending.append((copy, None))

        def start_body(col, start, size):
            where = pl.ds(at_row(col, start), size)
            x_u[where, :] = half_u[where, :] * b_u[where, :]
            x_v[where, :] = half_v[where, :] * b_v[where, :]

        def down(tier):
            rows = START_ROWS[lv][tier]
            low, high = rows
            if tier == lv:
                if lv == 0:
                    over(1, 1, rows, SIDE, start_body)
                else:
                    over(0, columns + 2, rows, SIDE, start_body)
            else:
                def halos():
                    wait_edges(down_edge, lv + 1, tier)
                    for side in range(2):
                        col = columns + 1 if side == 0 else 0
                        limit = quarter * (fine_east if side == 0 else fine_west)
                        tile_t = columns_of(down_edge_recv[tier, side])[low:high]
                        where = pl.ds(at_row(col, low), high - low)
                        keep = below(low, high - low, limit)
                        for comp, (ref, half, to) in enumerate(
                            ((b_u, half_u, x_u), (b_v, half_v, x_v))
                        ):
                            got = lanes_from(tile_t, side, 3 * comp, 3)
                            new = jnp.where(keep, got, ref[where, :])
                            ref[where, :] = new
                            to[where, :] = half[where, :] * new

                if lv == 2:
                    halos()
                for copy in down_copies(lv + 1, tier):
                    copy.wait_recv()

                def place_body(col, start, size):
                    where = pl.ds(at_row(col, start), size)
                    keep = below(start, size, quarter * fine_own)
                    for comp, (ref, half, to) in enumerate(
                        ((b_u, half_u, x_u), (b_v, half_v, x_v))
                    ):
                        got = down_recv[lv][comp, col - 1, pl.ds(start, size), :]
                        new = jnp.where(keep, got, ref[where, :])
                        ref[where, :] = new
                        to[where, :] = half[where, :] * new

                over(1, columns, rows, SIDE, place_body)
                if lv == 1:
                    halos()
            if lv == 0:
                return
            first, count = (0, columns + 2) if lv == 1 else (1, columns)
            shift(x_u, x_v, rows, first, count)
            over(first, count, RESIDUAL_ROWS[lv][tier], 64, residual_body)
            send_down(tier, range(columns // 2))

        def residual_body(col, start, size):
            base = at_row(col, start)
            _, _, r_u, r_v = residual_at(x_u, x_v, base, size)
            y_u[pl.ds(base, size), :] = r_u
            y_v[pl.ds(base, size), :] = r_v

        def send_down(tier, which):
            low, high = RESIDUAL_ROWS[lv][tier]
            low, high = low // 2, high // 2
            pairs = columns // 2
            def join_halo(low, high):
                join_pair(0, (columns + 1, 0), halo_sum)

            def join_pair(k, pair=None, to=None):
                pair = (2 * k + 1, 2 * k + 2) if pair is None else pair
                to = down_send[lv].at[:, k] if to is None else to

                def join_body(_, start, size):
                    for comp, ref in enumerate((y_u, y_v)):
                        total = None
                        for half in range(2):
                            base = at_row(pair[half], 2 * start)
                            lines = (
                                ref[pl.ds(base, size, stride=2), :]
                                + ref[pl.ds(base + 1, size, stride=2), :]
                            )
                            term = split_dot(lines, joins[half])
                            total = term if total is None else total + term
                        to[comp, pl.ds(start, size), :] = total

                over(0, 1, (low, high), 64, join_body)
            def start_pairs(ks):
                for copy in down_copies(lv, tier, ks):
                    copy.start()
                    pending.append((copy, None))

            outer = tuple(k for k in sorted({0, pairs - 1}) if k in which)
            for k in outer:
                join_pair(k)
            if lv == 1:
                start_pairs(outer)
                join_halo(low, high)
            if lv > 1 and 0 in which:
                for side in range(2):
                    k = 0 if side == 0 else pairs - 1
                    three = slice(0, 3) if side == 0 else slice(SIDE - 3, SIDE)
                    lines = min(SIDE, tall // 2)
                    parts = []
                    for comp in range(2):
                        block_t = jnp.transpose(down_send[lv][comp, k, pl.ds(0, lines), :])
                        line = block_t[three]
                        if lines < SIDE:
                            line = jnp.concatenate([line, line], axis=1)
                        parts.append(line)
                    parts.append(jnp.zeros((2, SIDE), F32))
                    down_edge_send[tier, side] = jnp.concatenate(parts, axis=0)
                start_edges(down_edge, lv, tier)
            if lv > 1:
                start_pairs(outer)
            for k in range(1, pairs - 1):
                if k in which:
                    join_pair(k)
                    start_pairs((k,))

        def up(tier):
            low, high = SENT_UP[lv - 1][tier]
            if lv == 1:
                halo_up(tier)
            if lv > 1:
                for copy in up_copies(lv - 1, tier):
                    copy.wait_recv()
            prolong(tier, 0, columns // 2)
            if lv > 1:
                halo_up(tier)
            shift(z_u, z_v, (2 * low, 2 * high))
            rows = SMOOTH_ROWS[lv][tier]
            if lv == 2 and tier == 3:
                copies = up_copies(lv, tier)
                for col in (1, 4, 2, 3):
                    over(col, 1, rows, 64, smooth_body)
                    if col == 4:
                        fill_up_edges(tier)
                        start_edges(up_edge, lv, tier)
                        continue
                    for copy in copies[2 * col - 2 : 2 * col]:
                        copy.start()
                for copy in copies[6:8]:
                    copy.start()
                pending.extend((copy, None) for copy in copies)
            else:
                over(1, columns, rows, 64, smooth_body)

        def smooth_body(col, start, size):
            base = at_row(col, start)
            where = pl.ds(base, size)
            u, v, r_u, r_v = residual_at(z_u, z_v, base, size)
            u = u + half_u[where, :] * r_u
            v = v + half_v[where, :] * r_v
            if lv < levels - 1:
                y_u[where, :] = u
                y_v[where, :] = v
                return
            slot = col - 1
            lines = pl.ds(start, size)
            live = alive(0, own_rows)
            out_ref[slot, 0, lines, :] = u
            out_ref[slot, 1, lines, :] = v
            product = (
                velocity[slot, 0, lines, :].astype(F32) * u
                + velocity[slot, 1, lines, :].astype(F32) * v
            )
            grad_ref[slot, lines, :] = (
                -(friction[slot, lines, :].astype(F32) * product) * live
            ).astype(BF16)

        def up_last():
            tier = levels - 1
            rows = (0, tall)
            copies = up_copies(lv - 1, tier)
            def columns_done(first, count):
                shift(z_u, z_v, rows, first, count)
                over(first, count, rows, 64, smooth_body)

            for k in range(4):
                for copy in copies[2 * k : 2 * k + 2]:
                    copy.wait_recv()
                prolong(tier, k, 1)
                if k in (1, 2):
                    columns_done(2 * k, 2)
                if k == 2:
                    halo_up(tier)
                    columns_done(1, 1)
            columns_done(6, 3)

        def halo_up(tier, which=(0, 1)):
            low, high = SENT_UP[lv - 1][tier]
            if lv == 1:
                def halo_body(_, start, size):
                    limit = quarter * jnp.where(lane[:size] < quarter, east_rows, west_rows)
                    keep = lax.broadcasted_iota(jnp.int32, (size, SIDE), 0) + start < limit
                    for comp, (ref, to) in enumerate(((x_u, z_u), (x_v, z_v))):
                        lines = pl.ds(start, size)
                        wide = known_halo[comp, lines, :] * halo_sum[comp, lines, :]
                        wide = jnp.where(keep, wide, 0.0)
                        for col in (0, columns + 1):
                            for step in range(2):
                                where = pl.ds(at_row(col, 2 * start) + step, size, stride=2)
                                to[where, :] = ref[where, :] + wide

                over(0, 1, (low, high), 64, halo_body)
                return
            wait_edges(up_edge, lv - 1, tier, which)
            for side in which:
                col = columns + 1 if side == 0 else 0
                limit = quarter * (east_rows if side == 0 else west_rows)
                tile_t = jnp.transpose(up_edge_recv[tier, side])
                for part in range(2):
                    first, last = max(low, part * SIDE), min(high, (part + 1) * SIDE)
                    if first >= last:
                        continue
                    size = last - first
                    keep = below(first, size, limit)
                    for comp, (ref, to) in enumerate(((x_u, z_u), (x_v, z_v))):
                        wide = spread(tile_t, 2 * comp + part, first - part * SIDE, size)
                        wide = jnp.where(keep, wide, 0.0)
                        for step in range(2):
                            where = pl.ds(at_row(col, 2 * first) + step, size, stride=2)
                            to[where, :] = ref[where, :] + wide

        def prolong(tier, first, count):
            low, high = SENT_UP[lv - 1][tier]

            def prolong_body(k, start, size):
                keep = below(start, size, quarter * own_rows)
                for comp, (ref, to) in enumerate(((x_u, z_u), (x_v, z_v))):
                    coarse = up_recv[lv][comp, k, pl.ds(start, size), :]
                    if lv == 1:
                        coarse = coarse * down_send[1][comp, k, pl.ds(start, size), :]
                    coarse = jnp.where(keep, coarse, 0.0)
                    for half in range(2):
                        base = at_row(2 * k + half + 1, 2 * start)
                        wide = split_dot(coarse, spreads[half])
                        for step in range(2):
                            where = pl.ds(base + step, size, stride=2)
                            to[where, :] = ref[where, :] + wide

            over(first, count, (low, high), 64, prolong_body)

        if lv == levels - 1:
            if early:
                lax.fori_loop(1, columns + 1, coefficients, 0)
                over(1, columns, (0, tall), SIDE, start_body)
                shift(x_u, x_v, (0, tall), 2, columns - 2)
                over(3, columns - 4, (0, tall), 64, residual_body)
                send_down(lv, (1, 2))
                over(lambda i: 2 + 5 * i, 2, (0, tall), 64, residual_body)
                return
            ends = lambda i: jnp.where(i < 2, i, i + 6)
            inner = lambda i: 1 + 7 * i
            lax.fori_loop(0, 4, lambda i, carry: coefficients(ends(i), carry), 0)
            over(ends, 4, (0, tall), SIDE, start_body)
            shift(x_u, x_v, (0, tall), inner, 2)
            over(inner, 2, (0, tall), 64, residual_body)
            send_down(lv, (0, 3))
            pending.extend((copy, None) for copy in down_copies(lv, lv, (1, 2)))
            loads[3].wait()
            up_last()
        else:
            if lv == 0:
                for copy in known_copies():
                    copy.start()
                    pending.append((copy, None))
                for side, lines in enumerate(edges_of((half_u, half_v), 0, 2 * SIDE)):
                    lines.append(jnp.zeros((4, SIDE), F32))
                    base_edge_send[side] = jnp.concatenate(lines, axis=0)
                start_edges(base_edge, lv, 0)
            for word in ORDER[lv]:
                if word == "known0":
                    known()
                    continue
                {"down": down, "up": up, "send": send_up}[word[:-1]](int(word[-1]))
            loads[3].wait()

        finals = (x_u, x_v) if lv == 0 else (y_u, y_v)

        def finish(col, start, size):
            base = at_row(col, start)
            row = start // SIDE
            slot = row * columns + col - 1
            live = alive(row, own_rows)
            u = finals[0][pl.ds(base, size), :]
            v = finals[1][pl.ds(base, size), :]
            out_ref[slot, 0] = u
            out_ref[slot, 1] = v
            product = velocity[slot, 0].astype(F32) * u + velocity[slot, 1].astype(F32) * v
            grad_ref[slot] = (-(friction[slot].astype(F32) * product) * live).astype(BF16)

        if lv < levels - 1:
            over(1, columns, (0, tall), SIDE, finish)
        for copy, there in pending:
            if there is None:
                copy.wait_send()
            else:

                @pl.when(there)
                def _(copy=copy):
                    copy.wait_send()

    @pl.when(level == levels - 1)
    def _():
        program(levels - 1, True)

    @pl.when(jnp.logical_not(has_east))
    def _():
        init_recv[0] = jnp.ones((SLOTS, 16, SIDE), F32)

    @pl.when(jnp.logical_not(has_west))
    def _():
        init_recv[1] = jnp.ones((SLOTS, 16, SIDE), F32)

    init_each(lambda copy: copy.wait_recv(), True)

    def unpack_halo(row, carry):
        for side in range(2):
            col = cols + 1 if side == 0 else 0
            base = base_of(jnp.int32(0) + col, row)
            live = alive(row, east_rows if side == 0 else west_rows)
            tile_t = columns_of(init_recv[side, row])

            def place(first, width, other):
                valid = lane < width if side == 0 else lane >= SIDE - width
                return jnp.where(valid, lanes_from(tile_t, side, first, width), other)

            mu[pl.ds(base, SIDE), :] = place(0, 4, 0.0) * live
            fric[pl.ds(base, SIDE), :] = place(4, 3, 1.0)
            b_u[pl.ds(base, SIDE), :] = place(7, 3, 0.0) * live
            b_v[pl.ds(base, SIDE), :] = place(10, 3, 0.0) * live
        return carry

    lax.fori_loop(0, prows, unpack_halo, 0)

    @pl.when(level < levels - 1)
    def _():
        first = jnp.where(level == 0, prows, 0)
        last = jnp.where(level == 0, 2 * prows, (cols + 2) * prows)
        lax.fori_loop(first, last, coefficients, 0)

    for lv in range(levels):

        @pl.when(level == lv)
        def _(lv=lv):
            program(lv, False)

    init_each(lambda copy: copy.wait_send(), False)


def write_out(adjoint, gradient, adjoint_hbm, gradient_hbm, sem):
    copies = [
        pltpu.make_async_copy(adjoint, adjoint_hbm, sem.at[0]),
        pltpu.make_async_copy(gradient, gradient_hbm, sem.at[1]),
    ]
    for copy in copies:
        copy.start()
    for copy in copies:
        copy.wait()


def per_device(levels, patches, forcing, velocity, viscosity, friction, patch_rows):
    tall = pltpu.VMEM((TALL, SIDE), F32)
    vmem = pl.BlockSpec(memory_space=pltpu.VMEM)
    coarse = {
        sender: pltpu.VMEM((2, 2**sender // 2, SLOTS // 2**sender * SIDE // 2, SIDE), F32)
        for sender in range(1, levels)
    }
    adjoint, gradient = pl.pallas_call(
        functools.partial(kernel, levels, patches),
        out_shape=(
            jax.ShapeDtypeStruct((SLOTS, 2, SIDE, SIDE), F32),
            jax.ShapeDtypeStruct((SLOTS, SIDE, SIDE), BF16),
        ),
        in_specs=[pl.BlockSpec(memory_space=pltpu.HBM)] * 5,
        out_specs=(vmem, vmem),
        scratch_shapes=[
            pltpu.SMEM((levels, patches), jnp.int32),
            pltpu.VMEM((SLOTS, 2, SIDE, SIDE), BF16),
            pltpu.VMEM((SLOTS, 2, SIDE, SIDE), BF16),
            pltpu.VMEM((SLOTS, SIDE, SIDE), F32),
            pltpu.VMEM((SLOTS, SIDE, SIDE), BF16),
        ]
        + [tall] * 20
        + [
            pltpu.VMEM((2, SLOTS, 16, SIDE), F32),
            pltpu.VMEM((2, SLOTS, 16, SIDE), F32),
        ]
        + [coarse[sender] for sender in range(1, levels)] * 3
        + [pltpu.VMEM((4, 2, 8, SIDE), F32)] * 4
        + [pltpu.VMEM((2, 2 * SIDE, SIDE), F32)] * 2
        + [pltpu.VMEM((2, 8, SIDE), F32)] * 2
        + [
            pltpu.SemaphoreType.DMA((5,)),
            pltpu.SemaphoreType.DMA((4,)),
            pltpu.SemaphoreType.DMA((2, 16)),
            pltpu.SemaphoreType.DMA((2, 8)),
            pltpu.SemaphoreType.DMA((2, 32)),
            pltpu.SemaphoreType.DMA((2, 8)),
            pltpu.SemaphoreType.DMA((4,)),
        ],
        compiler_params=pltpu.CompilerParams(
            collective_id=0, has_side_effects=True, vmem_limit_bytes=44 << 20
        ),
    )(
        *(
            pltpu.with_memory_space_constraint(x, pltpu.HBM)
            for x in (patch_rows, forcing[0], velocity[0], viscosity[0], friction[0])
        )
    )
    adjoint, gradient = pl.pallas_call(
        write_out,
        out_shape=(
            jax.ShapeDtypeStruct(adjoint.shape, adjoint.dtype),
            jax.ShapeDtypeStruct(gradient.shape, gradient.dtype),
        ),
        in_specs=[vmem, vmem],
        out_specs=(pl.BlockSpec(memory_space=pltpu.HBM),) * 2,
        scratch_shapes=[pltpu.SemaphoreType.DMA((2,))],
        compiler_params=pltpu.CompilerParams(vmem_limit_bytes=4 << 20),
    )(adjoint, gradient)
    return adjoint[None], gradient[None]


def solution(mesh):
    in_specs = (
        P("level", "patch", None, None, None),
        P("level", "patch", None, None, None),
        P("level", "patch", None, None),
        P("level", "patch", None, None),
        P(),
    )
    out_specs = (P("level", "patch", None, None, None), P("level", "patch", None, None))
    return jax.shard_map(
        functools.partial(per_device, mesh.shape["level"], mesh.shape["patch"]),
        mesh=mesh,
        in_specs=in_specs,
        out_specs=out_specs,
        check_vma=False,
    )
```

```python
import functools

import jax
import jax.numpy as jnp
from jax import lax
from jax.experimental import pallas as pl
from jax.experimental.pallas import tpu as pltpu
from jax.sharding import PartitionSpec as P

MESH = pl.DeviceIdType.MESH
F32 = jnp.float32
BF16 = jnp.bfloat16
SIDE = 128
SLOTS = 8
PAD = 8
TALL = 3 * (SLOTS * SIDE + 2 * PAD)


def split_dot(x, matrix):
    high = x.astype(BF16)
    low = (x - high.astype(F32)).astype(BF16)
    return jnp.dot(high, matrix, preferred_element_type=F32) + jnp.dot(
        low, matrix, preferred_element_type=F32
    )


START_ROWS = {
    0: {0: (256, 1024), 1: (72, 256), 2: (24, 72), 3: (0, 24)},
    1: {1: (128, 512), 2: (40, 128), 3: (0, 40)},
    2: {2: (64, 256), 3: (0, 64)},
    3: {3: (0, 128)},
}
RESIDUAL_ROWS = {
    1: {1: (144, 512), 2: (48, 144), 3: (0, 48)},
    2: {2: (80, 256), 3: (0, 80)},
    3: {3: (0, 128)},
}
SMOOTH_ROWS = {
    1: {1: (136, 512), 2: (56, 136), 3: (0, 56)},
    2: {2: (64, 256), 3: (0, 64)},
    3: {3: (0, 128)},
}
SENT_UP = {
    0: {1: (72, 256), 2: (24, 72), 3: (0, 24)},
    1: {2: (40, 128), 3: (0, 40)},
    2: {3: (0, 64)},
}
ORDER = {
    0: ("down0", "down1", "down2", "down3"),
    1: ("down1", "known0", "down2", "down3", "up2", "up3", "send3", "send2", "up1"),
    2: ("down2", "down3", "up3", "up2"),
}


def over(col_at, col_count, rows, most, body, group=1):
    low, high = rows
    pieces = -(-(high - low) // most)
    size = -(-(high - low) // (8 * pieces)) * 8
    total = col_count * pieces

    def step(index):
        if isinstance(index, int):
            col, part = divmod(index, pieces)
            start = min(low + part * size, high - size)
        else:
            col = index // pieces
            part = index - col * pieces
            start = low if pieces == 1 else jnp.minimum(low + part * size, high - size)
        body(col_at + col if isinstance(col_at, int) else col_at(col), start, size)

    def steps(index, carry):
        for inner in range(group):
            step(index * group + inner)
        return carry

    done = 0
    if total > group:
        lax.fori_loop(0, total // group, steps, 0)
        done = total // group * group
    for index in range(done, total):
        step(index)


def kernel(
    levels,
    patches,
    rows_hbm,
    forcing_hbm,
    velocity_hbm,
    viscosity_hbm,
    friction_hbm,
    out_ref,
    grad_ref,
    rows_ref,
    forcing,
    velocity,
    viscosity,
    friction,
    mu,
    fric,
    mu_e,
    mu_w,
    diag_u,
    diag_v,
    half_u,
    half_v,
    b_u,
    b_v,
    x_u,
    x_v,
    z_u,
    z_v,
    ue,
    uw,
    ve,
    vw,
    y_u,
    y_v,
    init_send,
    init_recv,
    down_send_1,
    down_send_2,
    down_send_3,
    down_recv_0,
    down_recv_1,
    down_recv_2,
    up_recv_1,
    up_recv_2,
    up_recv_3,
    down_edge_send,
    down_edge_recv,
    up_edge_send,
    up_edge_recv,
    halo_sum,
    known_halo,
    base_edge_send,
    base_edge_recv,
    load_sem,
    init_sem,
    down_sem,
    down_edge_sem,
    up_sem,
    up_edge_sem,
    base_edge_sem,
):
    down_send = {1: down_send_1, 2: down_send_2, 3: down_send_3}
    down_recv = {0: down_recv_0, 1: down_recv_1, 2: down_recv_2}
    up_recv = {1: up_recv_1, 2: up_recv_2, 3: up_recv_3}
    level = lax.axis_index("level")
    patch = lax.axis_index("patch")
    cols = jnp.where(level == 0, 1, jnp.where(level == 1, 2, jnp.where(level == 2, 4, 8)))
    prows = jnp.where(level == 0, 8, jnp.where(level == 1, 4, jnp.where(level == 2, 2, 1)))
    height = prows * SIDE
    pitch = height + 2 * PAD
    has_west = patch > 0
    has_east = patch < patches - 1
    finer = jnp.minimum(level + 1, levels - 1)
    west = jnp.maximum(patch - 1, 0)
    east = jnp.minimum(patch + 1, patches - 1)
    loads = [
        pltpu.make_async_copy(src, dst, load_sem.at[i])
        for i, (src, dst) in enumerate(
            (
                (viscosity_hbm, viscosity),
                (friction_hbm, friction),
                (forcing_hbm, forcing),
                (velocity_hbm, velocity),
                (rows_hbm, rows_ref),
            )
        )
    ]
    for load in loads:
        load.start()

    barrier = pltpu.get_barrier_semaphore()
    count = jnp.int32(0)
    for dl in (-1, 0, 1):
        for dp in (-1, 0, 1):
            if (dl == 0) == (dp == 0):
                continue
            there = (level + dl >= 0) & (level + dl < levels) & (patch + dp >= 0) & (patch + dp < patches)
            count = count + jnp.where(there, 1, 0)

            @pl.when(there)
            def _(dl=dl, dp=dp):
                pl.semaphore_signal(
                    barrier,
                    inc=1,
                    device_id={"level": level + dl, "patch": patch + dp},
                    device_id_type=MESH,
                )

    def base_of(col, row):
        return pl.multiple_of((col * pitch + PAD + row * SIDE).astype(jnp.int32), 8)

    def alive(row, total):
        return jnp.where(row < total, 1.0, 0.0).astype(F32)

    lane = lax.broadcasted_iota(jnp.int32, (SIDE, SIDE), 1)

    zeros = jnp.zeros((PAD, SIDE), F32)

    def clear(col, carry):
        first = pl.multiple_of(col * pitch, 8)
        last = pl.multiple_of(col * pitch + PAD + height, 8)
        for ref in (mu, x_u, x_v, z_u, z_v, ue, uw, ve, vw):
            ref[pl.ds(first, PAD), :] = zeros
            ref[pl.ds(last, PAD), :] = zeros
        return carry

    lax.fori_loop(0, cols + 2, clear, 0)

    loads[4].wait()
    own_rows = rows_ref[level, patch]
    west_rows = jnp.where(has_west, rows_ref[level, west], 0)
    east_rows = jnp.where(has_east, rows_ref[level, east], 0)
    fine_own = rows_ref[finer, patch]
    fine_west = jnp.where(has_west, rows_ref[finer, west], 0)
    fine_east = jnp.where(has_east, rows_ref[finer, east], 0)

    for load in loads[:3]:
        load.wait()

    def unpack(slot_id, carry):
        col = slot_id // prows
        row = slot_id - col * prows
        base = base_of(col + 1, row)
        slot = row * cols + col
        live = alive(row, own_rows)
        mu[pl.ds(base, SIDE), :] = viscosity[slot] * live
        fric[pl.ds(base, SIDE), :] = friction[slot].astype(F32)
        b_u[pl.ds(base, SIDE), :] = forcing[slot, 0].astype(F32) * live
        b_v[pl.ds(base, SIDE), :] = forcing[slot, 1].astype(F32) * live
        return carry

    lax.fori_loop(0, SLOTS, unpack, 0)

    def pack(row, carry):
        for side in range(2):
            base = base_of(jnp.where(side == 0, 1, cols), row)
            four = slice(0, 4) if side == 0 else slice(SIDE - 4, SIDE)
            three = slice(0, 3) if side == 0 else slice(SIDE - 3, SIDE)
            mu_t = jnp.transpose(mu[pl.ds(base, SIDE), :])
            fr_t = jnp.transpose(fric[pl.ds(base, SIDE), :])
            bu_t = jnp.transpose(b_u[pl.ds(base, SIDE), :])
            bv_t = jnp.transpose(b_v[pl.ds(base, SIDE), :])
            parts = [
                mu_t[four],
                fr_t[three],
                bu_t[three],
                bv_t[three],
                jnp.zeros((3, SIDE), F32),
            ]
            init_send[side, row] = jnp.concatenate(parts, axis=0)
        return carry

    lax.fori_loop(0, prows, pack, 0)


    def copy_to(src, dst, send, recv, there, dp):
        return pltpu.make_async_remote_copy(
            src_ref=src,
            dst_ref=dst,
            send_sem=send,
            recv_sem=recv,
            device_id={"level": there, "patch": patch + dp},
            device_id_type=MESH,
        )

    def init_copies(lv, side):
        used = pl.ds(0, SLOTS // 2**lv)
        return copy_to(
            init_send.at[side, used],
            init_recv.at[side, used],
            init_sem.at[side],
            init_sem.at[2 + side],
            lv,
            -1 if side == 0 else 1,
        )

    def init_each(act, flip):
        for lv in range(levels):
            for side in range(2):
                there = has_west if (side == 0) != flip else has_east

                @pl.when((level == lv) & there)
                def _(lv=lv, side=side):
                    act(init_copies(lv, side))


    def columns_of(tile):
        blank = jnp.zeros((SIDE - tile.shape[0], SIDE), F32)
        return jnp.transpose(jnp.concatenate([tile, blank], axis=0))

    def lanes_from(tile_t, side, first, width):
        steps = (-first if side == 0 else SIDE - width - first) % SIDE
        return tile_t if steps == 0 else pltpu.roll(tile_t, steps, 1)

    def spread(tile_t, index, first=0, count=SIDE):
        return jnp.broadcast_to(tile_t[first : first + count, index : index + 1], (count, SIDE))

    def coefficients(index, carry):
        col = index // prows
        row = index - col * prows
        base = base_of(col, row)
        to_east = pl.multiple_of(base + jnp.where(col == cols + 1, 0, pitch), 8)
        to_west = pl.multiple_of(base - jnp.where(col == 0, 0, pitch), 8)
        total = jnp.where(col == 0, west_rows, jnp.where(col == cols + 1, east_rows, own_rows))
        live = 0.5 * alive(row, total)
        here = mu[pl.ds(base, SIDE), :]
        m_e = pltpu.roll(jnp.where(lane == 0, mu[pl.ds(to_east, SIDE), :], here), SIDE - 1, 1)
        m_w = pltpu.roll(jnp.where(lane == SIDE - 1, mu[pl.ds(to_west, SIDE), :], here), 1, 1)
        across = m_e + m_w + 2.0 * here
        along = mu[pl.ds(base + 1, SIDE), :] + mu[pl.ds(base - 1, SIDE), :] + 2.0 * here
        fr = fric[pl.ds(base, SIDE), :]
        d_u = 2.0 * across + 0.5 * along + fr
        d_v = 2.0 * along + 0.5 * across + fr
        mu_e[pl.ds(base, SIDE), :] = m_e
        mu_w[pl.ds(base, SIDE), :] = m_w
        diag_u[pl.ds(base, SIDE), :] = d_u
        diag_v[pl.ds(base, SIDE), :] = d_v
        half_u[pl.ds(base, SIDE), :] = live / d_u
        half_v[pl.ds(base, SIDE), :] = live / d_v
        return carry

    quarter = SIDE // 2
    lane_row = lax.broadcasted_iota(jnp.int32, (SIDE, SIDE), 0)
    joins = [
        jnp.where(lane_row // 2 + half * quarter == lane, 1.0, 0.0).astype(BF16)
        for half in range(2)
    ]
    spreads = [
        jnp.where(lane // 2 + half * quarter == lane_row, 1.0, 0.0).astype(BF16)
        for half in range(2)
    ]

    def program(lv, early):
        columns = 2**lv
        tall = SLOTS // columns * SIDE
        step_col = tall + 2 * PAD
        pending = []

        def at_row(col, row):
            return pl.multiple_of(col * step_col + PAD + row, 8)

        def below(start, size, limit):
            rows = lax.broadcasted_iota(jnp.int32, (size, SIDE), 0) + start
            return rows < limit

        def shift(src_u, src_v, rows, first=1, count=columns):
            def body(col, start, size):
                base = at_row(col, start)
                to_east = pl.multiple_of(base + jnp.where(col == columns + 1, 0, step_col), 8)
                to_west = pl.multiple_of(base - jnp.where(col == 0, 0, step_col), 8)
                here_lane = lane[:size]
                for src, dst_e, dst_w in ((src_u, ue, uw), (src_v, ve, vw)):
                    here = src[pl.ds(base, size), :]
                    dst_e[pl.ds(base, size), :] = pltpu.roll(
                        jnp.where(here_lane == 0, src[pl.ds(to_east, size), :], here), SIDE - 1, 1
                    )
                    dst_w[pl.ds(base, size), :] = pltpu.roll(
                        jnp.where(here_lane == SIDE - 1, src[pl.ds(to_west, size), :], here), 1, 1
                    )

            over(first, count, rows, SIDE, body, 4 if rows[1] - rows[0] <= 80 else 2)

        def residual_at(src_u, src_v, base, size):
            def at(ref, step=0):
                return ref[pl.ds(base + step, size), :]

            m, m_e, m_w, m_n, m_s = at(mu), at(mu_e), at(mu_w), at(mu, 1), at(mu, -1)
            p_e, p_w, p_n, p_s = m + m_e, m + m_w, m + m_n, m + m_s
            ue_n, ue_s, uw_n, uw_s = at(ue, 1), at(ue, -1), at(uw, 1), at(uw, -1)
            ve_n, ve_s, vw_n, vw_s = at(ve, 1), at(ve, -1), at(vw, 1), at(vw, -1)
            u, v = at(src_u), at(src_v)
            cross_u = 0.5 * (m_e * (ve_n - ve_s) - m_w * (vw_n - vw_s)) + 0.25 * (
                m_n * (ve_n - vw_n) - m_s * (ve_s - vw_s)
            )
            cross_v = 0.5 * (m_n * (ue_n - uw_n) - m_s * (ue_s - uw_s)) + 0.25 * (
                m_e * (ue_n - ue_s) - m_w * (uw_n - uw_s)
            )
            near_u = 2.0 * (p_e * at(ue) + p_w * at(uw)) + 0.5 * (
                p_n * at(src_u, 1) + p_s * at(src_u, -1)
            )
            near_v = 2.0 * (p_n * at(src_v, 1) + p_s * at(src_v, -1)) + 0.5 * (
                p_e * at(ve) + p_w * at(vw)
            )
            r_u = at(b_u) - (at(diag_u) * u - near_u - cross_u)
            r_v = at(b_v) - (at(diag_v) * v - near_v - cross_v)
            return u, v, r_u, r_v

        def sides():
            return ((0, has_west, has_east, -1), (1, has_east, has_west, 1))

        def down_copies(sender, tier, which=None):
            low, high = RESIDUAL_ROWS[sender][tier]
            low, high = low // 2, high // 2
            copies = []
            for k in range(2**sender // 2) if which is None else which:
                part = (slice(None), k, pl.ds(low, high - low))
                copies.append(
                    copy_to(
                        down_send[sender].at[part],
                        down_recv[sender - 1].at[part],
                        down_sem.at[0, tier * 4 + k],
                        down_sem.at[1, tier * 4 + k],
                        sender - 1,
                        0,
                    )
                )
            return copies

        def down_edge(sender, tier, side, dp):
            return copy_to(
                down_edge_send.at[tier, side],
                down_edge_recv.at[tier, side],
                down_edge_sem.at[0, tier * 2 + side],
                down_edge_sem.at[1, tier * 2 + side],
                sender - 1,
                dp,
            )

        def up_copies(sender, tier):
            low, high = SENT_UP[sender][tier]
            sources = (x_u, x_v) if sender == 0 else (y_u, y_v)
            pitch_here = SLOTS // 2**sender * SIDE + 2 * PAD
            copies = []
            for k in range(2**sender):
                for comp in range(2):
                    index = tier * 8 + k * 2 + comp
                    copies.append(
                        copy_to(
                            sources[comp].at[pl.ds((k + 1) * pitch_here + PAD + low, high - low)],
                            up_recv[sender + 1].at[comp, k, pl.ds(low, high - low)],
                            up_sem.at[0, index],
                            up_sem.at[1, index],
                            sender + 1,
                            0,
                        )
                    )
            return copies

        def up_edge(sender, tier, side, dp):
            return copy_to(
                up_edge_send.at[tier, side],
                up_edge_recv.at[tier, side],
                up_edge_sem.at[0, tier * 2 + side],
                up_edge_sem.at[1, tier * 2 + side],
                sender + 1,
                dp,
            )

        def known_copies():
            rows = 2 * SIDE
            return [
                copy_to(
                    ref.at[pl.ds(SLOTS * SIDE + 2 * PAD + PAD, rows)],
                    up_recv[1].at[comp, 0, pl.ds(0, rows)],
                    up_sem.at[0, comp],
                    up_sem.at[1, comp],
                    1,
                    0,
                )
                for comp, ref in enumerate((half_u, half_v))
            ]

        def known():
            wait_edges(base_edge, 0, 0)
            tiles = [jnp.transpose(base_edge_recv[side]) for side in range(2)]
            for comp in range(2):
                for part in range(2):
                    index = 2 * comp + part
                    known_halo[comp, pl.ds(part * SIDE, SIDE), :] = jnp.where(
                        lane < quarter, spread(tiles[0], index), spread(tiles[1], index)
                    )
            for copy in known_copies():
                copy.wait_recv()

        def base_edge(sender, tier, side, dp):
            return copy_to(
                base_edge_send.at[side],
                base_edge_recv.at[side],
                base_edge_sem.at[side],
                base_edge_sem.at[2 + side],
                1,
                dp,
            )

        def edges_of(refs, low, high):
            blocks = []
            for ref in refs:
                for part in range(2):
                    if part * SIDE < high and low < (part + 1) * SIDE:
                        rows = pl.ds(at_row(1, part * SIDE), SIDE)
                        blocks.append(jnp.transpose(ref[rows, :]))
            return [
                [block[near : near + 1] for block in blocks] for near in (0, SIDE - 1)
            ]

        def start_edges(make, sender, tier, which=(0, 1)):
            for side, there, _, dp in sides():
                if side not in which:
                    continue
                copy = make(sender, tier, side, dp)

                @pl.when(there)
                def _(copy=copy):
                    copy.start()

                pending.append((copy, there))

        def wait_edges(make, sender, tier, which=(0, 1)):
            for side, _, there, dp in sides():
                if side not in which:
                    continue
                copy = make(sender, tier, side, dp)

                @pl.when(there)
                def _(copy=copy):
                    copy.wait_recv()

        def fill_up_edges(tier, which=(0, 1)):
            low, high = SENT_UP[lv][tier]
            sources = (x_u, x_v) if lv == 0 else (y_u, y_v)
            for side in which:
                col = 1 if side == 0 else columns
                near = 0 if side == 0 else SIDE - 1
                parts = []
                for ref in sources:
                    for part in range(2):
                        if part * SIDE < high and low < (part + 1) * SIDE:
                            block_t = jnp.transpose(ref[pl.ds(at_row(col, part * SIDE), SIDE), :])
                            parts.append(block_t[near : near + 1])
                        else:
                            parts.append(jnp.zeros((1, SIDE), F32))
                parts.append(jnp.zeros((4, SIDE), F32))
                up_edge_send[tier, side] = jnp.concatenate(parts, axis=0)

        def send_up(tier):
            fill_up_edges(tier)
            start_edges(up_edge, lv, tier)
            for copy in up_copies(lv, tier):
                copy.start()
                pending.append((copy, None))

        def start_body(col, start, size):
            where = pl.ds(at_row(col, start), size)
            x_u[where, :] = half_u[where, :] * b_u[where, :]
            x_v[where, :] = half_v[where, :] * b_v[where, :]

        def down(tier):
            rows = START_ROWS[lv][tier]
            low, high = rows
            if tier == lv:
                if lv == 0:
                    over(1, 1, rows, SIDE, start_body)
                else:
                    over(0, columns + 2, rows, SIDE, start_body)
            else:
                def halos():
                    wait_edges(down_edge, lv + 1, tier)
                    for side in range(2):
                        col = columns + 1 if side == 0 else 0
                        limit = quarter * (fine_east if side == 0 else fine_west)
                        tile_t = columns_of(down_edge_recv[tier, side])[low:high]
                        where = pl.ds(at_row(col, low), high - low)
                        keep = below(low, high - low, limit)
                        for comp, (ref, half, to) in enumerate(
                            ((b_u, half_u, x_u), (b_v, half_v, x_v))
                        ):
                            got = lanes_from(tile_t, side, 3 * comp, 3)
                            new = jnp.where(keep, got, ref[where, :])
                            ref[where, :] = new
                            to[where, :] = half[where, :] * new

                if lv == 2:
                    halos()
                for copy in down_copies(lv + 1, tier):
                    copy.wait_recv()

                def place_body(col, start, size):
                    where = pl.ds(at_row(col, start), size)
                    keep = below(start, size, quarter * fine_own)
                    for comp, (ref, half, to) in enumerate(
                        ((b_u, half_u, x_u), (b_v, half_v, x_v))
                    ):
                        got = down_recv[lv][comp, col - 1, pl.ds(start, size), :]
                        new = jnp.where(keep, got, ref[where, :])
                        ref[where, :] = new
                        to[where, :] = half[where, :] * new

                over(1, columns, rows, SIDE, place_body, 4 if rows[1] <= 64 else 1)
                if lv == 1:
                    halos()
            if lv == 0:
                return
            first, count = (0, columns + 2) if lv == 1 else (1, columns)
            shift(x_u, x_v, rows, first, count)
            over(first, count, RESIDUAL_ROWS[lv][tier], 64, residual_body, 2)
            send_down(tier, range(columns // 2))

        def residual_body(col, start, size):
            base = at_row(col, start)
            _, _, r_u, r_v = residual_at(x_u, x_v, base, size)
            y_u[pl.ds(base, size), :] = r_u
            y_v[pl.ds(base, size), :] = r_v

        def send_down(tier, which):
            low, high = RESIDUAL_ROWS[lv][tier]
            low, high = low // 2, high // 2
            pairs = columns // 2
            def join_halo(low, high):
                join_pair(0, (columns + 1, 0), halo_sum)

            def join_pair(k, pair=None, to=None):
                pair = (2 * k + 1, 2 * k + 2) if pair is None else pair
                to = down_send[lv].at[:, k] if to is None else to

                def join_body(_, start, size):
                    for comp, ref in enumerate((y_u, y_v)):
                        total = None
                        for half in range(2):
                            base = at_row(pair[half], 2 * start)
                            lines = (
                                ref[pl.ds(base, size, stride=2), :]
                                + ref[pl.ds(base + 1, size, stride=2), :]
                            )
                            term = split_dot(lines, joins[half])
                            total = term if total is None else total + term
                        to[comp, pl.ds(start, size), :] = total

                over(0, 1, (low, high), 64, join_body)
            def start_pairs(ks):
                for copy in down_copies(lv, tier, ks):
                    copy.start()
                    pending.append((copy, None))

            outer = tuple(k for k in sorted({0, pairs - 1}) if k in which)
            for k in outer:
                join_pair(k)
            if lv == 1:
                start_pairs(outer)
                join_halo(low, high)
            if lv > 1 and 0 in which:
                for side in range(2):
                    k = 0 if side == 0 else pairs - 1
                    three = slice(0, 3) if side == 0 else slice(SIDE - 3, SIDE)
                    lines = min(SIDE, tall // 2)
                    parts = []
                    for comp in range(2):
                        block_t = jnp.transpose(down_send[lv][comp, k, pl.ds(0, lines), :])
                        line = block_t[three]
                        if lines < SIDE:
                            line = jnp.concatenate([line, line], axis=1)
                        parts.append(line)
                    parts.append(jnp.zeros((2, SIDE), F32))
                    down_edge_send[tier, side] = jnp.concatenate(parts, axis=0)
                start_edges(down_edge, lv, tier)
            if lv > 1:
                start_pairs(outer)
            for k in range(1, pairs - 1):
                if k in which:
                    join_pair(k)
                    start_pairs((k,))

        def up(tier):
            low, high = SENT_UP[lv - 1][tier]
            if lv == 1:
                halo_up(tier)
            if lv > 1:
                for copy in up_copies(lv - 1, tier):
                    copy.wait_recv()
            prolong(tier, 0, columns // 2)
            rows = SMOOTH_ROWS[lv][tier]
            fine = (2 * low, 2 * high)
            if lv == 2 and tier == 3:
                copies = up_copies(lv, tier)

                def ready(col):
                    for copy in copies[2 * col - 2 : 2 * col]:
                        copy.start()

                shift(z_u, z_v, fine, 2, 2)
                for col in (2, 3):
                    over(col, 1, rows, 64, smooth_body)
                    ready(col)
                halo_up(tier)
                shift(z_u, z_v, fine, lambda i: 1 + 3 * i, 2)
                over(lambda i: 1 + 3 * i, 2, rows, 64, smooth_body, 2)
                fill_up_edges(tier)
                start_edges(up_edge, lv, tier)
                for col in (1, 4):
                    ready(col)
                pending.extend((copy, None) for copy in copies)
                return
            if lv > 1:
                halo_up(tier)
            shift(z_u, z_v, fine)
            over(1, columns, rows, 64, smooth_body, 2)

        def smooth_body(col, start, size):
            base = at_row(col, start)
            where = pl.ds(base, size)
            u, v, r_u, r_v = residual_at(z_u, z_v, base, size)
            u = u + half_u[where, :] * r_u
            v = v + half_v[where, :] * r_v
            if lv < levels - 1:
                y_u[where, :] = u
                y_v[where, :] = v
                return
            slot = col - 1
            lines = pl.ds(start, size)
            live = alive(0, own_rows)
            out_ref[slot, 0, lines, :] = u
            out_ref[slot, 1, lines, :] = v
            product = (
                velocity[slot, 0, lines, :].astype(F32) * u
                + velocity[slot, 1, lines, :].astype(F32) * v
            )
            grad_ref[slot, lines, :] = (
                -(friction[slot, lines, :].astype(F32) * product) * live
            ).astype(BF16)

        def up_last():
            tier = levels - 1
            rows = (0, tall)
            copies = up_copies(lv - 1, tier)
            def columns_done(first, count):
                shift(z_u, z_v, rows, first, count)
                over(first, count, rows, 64, smooth_body, 2)

            for k in (1, 2, 0, 3):
                for copy in copies[2 * k : 2 * k + 2]:
                    copy.wait_recv()
                prolong(tier, k, 1)
                if k == 2:
                    columns_done(4, 2)
                if k == 0:
                    columns_done(2, 2)
                    halo_up(tier)
                    columns_done(1, 1)
            columns_done(6, 3)

        def halo_up(tier, which=(0, 1)):
            low, high = SENT_UP[lv - 1][tier]
            if lv == 1:
                def halo_body(_, start, size):
                    limit = quarter * jnp.where(lane[:size] < quarter, east_rows, west_rows)
                    keep = lax.broadcasted_iota(jnp.int32, (size, SIDE), 0) + start < limit
                    for comp, (ref, to) in enumerate(((x_u, z_u), (x_v, z_v))):
                        lines = pl.ds(start, size)
                        wide = known_halo[comp, lines, :] * halo_sum[comp, lines, :]
                        wide = jnp.where(keep, wide, 0.0)
                        for col in (0, columns + 1):
                            for step in range(2):
                                where = pl.ds(at_row(col, 2 * start) + step, size, stride=2)
                                to[where, :] = ref[where, :] + wide

                over(0, 1, (low, high), 64, halo_body)
                return
            wait_edges(up_edge, lv - 1, tier, which)
            for side in which:
                col = columns + 1 if side == 0 else 0
                limit = quarter * (east_rows if side == 0 else west_rows)
                tile_t = jnp.transpose(up_edge_recv[tier, side])
                for part in range(2):
                    first, last = max(low, part * SIDE), min(high, (part + 1) * SIDE)
                    if first >= last:
                        continue
                    size = last - first
                    keep = below(first, size, limit)
                    for comp, (ref, to) in enumerate(((x_u, z_u), (x_v, z_v))):
                        wide = spread(tile_t, 2 * comp + part, first - part * SIDE, size)
                        wide = jnp.where(keep, wide, 0.0)
                        for step in range(2):
                            where = pl.ds(at_row(col, 2 * first) + step, size, stride=2)
                            to[where, :] = ref[where, :] + wide

        def prolong(tier, first, count):
            low, high = SENT_UP[lv - 1][tier]

            def prolong_body(k, start, size):
                keep = below(start, size, quarter * own_rows)
                for comp, (ref, to) in enumerate(((x_u, z_u), (x_v, z_v))):
                    coarse = up_recv[lv][comp, k, pl.ds(start, size), :]
                    if lv == 1:
                        coarse = coarse * down_send[1][comp, k, pl.ds(start, size), :]
                    coarse = jnp.where(keep, coarse, 0.0)
                    for half in range(2):
                        base = at_row(2 * k + half + 1, 2 * start)
                        wide = split_dot(coarse, spreads[half])
                        for step in range(2):
                            where = pl.ds(base + step, size, stride=2)
                            to[where, :] = ref[where, :] + wide

            over(first, count, (low, high), 64, prolong_body, 2)

        if lv == levels - 1:
            if early:
                if early == 1:
                    lax.fori_loop(1, columns + 1, coefficients, 0)
                    over(1, columns, (0, tall), SIDE, start_body, 2)
                    shift(x_u, x_v, (0, tall), 2, columns - 2)
                    return
                over(3, columns - 4, (0, tall), 64, residual_body, 2)
                send_down(lv, (1, 2))
                over(lambda i: 2 + 5 * i, 2, (0, tall), 64, residual_body, 2)
                return
            ends = lambda i: jnp.where(i < 2, i, i + 6)
            inner = lambda i: 1 + 7 * i
            lax.fori_loop(0, 4, lambda i, carry: coefficients(ends(i), carry), 0)
            over(ends, 4, (0, tall), SIDE, start_body)
            shift(x_u, x_v, (0, tall), inner, 2)
            over(inner, 2, (0, tall), 64, residual_body, 2)
            send_down(lv, (0, 3))
            pending.extend((copy, None) for copy in down_copies(lv, lv, (1, 2)))
            loads[3].wait()
            up_last()
        else:
            if lv == 0:
                for copy in known_copies():
                    copy.start()
                    pending.append((copy, None))
                for side, lines in enumerate(edges_of((half_u, half_v), 0, 2 * SIDE)):
                    lines.append(jnp.zeros((4, SIDE), F32))
                    base_edge_send[side] = jnp.concatenate(lines, axis=0)
                start_edges(base_edge, lv, 0)
            for word in ORDER[lv]:
                if word == "known0":
                    known()
                    continue
                {"down": down, "up": up, "send": send_up}[word[:-1]](int(word[-1]))
            loads[3].wait()

        finals = (x_u, x_v) if lv == 0 else (y_u, y_v)

        def finish(col, start, size):
            base = at_row(col, start)
            row = start // SIDE
            slot = row * columns + col - 1
            live = alive(row, own_rows)
            u = finals[0][pl.ds(base, size), :]
            v = finals[1][pl.ds(base, size), :]
            out_ref[slot, 0] = u
            out_ref[slot, 1] = v
            product = velocity[slot, 0].astype(F32) * u + velocity[slot, 1].astype(F32) * v
            grad_ref[slot] = (-(friction[slot].astype(F32) * product) * live).astype(BF16)

        if lv < levels - 1:
            over(1, columns, (0, tall), SIDE, finish)
        for copy, there in pending:
            if there is None:
                copy.wait_send()
            else:

                @pl.when(there)
                def _(copy=copy):
                    copy.wait_send()

    @pl.when(level == levels - 1)
    def _():
        program(levels - 1, 1)

    pl.semaphore_wait(barrier, count)
    init_each(lambda copy: copy.start(), False)

    @pl.when(level == levels - 1)
    def _():
        program(levels - 1, 2)

    @pl.when(jnp.logical_not(has_east))
    def _():
        init_recv[0] = jnp.ones((SLOTS, 16, SIDE), F32)

    @pl.when(jnp.logical_not(has_west))
    def _():
        init_recv[1] = jnp.ones((SLOTS, 16, SIDE), F32)

    init_each(lambda copy: copy.wait_recv(), True)

    def unpack_halo(row, carry):
        for side in range(2):
            col = cols + 1 if side == 0 else 0
            base = base_of(jnp.int32(0) + col, row)
            live = alive(row, east_rows if side == 0 else west_rows)
            tile_t = columns_of(init_recv[side, row])

            def place(first, width, other):
                valid = lane < width if side == 0 else lane >= SIDE - width
                return jnp.where(valid, lanes_from(tile_t, side, first, width), other)

            mu[pl.ds(base, SIDE), :] = place(0, 4, 0.0) * live
            fric[pl.ds(base, SIDE), :] = place(4, 3, 1.0)
            b_u[pl.ds(base, SIDE), :] = place(7, 3, 0.0) * live
            b_v[pl.ds(base, SIDE), :] = place(10, 3, 0.0) * live
        return carry

    lax.fori_loop(0, prows, unpack_halo, 0)

    @pl.when(level < levels - 1)
    def _():
        first = jnp.where(level == 0, prows, 0)
        last = jnp.where(level == 0, 2 * prows, (cols + 2) * prows)
        lax.fori_loop(first, last, coefficients, 0)

    for lv in range(levels):

        @pl.when(level == lv)
        def _(lv=lv):
            program(lv, 0)

    init_each(lambda copy: copy.wait_send(), False)


def write_out(adjoint, gradient, adjoint_hbm, gradient_hbm, sem):
    copies = [
        pltpu.make_async_copy(adjoint, adjoint_hbm, sem.at[0]),
        pltpu.make_async_copy(gradient, gradient_hbm, sem.at[1]),
    ]
    for copy in copies:
        copy.start()
    for copy in copies:
        copy.wait()


def per_device(levels, patches, forcing, velocity, viscosity, friction, patch_rows):
    tall = pltpu.VMEM((TALL, SIDE), F32)
    vmem = pl.BlockSpec(memory_space=pltpu.VMEM)
    coarse = {
        sender: pltpu.VMEM((2, 2**sender // 2, SLOTS // 2**sender * SIDE // 2, SIDE), F32)
        for sender in range(1, levels)
    }
    adjoint, gradient = pl.pallas_call(
        functools.partial(kernel, levels, patches),
        out_shape=(
            jax.ShapeDtypeStruct((SLOTS, 2, SIDE, SIDE), F32),
            jax.ShapeDtypeStruct((SLOTS, SIDE, SIDE), BF16),
        ),
        in_specs=[pl.BlockSpec(memory_space=pltpu.HBM)] * 5,
        out_specs=(vmem, vmem),
        scratch_shapes=[
            pltpu.SMEM((levels, patches), jnp.int32),
            pltpu.VMEM((SLOTS, 2, SIDE, SIDE), BF16),
            pltpu.VMEM((SLOTS, 2, SIDE, SIDE), BF16),
            pltpu.VMEM((SLOTS, SIDE, SIDE), F32),
            pltpu.VMEM((SLOTS, SIDE, SIDE), BF16),
        ]
        + [tall] * 20
        + [
            pltpu.VMEM((2, SLOTS, 16, SIDE), F32),
            pltpu.VMEM((2, SLOTS, 16, SIDE), F32),
        ]
        + [coarse[sender] for sender in range(1, levels)] * 3
        + [pltpu.VMEM((4, 2, 8, SIDE), F32)] * 4
        + [pltpu.VMEM((2, 2 * SIDE, SIDE), F32)] * 2
        + [pltpu.VMEM((2, 8, SIDE), F32)] * 2
        + [
            pltpu.SemaphoreType.DMA((5,)),
            pltpu.SemaphoreType.DMA((4,)),
            pltpu.SemaphoreType.DMA((2, 16)),
            pltpu.SemaphoreType.DMA((2, 8)),
            pltpu.SemaphoreType.DMA((2, 32)),
            pltpu.SemaphoreType.DMA((2, 8)),
            pltpu.SemaphoreType.DMA((4,)),
        ],
        compiler_params=pltpu.CompilerParams(
            collective_id=0, has_side_effects=True, vmem_limit_bytes=44 << 20
        ),
    )(
        *(
            pltpu.with_memory_space_constraint(x, pltpu.HBM)
            for x in (patch_rows, forcing[0], velocity[0], viscosity[0], friction[0])
        )
    )
    adjoint, gradient = pl.pallas_call(
        write_out,
        out_shape=(
            jax.ShapeDtypeStruct(adjoint.shape, adjoint.dtype),
            jax.ShapeDtypeStruct(gradient.shape, gradient.dtype),
        ),
        in_specs=[vmem, vmem],
        out_specs=(pl.BlockSpec(memory_space=pltpu.HBM),) * 2,
        scratch_shapes=[pltpu.SemaphoreType.DMA((2,))],
        compiler_params=pltpu.CompilerParams(vmem_limit_bytes=4 << 20),
    )(adjoint, gradient)
    return adjoint[None], gradient[None]


def solution(mesh):
    in_specs = (
        P("level", "patch", None, None, None),
        P("level", "patch", None, None, None),
        P("level", "patch", None, None),
        P("level", "patch", None, None),
        P(),
    )
    out_specs = (P("level", "patch", None, None, None), P("level", "patch", None, None))
    return jax.shard_map(
        functools.partial(per_device, mesh.shape["level"], mesh.shape["patch"]),
        mesh=mesh,
        in_specs=in_specs,
        out_specs=out_specs,
        check_vma=False,
    )
```

```python
import functools

import jax
import jax.numpy as jnp
from jax import lax
from jax.experimental import pallas as pl
from jax.experimental.pallas import tpu as pltpu
from jax.sharding import PartitionSpec as P

MESH = pl.DeviceIdType.MESH
F32 = jnp.float32
BF16 = jnp.bfloat16
SIDE = 128
SLOTS = 8
PAD = 8
TALL = 3 * (SLOTS * SIDE + 2 * PAD)


def split_dot(x, matrix):
    high = x.astype(BF16)
    low = (x - high.astype(F32)).astype(BF16)
    return jnp.dot(high, matrix, preferred_element_type=F32) + jnp.dot(
        low, matrix, preferred_element_type=F32
    )


START_ROWS = {
    0: {0: (256, 1024), 1: (72, 256), 2: (24, 72), 3: (0, 24)},
    1: {1: (128, 512), 2: (40, 128), 3: (0, 40)},
    2: {2: (64, 256), 3: (0, 64)},
    3: {3: (0, 128)},
}
RESIDUAL_ROWS = {
    1: {1: (144, 512), 2: (48, 144), 3: (0, 48)},
    2: {2: (80, 256), 3: (0, 80)},
    3: {3: (0, 128)},
}
SMOOTH_ROWS = {
    1: {1: (136, 512), 2: (56, 136), 3: (0, 56)},
    2: {2: (64, 256), 3: (0, 64)},
    3: {3: (0, 128)},
}
SENT_UP = {
    0: {1: (72, 256), 2: (24, 72), 3: (0, 24)},
    1: {2: (40, 128), 3: (0, 40)},
    2: {3: (0, 64)},
}
ORDER = {
    0: ("down0", "down1", "down2", "down3"),
    1: ("down1", "down2", "known0", "down3", "up2", "up3", "send3", "send2", "up1"),
    2: ("down2", "down3", "up3", "up2"),
}


def over(col_at, col_count, rows, most, body, group=1):
    low, high = rows
    pieces = -(-(high - low) // most)
    size = -(-(high - low) // (8 * pieces)) * 8
    total = col_count * pieces

    def step(index):
        if isinstance(index, int):
            col, part = divmod(index, pieces)
            start = min(low + part * size, high - size)
        else:
            col = index // pieces
            part = index - col * pieces
            start = low if pieces == 1 else jnp.minimum(low + part * size, high - size)
        body(col_at + col if isinstance(col_at, int) else col_at(col), start, size)

    def steps(index, carry):
        for inner in range(group):
            step(index * group + inner)
        return carry

    done = 0
    if total > group:
        lax.fori_loop(0, total // group, steps, 0)
        done = total // group * group
    for index in range(done, total):
        step(index)


def kernel(
    levels,
    patches,
    rows_hbm,
    forcing_hbm,
    velocity_hbm,
    viscosity_hbm,
    friction_hbm,
    out_ref,
    grad_ref,
    rows_ref,
    forcing,
    velocity,
    viscosity,
    friction,
    mu,
    fric,
    mu_e,
    mu_w,
    diag_u,
    diag_v,
    half_u,
    half_v,
    b_u,
    b_v,
    x_u,
    x_v,
    z_u,
    z_v,
    ue,
    uw,
    ve,
    vw,
    y_u,
    y_v,
    init_send,
    init_recv,
    down_send_1,
    down_send_2,
    down_send_3,
    down_recv_0,
    down_recv_1,
    down_recv_2,
    up_recv_1,
    up_recv_2,
    up_recv_3,
    down_edge_send,
    down_edge_recv,
    up_edge_send,
    up_edge_recv,
    halo_sum,
    known_halo,
    base_edge_send,
    base_edge_recv,
    load_sem,
    init_sem,
    down_sem,
    down_edge_sem,
    up_sem,
    up_edge_sem,
    base_edge_sem,
):
    down_send = {1: down_send_1, 2: down_send_2, 3: down_send_3}
    down_recv = {0: down_recv_0, 1: down_recv_1, 2: down_recv_2}
    up_recv = {1: up_recv_1, 2: up_recv_2, 3: up_recv_3}
    level = lax.axis_index("level")
    patch = lax.axis_index("patch")
    cols = jnp.where(level == 0, 1, jnp.where(level == 1, 2, jnp.where(level == 2, 4, 8)))
    prows = jnp.where(level == 0, 8, jnp.where(level == 1, 4, jnp.where(level == 2, 2, 1)))
    height = prows * SIDE
    pitch = height + 2 * PAD
    has_west = patch > 0
    has_east = patch < patches - 1
    finer = jnp.minimum(level + 1, levels - 1)
    west = jnp.maximum(patch - 1, 0)
    east = jnp.minimum(patch + 1, patches - 1)
    loads = [
        pltpu.make_async_copy(src, dst, load_sem.at[i])
        for i, (src, dst) in enumerate(
            (
                (viscosity_hbm, viscosity),
                (friction_hbm, friction),
                (forcing_hbm, forcing),
                (velocity_hbm, velocity),
                (rows_hbm, rows_ref),
            )
        )
    ]
    for load in loads:
        load.start()

    barrier = pltpu.get_barrier_semaphore()
    count = jnp.int32(0)
    for dl in (-1, 0, 1):
        for dp in (-1, 0, 1):
            if (dl == 0) == (dp == 0):
                continue
            there = (level + dl >= 0) & (level + dl < levels) & (patch + dp >= 0) & (patch + dp < patches)
            count = count + jnp.where(there, 1, 0)

            @pl.when(there)
            def _(dl=dl, dp=dp):
                pl.semaphore_signal(
                    barrier,
                    inc=1,
                    device_id={"level": level + dl, "patch": patch + dp},
                    device_id_type=MESH,
                )

    def base_of(col, row):
        return pl.multiple_of((col * pitch + PAD + row * SIDE).astype(jnp.int32), 8)

    def alive(row, total):
        return jnp.where(row < total, 1.0, 0.0).astype(F32)

    lane = lax.broadcasted_iota(jnp.int32, (SIDE, SIDE), 1)

    zeros = jnp.zeros((PAD, SIDE), F32)

    def clear(col, carry):
        first = pl.multiple_of(col * pitch, 8)
        last = pl.multiple_of(col * pitch + PAD + height, 8)
        for ref in (mu, x_u, x_v, z_u, z_v, ue, uw, ve, vw):
            ref[pl.ds(first, PAD), :] = zeros
            ref[pl.ds(last, PAD), :] = zeros
        return carry

    lax.fori_loop(0, cols + 2, clear, 0)

    loads[4].wait()
    own_rows = rows_ref[level, patch]
    west_rows = jnp.where(has_west, rows_ref[level, west], 0)
    east_rows = jnp.where(has_east, rows_ref[level, east], 0)
    fine_own = rows_ref[finer, patch]
    fine_west = jnp.where(has_west, rows_ref[finer, west], 0)
    fine_east = jnp.where(has_east, rows_ref[finer, east], 0)

    for load in loads[:3]:
        load.wait()

    def unpack(slot_id, carry):
        col = slot_id // prows
        row = slot_id - col * prows
        base = base_of(col + 1, row)
        slot = row * cols + col
        live = alive(row, own_rows)
        mu[pl.ds(base, SIDE), :] = viscosity[slot] * live
        fric[pl.ds(base, SIDE), :] = friction[slot].astype(F32)
        b_u[pl.ds(base, SIDE), :] = forcing[slot, 0].astype(F32) * live
        b_v[pl.ds(base, SIDE), :] = forcing[slot, 1].astype(F32) * live
        return carry

    lax.fori_loop(0, SLOTS, unpack, 0)

    def pack(row, carry):
        for side in range(2):
            base = base_of(jnp.where(side == 0, 1, cols), row)
            four = slice(0, 4) if side == 0 else slice(SIDE - 4, SIDE)
            three = slice(0, 3) if side == 0 else slice(SIDE - 3, SIDE)
            mu_t = jnp.transpose(mu[pl.ds(base, SIDE), :])
            fr_t = jnp.transpose(fric[pl.ds(base, SIDE), :])
            bu_t = jnp.transpose(b_u[pl.ds(base, SIDE), :])
            bv_t = jnp.transpose(b_v[pl.ds(base, SIDE), :])
            parts = [
                mu_t[four],
                fr_t[three],
                bu_t[three],
                bv_t[three],
                jnp.zeros((3, SIDE), F32),
            ]
            init_send[side, row] = jnp.concatenate(parts, axis=0)
        return carry

    lax.fori_loop(0, prows, pack, 0)


    def copy_to(src, dst, send, recv, there, dp):
        return pltpu.make_async_remote_copy(
            src_ref=src,
            dst_ref=dst,
            send_sem=send,
            recv_sem=recv,
            device_id={"level": there, "patch": patch + dp},
            device_id_type=MESH,
        )

    def init_copies(lv, side):
        used = pl.ds(0, SLOTS // 2**lv)
        return copy_to(
            init_send.at[side, used],
            init_recv.at[side, used],
            init_sem.at[side],
            init_sem.at[2 + side],
            lv,
            -1 if side == 0 else 1,
        )

    def init_each(act, flip):
        for lv in range(levels):
            for side in range(2):
                there = has_west if (side == 0) != flip else has_east

                @pl.when((level == lv) & there)
                def _(lv=lv, side=side):
                    act(init_copies(lv, side))


    def columns_of(tile):
        blank = jnp.zeros((SIDE - tile.shape[0], SIDE), F32)
        return jnp.transpose(jnp.concatenate([tile, blank], axis=0))

    def lanes_from(tile_t, side, first, width):
        steps = (-first if side == 0 else SIDE - width - first) % SIDE
        return tile_t if steps == 0 else pltpu.roll(tile_t, steps, 1)

    def spread(tile_t, index, first=0, count=SIDE):
        return jnp.broadcast_to(tile_t[first : first + count, index : index + 1], (count, SIDE))

    def coefficients(index, carry):
        col = index // prows
        row = index - col * prows
        base = base_of(col, row)
        to_east = pl.multiple_of(base + jnp.where(col == cols + 1, 0, pitch), 8)
        to_west = pl.multiple_of(base - jnp.where(col == 0, 0, pitch), 8)
        total = jnp.where(col == 0, west_rows, jnp.where(col == cols + 1, east_rows, own_rows))
        live = 0.5 * alive(row, total)
        here = mu[pl.ds(base, SIDE), :]
        m_e = pltpu.roll(jnp.where(lane == 0, mu[pl.ds(to_east, SIDE), :], here), SIDE - 1, 1)
        m_w = pltpu.roll(jnp.where(lane == SIDE - 1, mu[pl.ds(to_west, SIDE), :], here), 1, 1)
        across = m_e + m_w + 2.0 * here
        along = mu[pl.ds(base + 1, SIDE), :] + mu[pl.ds(base - 1, SIDE), :] + 2.0 * here
        fr = fric[pl.ds(base, SIDE), :]
        d_u = 2.0 * across + 0.5 * along + fr
        d_v = 2.0 * along + 0.5 * across + fr
        mu_e[pl.ds(base, SIDE), :] = m_e
        mu_w[pl.ds(base, SIDE), :] = m_w
        diag_u[pl.ds(base, SIDE), :] = d_u
        diag_v[pl.ds(base, SIDE), :] = d_v
        half_u[pl.ds(base, SIDE), :] = live / d_u
        half_v[pl.ds(base, SIDE), :] = live / d_v
        return carry

    quarter = SIDE // 2
    lane_row = lax.broadcasted_iota(jnp.int32, (SIDE, SIDE), 0)
    joins = [
        jnp.where(lane_row // 2 + half * quarter == lane, 1.0, 0.0).astype(BF16)
        for half in range(2)
    ]
    spreads = [
        jnp.where(lane // 2 + half * quarter == lane_row, 1.0, 0.0).astype(BF16)
        for half in range(2)
    ]

    def program(lv, early):
        columns = 2**lv
        tall = SLOTS // columns * SIDE
        step_col = tall + 2 * PAD
        pending = []

        def at_row(col, row):
            return pl.multiple_of(col * step_col + PAD + row, 8)

        def below(start, size, limit):
            rows = lax.broadcasted_iota(jnp.int32, (size, SIDE), 0) + start
            return rows < limit

        def shift(src_u, src_v, rows, first=1, count=columns):
            def body(col, start, size):
                base = at_row(col, start)
                to_east = pl.multiple_of(base + jnp.where(col == columns + 1, 0, step_col), 8)
                to_west = pl.multiple_of(base - jnp.where(col == 0, 0, step_col), 8)
                here_lane = lane[:size]
                for src, dst_e, dst_w in ((src_u, ue, uw), (src_v, ve, vw)):
                    here = src[pl.ds(base, size), :]
                    dst_e[pl.ds(base, size), :] = pltpu.roll(
                        jnp.where(here_lane == 0, src[pl.ds(to_east, size), :], here), SIDE - 1, 1
                    )
                    dst_w[pl.ds(base, size), :] = pltpu.roll(
                        jnp.where(here_lane == SIDE - 1, src[pl.ds(to_west, size), :], here), 1, 1
                    )

            over(first, count, rows, SIDE, body, 4 if rows[1] - rows[0] <= 80 else 2)

        def residual_at(src_u, src_v, base, size):
            def at(ref, step=0):
                return ref[pl.ds(base + step, size), :]

            m, m_e, m_w, m_n, m_s = at(mu), at(mu_e), at(mu_w), at(mu, 1), at(mu, -1)
            p_e, p_w, p_n, p_s = m + m_e, m + m_w, m + m_n, m + m_s
            ue_n, ue_s, uw_n, uw_s = at(ue, 1), at(ue, -1), at(uw, 1), at(uw, -1)
            ve_n, ve_s, vw_n, vw_s = at(ve, 1), at(ve, -1), at(vw, 1), at(vw, -1)
            u, v = at(src_u), at(src_v)
            cross_u = 0.5 * (m_e * (ve_n - ve_s) - m_w * (vw_n - vw_s)) + 0.25 * (
                m_n * (ve_n - vw_n) - m_s * (ve_s - vw_s)
            )
            cross_v = 0.5 * (m_n * (ue_n - uw_n) - m_s * (ue_s - uw_s)) + 0.25 * (
                m_e * (ue_n - ue_s) - m_w * (uw_n - uw_s)
            )
            near_u = 2.0 * (p_e * at(ue) + p_w * at(uw)) + 0.5 * (
                p_n * at(src_u, 1) + p_s * at(src_u, -1)
            )
            near_v = 2.0 * (p_n * at(src_v, 1) + p_s * at(src_v, -1)) + 0.5 * (
                p_e * at(ve) + p_w * at(vw)
            )
            r_u = at(b_u) - (at(diag_u) * u - near_u - cross_u)
            r_v = at(b_v) - (at(diag_v) * v - near_v - cross_v)
            return u, v, r_u, r_v

        def sides():
            return ((0, has_west, has_east, -1), (1, has_east, has_west, 1))

        def down_copies(sender, tier, which=None):
            low, high = RESIDUAL_ROWS[sender][tier]
            low, high = low // 2, high // 2
            copies = []
            for k in range(2**sender // 2) if which is None else which:
                part = (slice(None), k, pl.ds(low, high - low))
                copies.append(
                    copy_to(
                        down_send[sender].at[part],
                        down_recv[sender - 1].at[part],
                        down_sem.at[0, tier * 4 + k],
                        down_sem.at[1, tier * 4 + k],
                        sender - 1,
                        0,
                    )
                )
            return copies

        def down_edge(sender, tier, side, dp):
            return copy_to(
                down_edge_send.at[tier, side],
                down_edge_recv.at[tier, side],
                down_edge_sem.at[0, tier * 2 + side],
                down_edge_sem.at[1, tier * 2 + side],
                sender - 1,
                dp,
            )

        def up_copies(sender, tier):
            low, high = SENT_UP[sender][tier]
            sources = (x_u, x_v) if sender == 0 else (y_u, y_v)
            pitch_here = SLOTS // 2**sender * SIDE + 2 * PAD
            copies = []
            for k in range(2**sender):
                for comp in range(2):
                    index = tier * 8 + k * 2 + comp
                    copies.append(
                        copy_to(
                            sources[comp].at[pl.ds((k + 1) * pitch_here + PAD + low, high - low)],
                            up_recv[sender + 1].at[comp, k, pl.ds(low, high - low)],
                            up_sem.at[0, index],
                            up_sem.at[1, index],
                            sender + 1,
                            0,
                        )
                    )
            return copies

        def up_edge(sender, tier, side, dp):
            return copy_to(
                up_edge_send.at[tier, side],
                up_edge_recv.at[tier, side],
                up_edge_sem.at[0, tier * 2 + side],
                up_edge_sem.at[1, tier * 2 + side],
                sender + 1,
                dp,
            )

        def known_copies():
            rows = 2 * SIDE
            return [
                copy_to(
                    ref.at[pl.ds(SLOTS * SIDE + 2 * PAD + PAD, rows)],
                    up_recv[1].at[comp, 0, pl.ds(0, rows)],
                    up_sem.at[0, comp],
                    up_sem.at[1, comp],
                    1,
                    0,
                )
                for comp, ref in enumerate((half_u, half_v))
            ]

        def known():
            wait_edges(base_edge, 0, 0)
            tiles = [jnp.transpose(base_edge_recv[side]) for side in range(2)]
            for comp in range(2):
                for part in range(2):
                    index = 2 * comp + part
                    known_halo[comp, pl.ds(part * SIDE, SIDE), :] = jnp.where(
                        lane < quarter, spread(tiles[0], index), spread(tiles[1], index)
                    )
            for copy in known_copies():
                copy.wait_recv()

        def base_edge(sender, tier, side, dp):
            return copy_to(
                base_edge_send.at[side],
                base_edge_recv.at[side],
                base_edge_sem.at[side],
                base_edge_sem.at[2 + side],
                1,
                dp,
            )

        def edges_of(refs, low, high):
            blocks = []
            for ref in refs:
                for part in range(2):
                    if part * SIDE < high and low < (part + 1) * SIDE:
                        rows = pl.ds(at_row(1, part * SIDE), SIDE)
                        blocks.append(jnp.transpose(ref[rows, :]))
            return [
                [block[near : near + 1] for block in blocks] for near in (0, SIDE - 1)
            ]

        def start_edges(make, sender, tier, which=(0, 1)):
            for side, there, _, dp in sides():
                if side not in which:
                    continue
                copy = make(sender, tier, side, dp)

                @pl.when(there)
                def _(copy=copy):
                    copy.start()

                pending.append((copy, there))

        def wait_edges(make, sender, tier, which=(0, 1)):
            for side, _, there, dp in sides():
                if side not in which:
                    continue
                copy = make(sender, tier, side, dp)

                @pl.when(there)
                def _(copy=copy):
                    copy.wait_recv()

        def fill_up_edges(tier, which=(0, 1)):
            low, high = SENT_UP[lv][tier]
            sources = (x_u, x_v) if lv == 0 else (y_u, y_v)
            for side in which:
                col = 1 if side == 0 else columns
                near = 0 if side == 0 else SIDE - 1
                parts = []
                for ref in sources:
                    for part in range(2):
                        if part * SIDE < high and low < (part + 1) * SIDE:
                            block_t = jnp.transpose(ref[pl.ds(at_row(col, part * SIDE), SIDE), :])
                            parts.append(block_t[near : near + 1])
                        else:
                            parts.append(jnp.zeros((1, SIDE), F32))
                parts.append(jnp.zeros((4, SIDE), F32))
                up_edge_send[tier, side] = jnp.concatenate(parts, axis=0)

        def send_up(tier):
            fill_up_edges(tier)
            start_edges(up_edge, lv, tier)
            for copy in up_copies(lv, tier):
                copy.start()
                pending.append((copy, None))

        def start_body(col, start, size):
            where = pl.ds(at_row(col, start), size)
            x_u[where, :] = half_u[where, :] * b_u[where, :]
            x_v[where, :] = half_v[where, :] * b_v[where, :]

        def down(tier):
            rows = START_ROWS[lv][tier]
            low, high = rows
            if tier == lv:
                if lv == 2:
                    ends = lambda i: jnp.where(i < 2, i, i + 2)
                    lax.fori_loop(
                        0,
                        8,
                        lambda i, carry: coefficients(ends(i // 2) * 2 + i % 2, carry),
                        0,
                    )
                    for col in (0, 1, 4, 5):
                        over(col, 1, rows, SIDE, start_body, 2)
                elif lv == 0:
                    over(1, 1, rows, SIDE, start_body)
                else:
                    over(0, columns + 2, rows, SIDE, start_body)
            else:
                def halos():
                    wait_edges(down_edge, lv + 1, tier)
                    for side in range(2):
                        col = columns + 1 if side == 0 else 0
                        limit = quarter * (fine_east if side == 0 else fine_west)
                        tile_t = columns_of(down_edge_recv[tier, side])[low:high]
                        where = pl.ds(at_row(col, low), high - low)
                        keep = below(low, high - low, limit)
                        for comp, (ref, half, to) in enumerate(
                            ((b_u, half_u, x_u), (b_v, half_v, x_v))
                        ):
                            got = lanes_from(tile_t, side, 3 * comp, 3)
                            new = jnp.where(keep, got, ref[where, :])
                            ref[where, :] = new
                            to[where, :] = half[where, :] * new

                if lv == 2:
                    halos()
                for copy in down_copies(lv + 1, tier):
                    copy.wait_recv()

                def place_body(col, start, size):
                    where = pl.ds(at_row(col, start), size)
                    keep = below(start, size, quarter * fine_own)
                    for comp, (ref, half, to) in enumerate(
                        ((b_u, half_u, x_u), (b_v, half_v, x_v))
                    ):
                        got = down_recv[lv][comp, col - 1, pl.ds(start, size), :]
                        new = jnp.where(keep, got, ref[where, :])
                        ref[where, :] = new
                        to[where, :] = half[where, :] * new

                over(1, columns, rows, SIDE, place_body, 4 if rows[1] <= 64 else 1)
                if lv == 1:
                    halos()
            if lv == 0:
                return
            first, count = (0, columns + 2) if lv == 1 else (1, columns)
            if lv == tier == 2:
                first, count = lambda i: 1 + 3 * i, 2
            shift(x_u, x_v, rows, first, count)
            over(first, count, RESIDUAL_ROWS[lv][tier], 64, residual_body, 2)
            send_down(tier, range(columns // 2))

        def residual_body(col, start, size):
            base = at_row(col, start)
            _, _, r_u, r_v = residual_at(x_u, x_v, base, size)
            y_u[pl.ds(base, size), :] = r_u
            y_v[pl.ds(base, size), :] = r_v

        def send_down(tier, which):
            low, high = RESIDUAL_ROWS[lv][tier]
            low, high = low // 2, high // 2
            pairs = columns // 2
            def join_halo(low, high):
                join_pair(0, (columns + 1, 0), halo_sum)

            def join_pair(k, pair=None, to=None):
                pair = (2 * k + 1, 2 * k + 2) if pair is None else pair
                to = down_send[lv].at[:, k] if to is None else to

                def join_body(_, start, size):
                    for comp, ref in enumerate((y_u, y_v)):
                        total = None
                        for half in range(2):
                            base = at_row(pair[half], 2 * start)
                            lines = (
                                ref[pl.ds(base, size, stride=2), :]
                                + ref[pl.ds(base + 1, size, stride=2), :]
                            )
                            term = split_dot(lines, joins[half])
                            total = term if total is None else total + term
                        to[comp, pl.ds(start, size), :] = total

                over(0, 1, (low, high), 64, join_body)
            def start_pairs(ks):
                for copy in down_copies(lv, tier, ks):
                    copy.start()
                    pending.append((copy, None))

            outer = tuple(k for k in sorted({0, pairs - 1}) if k in which)
            for k in outer:
                join_pair(k)
            if lv == 1:
                start_pairs(outer)
                join_halo(low, high)
            if lv > 1 and 0 in which:
                for side in range(2):
                    k = 0 if side == 0 else pairs - 1
                    three = slice(0, 3) if side == 0 else slice(SIDE - 3, SIDE)
                    lines = min(SIDE, tall // 2)
                    parts = []
                    for comp in range(2):
                        block_t = jnp.transpose(down_send[lv][comp, k, pl.ds(0, lines), :])
                        line = block_t[three]
                        if lines < SIDE:
                            line = jnp.concatenate([line, line], axis=1)
                        parts.append(line)
                    parts.append(jnp.zeros((2, SIDE), F32))
                    down_edge_send[tier, side] = jnp.concatenate(parts, axis=0)
                start_edges(down_edge, lv, tier)
            if lv > 1:
                start_pairs(outer)
            for k in range(1, pairs - 1):
                if k in which:
                    join_pair(k)
                    start_pairs((k,))

        def up(tier):
            low, high = SENT_UP[lv - 1][tier]
            if lv == 1:
                halo_up(tier)
            if lv > 1:
                for copy in up_copies(lv - 1, tier):
                    copy.wait_recv()
            prolong(tier, 0, columns // 2)
            rows = SMOOTH_ROWS[lv][tier]
            fine = (2 * low, 2 * high)
            if lv == 2 and tier == 3:
                copies = up_copies(lv, tier)

                def ready(col):
                    for copy in copies[2 * col - 2 : 2 * col]:
                        copy.start()

                shift(z_u, z_v, fine, 2, 2)
                for col in (2, 3):
                    over(col, 1, rows, 64, smooth_body)
                    ready(col)
                halo_up(tier)
                shift(z_u, z_v, fine, lambda i: 1 + 3 * i, 2)
                over(lambda i: 1 + 3 * i, 2, rows, 64, smooth_body, 2)
                fill_up_edges(tier)
                start_edges(up_edge, lv, tier)
                for col in (1, 4):
                    ready(col)
                pending.extend((copy, None) for copy in copies)
                return
            if lv > 1:
                halo_up(tier)
            shift(z_u, z_v, fine)
            over(1, columns, rows, 64, smooth_body, 2)

        def smooth_body(col, start, size):
            base = at_row(col, start)
            where = pl.ds(base, size)
            u, v, r_u, r_v = residual_at(z_u, z_v, base, size)
            u = u + half_u[where, :] * r_u
            v = v + half_v[where, :] * r_v
            if lv < levels - 1:
                y_u[where, :] = u
                y_v[where, :] = v
                return
            slot = col - 1
            lines = pl.ds(start, size)
            live = alive(0, own_rows)
            out_ref[slot, 0, lines, :] = u
            out_ref[slot, 1, lines, :] = v
            product = (
                velocity[slot, 0, lines, :].astype(F32) * u
                + velocity[slot, 1, lines, :].astype(F32) * v
            )
            grad_ref[slot, lines, :] = (
                -(friction[slot, lines, :].astype(F32) * product) * live
            ).astype(BF16)

        def up_last():
            tier = levels - 1
            rows = (0, tall)
            copies = up_copies(lv - 1, tier)
            def columns_done(first, count):
                shift(z_u, z_v, rows, first, count)
                over(first, count, rows, 64, smooth_body, 2)

            for k in (1, 2, 0, 3):
                for copy in copies[2 * k : 2 * k + 2]:
                    copy.wait_recv()
                prolong(tier, k, 1)
                if k == 2:
                    columns_done(4, 2)
                if k == 0:
                    columns_done(2, 2)
                    halo_up(tier)
                    columns_done(1, 1)
            columns_done(6, 3)

        def halo_up(tier, which=(0, 1)):
            low, high = SENT_UP[lv - 1][tier]
            if lv == 1:
                def halo_body(_, start, size):
                    limit = quarter * jnp.where(lane[:size] < quarter, east_rows, west_rows)
                    keep = lax.broadcasted_iota(jnp.int32, (size, SIDE), 0) + start < limit
                    for comp, (ref, to) in enumerate(((x_u, z_u), (x_v, z_v))):
                        lines = pl.ds(start, size)
                        wide = known_halo[comp, lines, :] * halo_sum[comp, lines, :]
                        wide = jnp.where(keep, wide, 0.0)
                        for col in (0, columns + 1):
                            for step in range(2):
                                where = pl.ds(at_row(col, 2 * start) + step, size, stride=2)
                                to[where, :] = ref[where, :] + wide

                over(0, 1, (low, high), 64, halo_body)
                return
            wait_edges(up_edge, lv - 1, tier, which)
            for side in which:
                col = columns + 1 if side == 0 else 0
                limit = quarter * (east_rows if side == 0 else west_rows)
                tile_t = jnp.transpose(up_edge_recv[tier, side])
                for part in range(2):
                    first, last = max(low, part * SIDE), min(high, (part + 1) * SIDE)
                    if first >= last:
                        continue
                    size = last - first
                    keep = below(first, size, limit)
                    for comp, (ref, to) in enumerate(((x_u, z_u), (x_v, z_v))):
                        wide = spread(tile_t, 2 * comp + part, first - part * SIDE, size)
                        wide = jnp.where(keep, wide, 0.0)
                        for step in range(2):
                            where = pl.ds(at_row(col, 2 * first) + step, size, stride=2)
                            to[where, :] = ref[where, :] + wide

        def prolong(tier, first, count):
            low, high = SENT_UP[lv - 1][tier]

            def prolong_body(k, start, size):
                keep = below(start, size, quarter * own_rows)
                for comp, (ref, to) in enumerate(((x_u, z_u), (x_v, z_v))):
                    coarse = up_recv[lv][comp, k, pl.ds(start, size), :]
                    if lv == 1:
                        coarse = coarse * down_send[1][comp, k, pl.ds(start, size), :]
                    coarse = jnp.where(keep, coarse, 0.0)
                    for half in range(2):
                        base = at_row(2 * k + half + 1, 2 * start)
                        wide = split_dot(coarse, spreads[half])
                        for step in range(2):
                            where = pl.ds(base + step, size, stride=2)
                            to[where, :] = ref[where, :] + wide

            over(first, count, (low, high), 64, prolong_body, 2)

        if lv == 2 and early:
            if early == 1:
                lax.fori_loop(2, 10, coefficients, 0)
                over(1, columns, START_ROWS[2][2], SIDE, start_body, 2)
                return
            shift(x_u, x_v, START_ROWS[2][2], 2, 2)
            over(2, 2, RESIDUAL_ROWS[2][2], 64, residual_body, 2)
            return
        if lv == levels - 1:
            if early:
                if early == 1:
                    lax.fori_loop(1, columns + 1, coefficients, 0)
                    over(1, columns, (0, tall), SIDE, start_body, 2)
                    shift(x_u, x_v, (0, tall), 2, columns - 2)
                    return
                over(3, columns - 4, (0, tall), 64, residual_body, 2)
                send_down(lv, (1, 2))
                over(lambda i: 2 + 5 * i, 2, (0, tall), 64, residual_body, 2)
                return
            ends = lambda i: jnp.where(i < 2, i, i + 6)
            inner = lambda i: 1 + 7 * i
            lax.fori_loop(0, 4, lambda i, carry: coefficients(ends(i), carry), 0)
            over(ends, 4, (0, tall), SIDE, start_body)
            shift(x_u, x_v, (0, tall), inner, 2)
            over(inner, 2, (0, tall), 64, residual_body, 2)
            send_down(lv, (0, 3))
            pending.extend((copy, None) for copy in down_copies(lv, lv, (1, 2)))
            loads[3].wait()
            up_last()
        else:
            if lv == 0:
                for copy in known_copies():
                    copy.start()
                    pending.append((copy, None))
                for side, lines in enumerate(edges_of((half_u, half_v), 0, 2 * SIDE)):
                    lines.append(jnp.zeros((4, SIDE), F32))
                    base_edge_send[side] = jnp.concatenate(lines, axis=0)
                start_edges(base_edge, lv, 0)
            for word in ORDER[lv]:
                if word == "known0":
                    known()
                    continue
                {"down": down, "up": up, "send": send_up}[word[:-1]](int(word[-1]))
            loads[3].wait()

        finals = (x_u, x_v) if lv == 0 else (y_u, y_v)

        def finish(col, start, size):
            base = at_row(col, start)
            row = start // SIDE
            slot = row * columns + col - 1
            live = alive(row, own_rows)
            u = finals[0][pl.ds(base, size), :]
            v = finals[1][pl.ds(base, size), :]
            out_ref[slot, 0] = u
            out_ref[slot, 1] = v
            product = velocity[slot, 0].astype(F32) * u + velocity[slot, 1].astype(F32) * v
            grad_ref[slot] = (-(friction[slot].astype(F32) * product) * live).astype(BF16)

        if lv < levels - 1:
            over(1, columns, (0, tall), SIDE, finish)
        for copy, there in pending:
            if there is None:
                copy.wait_send()
            else:

                @pl.when(there)
                def _(copy=copy):
                    copy.wait_send()

    for lv in (2, 3):

        @pl.when(level == lv)
        def _(lv=lv):
            program(lv, 1)

    pl.semaphore_wait(barrier, count)
    init_each(lambda copy: copy.start(), False)

    for lv in (2, 3):

        @pl.when(level == lv)
        def _(lv=lv):
            program(lv, 2)

    @pl.when(jnp.logical_not(has_east))
    def _():
        init_recv[0] = jnp.ones((SLOTS, 16, SIDE), F32)

    @pl.when(jnp.logical_not(has_west))
    def _():
        init_recv[1] = jnp.ones((SLOTS, 16, SIDE), F32)

    init_each(lambda copy: copy.wait_recv(), True)

    def unpack_halo(row, carry):
        for side in range(2):
            col = cols + 1 if side == 0 else 0
            base = base_of(jnp.int32(0) + col, row)
            live = alive(row, east_rows if side == 0 else west_rows)
            tile_t = columns_of(init_recv[side, row])

            def place(first, width, other):
                valid = lane < width if side == 0 else lane >= SIDE - width
                return jnp.where(valid, lanes_from(tile_t, side, first, width), other)

            mu[pl.ds(base, SIDE), :] = place(0, 4, 0.0) * live
            fric[pl.ds(base, SIDE), :] = place(4, 3, 1.0)
            b_u[pl.ds(base, SIDE), :] = place(7, 3, 0.0) * live
            b_v[pl.ds(base, SIDE), :] = place(10, 3, 0.0) * live
        return carry

    lax.fori_loop(0, prows, unpack_halo, 0)

    @pl.when(level < 2)
    def _():
        first = jnp.where(level == 0, prows, 0)
        last = jnp.where(level == 0, 2 * prows, (cols + 2) * prows)
        lax.fori_loop(first, last, coefficients, 0)

    for lv in range(levels):

        @pl.when(level == lv)
        def _(lv=lv):
            program(lv, 0)

    init_each(lambda copy: copy.wait_send(), False)


def write_out(adjoint, gradient, adjoint_hbm, gradient_hbm, sem):
    copies = [
        pltpu.make_async_copy(adjoint, adjoint_hbm, sem.at[0]),
        pltpu.make_async_copy(gradient, gradient_hbm, sem.at[1]),
    ]
    for copy in copies:
        copy.start()
    for copy in copies:
        copy.wait()


def per_device(levels, patches, forcing, velocity, viscosity, friction, patch_rows):
    tall = pltpu.VMEM((TALL, SIDE), F32)
    vmem = pl.BlockSpec(memory_space=pltpu.VMEM)
    coarse = {
        sender: pltpu.VMEM((2, 2**sender // 2, SLOTS // 2**sender * SIDE // 2, SIDE), F32)
        for sender in range(1, levels)
    }
    adjoint, gradient = pl.pallas_call(
        functools.partial(kernel, levels, patches),
        out_shape=(
            jax.ShapeDtypeStruct((SLOTS, 2, SIDE, SIDE), F32),
            jax.ShapeDtypeStruct((SLOTS, SIDE, SIDE), BF16),
        ),
        in_specs=[pl.BlockSpec(memory_space=pltpu.HBM)] * 5,
        out_specs=(vmem, vmem),
        scratch_shapes=[
            pltpu.SMEM((levels, patches), jnp.int32),
            pltpu.VMEM((SLOTS, 2, SIDE, SIDE), BF16),
            pltpu.VMEM((SLOTS, 2, SIDE, SIDE), BF16),
            pltpu.VMEM((SLOTS, SIDE, SIDE), F32),
            pltpu.VMEM((SLOTS, SIDE, SIDE), BF16),
        ]
        + [tall] * 20
        + [
            pltpu.VMEM((2, SLOTS, 16, SIDE), F32),
            pltpu.VMEM((2, SLOTS, 16, SIDE), F32),
        ]
        + [coarse[sender] for sender in range(1, levels)] * 3
        + [pltpu.VMEM((4, 2, 8, SIDE), F32)] * 4
        + [pltpu.VMEM((2, 2 * SIDE, SIDE), F32)] * 2
        + [pltpu.VMEM((2, 8, SIDE), F32)] * 2
        + [
            pltpu.SemaphoreType.DMA((5,)),
            pltpu.SemaphoreType.DMA((4,)),
            pltpu.SemaphoreType.DMA((2, 16)),
            pltpu.SemaphoreType.DMA((2, 8)),
            pltpu.SemaphoreType.DMA((2, 32)),
            pltpu.SemaphoreType.DMA((2, 8)),
            pltpu.SemaphoreType.DMA((4,)),
        ],
        compiler_params=pltpu.CompilerParams(
            collective_id=0, has_side_effects=True, vmem_limit_bytes=44 << 20
        ),
    )(
        *(
            pltpu.with_memory_space_constraint(x, pltpu.HBM)
            for x in (patch_rows, forcing[0], velocity[0], viscosity[0], friction[0])
        )
    )
    adjoint, gradient = pl.pallas_call(
        write_out,
        out_shape=(
            jax.ShapeDtypeStruct(adjoint.shape, adjoint.dtype),
            jax.ShapeDtypeStruct(gradient.shape, gradient.dtype),
        ),
        in_specs=[vmem, vmem],
        out_specs=(pl.BlockSpec(memory_space=pltpu.HBM),) * 2,
        scratch_shapes=[pltpu.SemaphoreType.DMA((2,))],
        compiler_params=pltpu.CompilerParams(vmem_limit_bytes=4 << 20),
    )(adjoint, gradient)
    return adjoint[None], gradient[None]


def solution(mesh):
    in_specs = (
        P("level", "patch", None, None, None),
        P("level", "patch", None, None, None),
        P("level", "patch", None, None),
        P("level", "patch", None, None),
        P(),
    )
    out_specs = (P("level", "patch", None, None, None), P("level", "patch", None, None))
    return jax.shard_map(
        functools.partial(per_device, mesh.shape["level"], mesh.shape["patch"]),
        mesh=mesh,
        in_specs=in_specs,
        out_specs=out_specs,
        check_vma=False,
    )
```

```python
import functools

import jax
import jax.numpy as jnp
from jax import lax
from jax.experimental import pallas as pl
from jax.experimental.pallas import tpu as pltpu
from jax.sharding import PartitionSpec as P

MESH = pl.DeviceIdType.MESH
F32 = jnp.float32
BF16 = jnp.bfloat16
SIDE = 128
SLOTS = 8
PAD = 8
TALL = 3 * (SLOTS * SIDE + 2 * PAD)


def split_dot(x, matrix):
    high = x.astype(BF16)
    low = (x - high.astype(F32)).astype(BF16)
    return jnp.dot(high, matrix, preferred_element_type=F32) + jnp.dot(
        low, matrix, preferred_element_type=F32
    )


START_ROWS = {
    0: {0: (256, 1024), 1: (72, 256), 2: (24, 72), 3: (0, 24)},
    1: {1: (128, 512), 2: (40, 128), 3: (0, 40)},
    2: {2: (64, 256), 3: (0, 64)},
    3: {3: (0, 128)},
}
RESIDUAL_ROWS = {
    1: {1: (144, 512), 2: (48, 144), 3: (0, 48)},
    2: {2: (80, 256), 3: (0, 80)},
    3: {3: (0, 128)},
}
SMOOTH_ROWS = {
    1: {1: (136, 512), 2: (56, 136), 3: (0, 56)},
    2: {2: (64, 256), 3: (0, 64)},
    3: {3: (0, 128)},
}
SENT_UP = {
    0: {1: (72, 256), 2: (24, 72), 3: (0, 24)},
    1: {2: (40, 128), 3: (0, 40)},
    2: {3: (0, 64)},
}
ORDER = {
    0: ("down0", "down1", "down2", "down3"),
    1: ("down1", "down2", "known0", "down3", "up2", "up3", "send3", "send2", "up1"),
    2: ("down2", "down3", "up3", "up2"),
}


def over(col_at, col_count, rows, most, body, group=1):
    low, high = rows
    pieces = -(-(high - low) // most)
    size = -(-(high - low) // (8 * pieces)) * 8
    total = col_count * pieces

    def step(index):
        if isinstance(index, int):
            col, part = divmod(index, pieces)
            start = min(low + part * size, high - size)
        else:
            col = index // pieces
            part = index - col * pieces
            start = low if pieces == 1 else jnp.minimum(low + part * size, high - size)
        body(col_at + col if isinstance(col_at, int) else col_at(col), start, size)

    def steps(index, carry):
        for inner in range(group):
            step(index * group + inner)
        return carry

    done = 0
    if total > group:
        lax.fori_loop(0, total // group, steps, 0)
        done = total // group * group
    for index in range(done, total):
        step(index)


def kernel(
    levels,
    patches,
    rows_hbm,
    forcing_hbm,
    velocity_hbm,
    viscosity_hbm,
    friction_hbm,
    out_ref,
    grad_ref,
    rows_ref,
    forcing,
    velocity,
    viscosity,
    friction,
    mu,
    fric,
    mu_e,
    mu_w,
    diag_u,
    diag_v,
    half_u,
    half_v,
    b_u,
    b_v,
    x_u,
    x_v,
    z_u,
    z_v,
    ue,
    uw,
    ve,
    vw,
    y_u,
    y_v,
    init_send,
    init_recv,
    down_send_1,
    down_send_2,
    down_send_3,
    down_recv_0,
    down_recv_1,
    down_recv_2,
    up_recv_1,
    up_recv_2,
    up_recv_3,
    down_edge_send,
    down_edge_recv,
    up_edge_send,
    up_edge_recv,
    halo_sum,
    known_halo,
    base_edge_send,
    base_edge_recv,
    load_sem,
    init_sem,
    down_sem,
    down_edge_sem,
    up_sem,
    up_edge_sem,
    base_edge_sem,
):
    down_send = {1: down_send_1, 2: down_send_2, 3: down_send_3}
    down_recv = {0: down_recv_0, 1: down_recv_1, 2: down_recv_2}
    up_recv = {1: up_recv_1, 2: up_recv_2, 3: up_recv_3}
    level = lax.axis_index("level")
    patch = lax.axis_index("patch")
    cols = jnp.where(level == 0, 1, jnp.where(level == 1, 2, jnp.where(level == 2, 4, 8)))
    prows = jnp.where(level == 0, 8, jnp.where(level == 1, 4, jnp.where(level == 2, 2, 1)))
    height = prows * SIDE
    pitch = height + 2 * PAD
    has_west = patch > 0
    has_east = patch < patches - 1
    finer = jnp.minimum(level + 1, levels - 1)
    west = jnp.maximum(patch - 1, 0)
    east = jnp.minimum(patch + 1, patches - 1)
    loads = [
        pltpu.make_async_copy(src, dst, load_sem.at[i])
        for i, (src, dst) in enumerate(
            (
                (viscosity_hbm, viscosity),
                (friction_hbm, friction),
                (forcing_hbm, forcing),
                (velocity_hbm, velocity),
                (rows_hbm, rows_ref),
            )
        )
    ]
    for load in loads:
        load.start()

    barrier = pltpu.get_barrier_semaphore()
    count = jnp.int32(0)
    for dl in (-1, 0, 1):
        for dp in (-1, 0, 1):
            if (dl == 0) == (dp == 0):
                continue
            there = (level + dl >= 0) & (level + dl < levels) & (patch + dp >= 0) & (patch + dp < patches)
            count = count + jnp.where(there, 1, 0)

            @pl.when(there)
            def _(dl=dl, dp=dp):
                pl.semaphore_signal(
                    barrier,
                    inc=1,
                    device_id={"level": level + dl, "patch": patch + dp},
                    device_id_type=MESH,
                )

    def base_of(col, row):
        return pl.multiple_of((col * pitch + PAD + row * SIDE).astype(jnp.int32), 8)

    def alive(row, total):
        return jnp.where(row < total, 1.0, 0.0).astype(F32)

    lane = lax.broadcasted_iota(jnp.int32, (SIDE, SIDE), 1)

    zeros = jnp.zeros((PAD, SIDE), F32)

    def clear(col, carry):
        first = pl.multiple_of(col * pitch, 8)
        last = pl.multiple_of(col * pitch + PAD + height, 8)
        for ref in (mu, x_u, x_v, z_u, z_v, ue, uw, ve, vw):
            ref[pl.ds(first, PAD), :] = zeros
            ref[pl.ds(last, PAD), :] = zeros
        return carry

    lax.fori_loop(0, cols + 2, clear, 0)

    loads[4].wait()
    own_rows = rows_ref[level, patch]
    west_rows = jnp.where(has_west, rows_ref[level, west], 0)
    east_rows = jnp.where(has_east, rows_ref[level, east], 0)
    fine_own = rows_ref[finer, patch]
    fine_west = jnp.where(has_west, rows_ref[finer, west], 0)
    fine_east = jnp.where(has_east, rows_ref[finer, east], 0)

    for load in loads[:3]:
        load.wait()

    def unpack(slot_id, carry):
        col = slot_id // prows
        row = slot_id - col * prows
        base = base_of(col + 1, row)
        slot = row * cols + col
        live = alive(row, own_rows)
        mu[pl.ds(base, SIDE), :] = viscosity[slot] * live
        fric[pl.ds(base, SIDE), :] = friction[slot].astype(F32)
        b_u[pl.ds(base, SIDE), :] = forcing[slot, 0].astype(F32) * live
        b_v[pl.ds(base, SIDE), :] = forcing[slot, 1].astype(F32) * live
        return carry

    lax.fori_loop(0, SLOTS, unpack, 0)

    def pack(row, carry):
        for side in range(2):
            base = base_of(jnp.where(side == 0, 1, cols), row)
            four = slice(0, 4) if side == 0 else slice(SIDE - 4, SIDE)
            three = slice(0, 3) if side == 0 else slice(SIDE - 3, SIDE)
            mu_t = jnp.transpose(mu[pl.ds(base, SIDE), :])
            fr_t = jnp.transpose(fric[pl.ds(base, SIDE), :])
            bu_t = jnp.transpose(b_u[pl.ds(base, SIDE), :])
            bv_t = jnp.transpose(b_v[pl.ds(base, SIDE), :])
            parts = [
                mu_t[four],
                fr_t[three],
                bu_t[three],
                bv_t[three],
                jnp.zeros((3, SIDE), F32),
            ]
            init_send[side, row] = jnp.concatenate(parts, axis=0)
        return carry

    lax.fori_loop(0, prows, pack, 0)


    def copy_to(src, dst, send, recv, there, dp):
        return pltpu.make_async_remote_copy(
            src_ref=src,
            dst_ref=dst,
            send_sem=send,
            recv_sem=recv,
            device_id={"level": there, "patch": patch + dp},
            device_id_type=MESH,
        )

    def init_copies(lv, side):
        used = pl.ds(0, SLOTS // 2**lv)
        return copy_to(
            init_send.at[side, used],
            init_recv.at[side, used],
            init_sem.at[side],
            init_sem.at[2 + side],
            lv,
            -1 if side == 0 else 1,
        )

    def init_each(act, flip, which=range(levels), sides=(0, 1)):
        for lv in which:
            for side in sides:
                there = has_west if (side == 0) != flip else has_east

                @pl.when((level == lv) & there)
                def _(lv=lv, side=side):
                    act(init_copies(lv, side))


    def columns_of(tile):
        blank = jnp.zeros((SIDE - tile.shape[0], SIDE), F32)
        return jnp.transpose(jnp.concatenate([tile, blank], axis=0))

    def lanes_from(tile_t, side, first, width):
        steps = (-first if side == 0 else SIDE - width - first) % SIDE
        return tile_t if steps == 0 else pltpu.roll(tile_t, steps, 1)

    def spread(tile_t, index, first=0, count=SIDE):
        return jnp.broadcast_to(tile_t[first : first + count, index : index + 1], (count, SIDE))

    def coefficients(index, carry):
        col = index // prows
        row = index - col * prows
        base = base_of(col, row)
        to_east = pl.multiple_of(base + jnp.where(col == cols + 1, 0, pitch), 8)
        to_west = pl.multiple_of(base - jnp.where(col == 0, 0, pitch), 8)
        total = jnp.where(col == 0, west_rows, jnp.where(col == cols + 1, east_rows, own_rows))
        live = 0.5 * alive(row, total)
        here = mu[pl.ds(base, SIDE), :]
        m_e = pltpu.roll(jnp.where(lane == 0, mu[pl.ds(to_east, SIDE), :], here), SIDE - 1, 1)
        m_w = pltpu.roll(jnp.where(lane == SIDE - 1, mu[pl.ds(to_west, SIDE), :], here), 1, 1)
        across = m_e + m_w + 2.0 * here
        along = mu[pl.ds(base + 1, SIDE), :] + mu[pl.ds(base - 1, SIDE), :] + 2.0 * here
        fr = fric[pl.ds(base, SIDE), :]
        d_u = 2.0 * across + 0.5 * along + fr
        d_v = 2.0 * along + 0.5 * across + fr
        mu_e[pl.ds(base, SIDE), :] = m_e
        mu_w[pl.ds(base, SIDE), :] = m_w
        diag_u[pl.ds(base, SIDE), :] = d_u
        diag_v[pl.ds(base, SIDE), :] = d_v
        half_u[pl.ds(base, SIDE), :] = live / d_u
        half_v[pl.ds(base, SIDE), :] = live / d_v
        return carry

    quarter = SIDE // 2
    lane_row = lax.broadcasted_iota(jnp.int32, (SIDE, SIDE), 0)
    joins = [
        jnp.where(lane_row // 2 + half * quarter == lane, 1.0, 0.0).astype(BF16)
        for half in range(2)
    ]
    spreads = [
        jnp.where(lane // 2 + half * quarter == lane_row, 1.0, 0.0).astype(BF16)
        for half in range(2)
    ]

    def program(lv, early):
        columns = 2**lv
        tall = SLOTS // columns * SIDE
        step_col = tall + 2 * PAD
        pending = []

        def at_row(col, row):
            return pl.multiple_of(col * step_col + PAD + row, 8)

        def below(start, size, limit):
            rows = lax.broadcasted_iota(jnp.int32, (size, SIDE), 0) + start
            return rows < limit

        def shift(src_u, src_v, rows, first=1, count=columns):
            def body(col, start, size):
                base = at_row(col, start)
                to_east = pl.multiple_of(base + jnp.where(col == columns + 1, 0, step_col), 8)
                to_west = pl.multiple_of(base - jnp.where(col == 0, 0, step_col), 8)
                here_lane = lane[:size]
                for src, dst_e, dst_w in ((src_u, ue, uw), (src_v, ve, vw)):
                    here = src[pl.ds(base, size), :]
                    dst_e[pl.ds(base, size), :] = pltpu.roll(
                        jnp.where(here_lane == 0, src[pl.ds(to_east, size), :], here), SIDE - 1, 1
                    )
                    dst_w[pl.ds(base, size), :] = pltpu.roll(
                        jnp.where(here_lane == SIDE - 1, src[pl.ds(to_west, size), :], here), 1, 1
                    )

            over(first, count, rows, SIDE, body, 4 if rows[1] - rows[0] <= 80 else 2)

        def residual_at(src_u, src_v, base, size):
            def at(ref, step=0):
                return ref[pl.ds(base + step, size), :]

            m, m_e, m_w, m_n, m_s = at(mu), at(mu_e), at(mu_w), at(mu, 1), at(mu, -1)
            p_e, p_w, p_n, p_s = m + m_e, m + m_w, m + m_n, m + m_s
            ue_n, ue_s, uw_n, uw_s = at(ue, 1), at(ue, -1), at(uw, 1), at(uw, -1)
            ve_n, ve_s, vw_n, vw_s = at(ve, 1), at(ve, -1), at(vw, 1), at(vw, -1)
            u, v = at(src_u), at(src_v)
            cross_u = 0.5 * (m_e * (ve_n - ve_s) - m_w * (vw_n - vw_s)) + 0.25 * (
                m_n * (ve_n - vw_n) - m_s * (ve_s - vw_s)
            )
            cross_v = 0.5 * (m_n * (ue_n - uw_n) - m_s * (ue_s - uw_s)) + 0.25 * (
                m_e * (ue_n - ue_s) - m_w * (uw_n - uw_s)
            )
            near_u = 2.0 * (p_e * at(ue) + p_w * at(uw)) + 0.5 * (
                p_n * at(src_u, 1) + p_s * at(src_u, -1)
            )
            near_v = 2.0 * (p_n * at(src_v, 1) + p_s * at(src_v, -1)) + 0.5 * (
                p_e * at(ve) + p_w * at(vw)
            )
            r_u = at(b_u) - (at(diag_u) * u - near_u - cross_u)
            r_v = at(b_v) - (at(diag_v) * v - near_v - cross_v)
            return u, v, r_u, r_v

        def sides():
            return ((0, has_west, has_east, -1), (1, has_east, has_west, 1))

        def down_copies(sender, tier, which=None):
            low, high = RESIDUAL_ROWS[sender][tier]
            low, high = low // 2, high // 2
            copies = []
            for k in range(2**sender // 2) if which is None else which:
                part = (slice(None), k, pl.ds(low, high - low))
                copies.append(
                    copy_to(
                        down_send[sender].at[part],
                        down_recv[sender - 1].at[part],
                        down_sem.at[0, tier * 4 + k],
                        down_sem.at[1, tier * 4 + k],
                        sender - 1,
                        0,
                    )
                )
            return copies

        def down_edge(sender, tier, side, dp):
            return copy_to(
                down_edge_send.at[tier, side],
                down_edge_recv.at[tier, side],
                down_edge_sem.at[0, tier * 2 + side],
                down_edge_sem.at[1, tier * 2 + side],
                sender - 1,
                dp,
            )

        def up_copies(sender, tier):
            low, high = SENT_UP[sender][tier]
            sources = (x_u, x_v) if sender == 0 else (y_u, y_v)
            pitch_here = SLOTS // 2**sender * SIDE + 2 * PAD
            copies = []
            for k in range(2**sender):
                for comp in range(2):
                    index = tier * 8 + k * 2 + comp
                    copies.append(
                        copy_to(
                            sources[comp].at[pl.ds((k + 1) * pitch_here + PAD + low, high - low)],
                            up_recv[sender + 1].at[comp, k, pl.ds(low, high - low)],
                            up_sem.at[0, index],
                            up_sem.at[1, index],
                            sender + 1,
                            0,
                        )
                    )
            return copies

        def up_edge(sender, tier, side, dp):
            return copy_to(
                up_edge_send.at[tier, side],
                up_edge_recv.at[tier, side],
                up_edge_sem.at[0, tier * 2 + side],
                up_edge_sem.at[1, tier * 2 + side],
                sender + 1,
                dp,
            )

        def known_copies():
            rows = 2 * SIDE
            return [
                copy_to(
                    ref.at[pl.ds(SLOTS * SIDE + 2 * PAD + PAD, rows)],
                    up_recv[1].at[comp, 0, pl.ds(0, rows)],
                    up_sem.at[0, comp],
                    up_sem.at[1, comp],
                    1,
                    0,
                )
                for comp, ref in enumerate((half_u, half_v))
            ]

        def known():
            wait_edges(base_edge, 0, 0)
            tiles = [jnp.transpose(base_edge_recv[side]) for side in range(2)]
            for comp in range(2):
                for part in range(2):
                    index = 2 * comp + part
                    known_halo[comp, pl.ds(part * SIDE, SIDE), :] = jnp.where(
                        lane < quarter, spread(tiles[0], index), spread(tiles[1], index)
                    )
            for copy in known_copies():
                copy.wait_recv()

        def base_edge(sender, tier, side, dp):
            return copy_to(
                base_edge_send.at[side],
                base_edge_recv.at[side],
                base_edge_sem.at[side],
                base_edge_sem.at[2 + side],
                1,
                dp,
            )

        def edges_of(refs, low, high):
            blocks = []
            for ref in refs:
                for part in range(2):
                    if part * SIDE < high and low < (part + 1) * SIDE:
                        rows = pl.ds(at_row(1, part * SIDE), SIDE)
                        blocks.append(jnp.transpose(ref[rows, :]))
            return [
                [block[near : near + 1] for block in blocks] for near in (0, SIDE - 1)
            ]

        def start_edges(make, sender, tier, which=(0, 1)):
            for side, there, _, dp in sides():
                if side not in which:
                    continue
                copy = make(sender, tier, side, dp)

                @pl.when(there)
                def _(copy=copy):
                    copy.start()

                pending.append((copy, there))

        def wait_edges(make, sender, tier, which=(0, 1)):
            for side, _, there, dp in sides():
                if side not in which:
                    continue
                copy = make(sender, tier, side, dp)

                @pl.when(there)
                def _(copy=copy):
                    copy.wait_recv()

        def fill_up_edges(tier, which=(0, 1)):
            low, high = SENT_UP[lv][tier]
            sources = (x_u, x_v) if lv == 0 else (y_u, y_v)
            for side in which:
                col = 1 if side == 0 else columns
                near = 0 if side == 0 else SIDE - 1
                parts = []
                for ref in sources:
                    for part in range(2):
                        if part * SIDE < high and low < (part + 1) * SIDE:
                            block_t = jnp.transpose(ref[pl.ds(at_row(col, part * SIDE), SIDE), :])
                            parts.append(block_t[near : near + 1])
                        else:
                            parts.append(jnp.zeros((1, SIDE), F32))
                parts.append(jnp.zeros((4, SIDE), F32))
                up_edge_send[tier, side] = jnp.concatenate(parts, axis=0)

        def send_up(tier):
            fill_up_edges(tier)
            start_edges(up_edge, lv, tier)
            for copy in up_copies(lv, tier):
                copy.start()
                pending.append((copy, None))

        def start_body(col, start, size):
            where = pl.ds(at_row(col, start), size)
            x_u[where, :] = half_u[where, :] * b_u[where, :]
            x_v[where, :] = half_v[where, :] * b_v[where, :]

        def down(tier):
            rows = START_ROWS[lv][tier]
            low, high = rows
            if tier == lv:
                if lv == 2:
                    ends = lambda i: jnp.where(i < 2, i, i + 2)
                    lax.fori_loop(
                        0,
                        8,
                        lambda i, carry: coefficients(ends(i // 2) * 2 + i % 2, carry),
                        0,
                    )
                    for col in (0, 1, 4, 5):
                        over(col, 1, rows, SIDE, start_body, 2)
                elif lv == 0:
                    over(1, 1, rows, SIDE, start_body)
                else:
                    over(0, columns + 2, rows, SIDE, start_body)
            else:
                def halos():
                    wait_edges(down_edge, lv + 1, tier)
                    for side in range(2):
                        col = columns + 1 if side == 0 else 0
                        limit = quarter * (fine_east if side == 0 else fine_west)
                        tile_t = columns_of(down_edge_recv[tier, side])[low:high]
                        where = pl.ds(at_row(col, low), high - low)
                        keep = below(low, high - low, limit)
                        for comp, (ref, half, to) in enumerate(
                            ((b_u, half_u, x_u), (b_v, half_v, x_v))
                        ):
                            got = lanes_from(tile_t, side, 3 * comp, 3)
                            new = jnp.where(keep, got, ref[where, :])
                            ref[where, :] = new
                            to[where, :] = half[where, :] * new

                if lv == 2:
                    halos()
                for copy in down_copies(lv + 1, tier):
                    copy.wait_recv()

                def place_body(col, start, size):
                    where = pl.ds(at_row(col, start), size)
                    keep = below(start, size, quarter * fine_own)
                    for comp, (ref, half, to) in enumerate(
                        ((b_u, half_u, x_u), (b_v, half_v, x_v))
                    ):
                        got = down_recv[lv][comp, col - 1, pl.ds(start, size), :]
                        new = jnp.where(keep, got, ref[where, :])
                        ref[where, :] = new
                        to[where, :] = half[where, :] * new

                over(1, columns, rows, SIDE, place_body, 4 if rows[1] <= 64 else 1)
                if lv == 1:
                    halos()
            if lv == 0:
                return
            first, count = (0, columns + 2) if lv == 1 else (1, columns)
            if lv == tier == 2:
                first, count = lambda i: 1 + 3 * i, 2
            shift(x_u, x_v, rows, first, count)
            over(first, count, RESIDUAL_ROWS[lv][tier], 64, residual_body, 2)
            send_down(tier, range(columns // 2))

        def residual_body(col, start, size):
            base = at_row(col, start)
            _, _, r_u, r_v = residual_at(x_u, x_v, base, size)
            y_u[pl.ds(base, size), :] = r_u
            y_v[pl.ds(base, size), :] = r_v

        def send_down(tier, which):
            low, high = RESIDUAL_ROWS[lv][tier]
            low, high = low // 2, high // 2
            pairs = columns // 2
            def join_halo(low, high):
                join_pair(0, (columns + 1, 0), halo_sum)

            def join_pair(k, pair=None, to=None):
                pair = (2 * k + 1, 2 * k + 2) if pair is None else pair
                to = down_send[lv].at[:, k] if to is None else to

                def join_body(_, start, size):
                    for comp, ref in enumerate((y_u, y_v)):
                        total = None
                        for half in range(2):
                            base = at_row(pair[half], 2 * start)
                            lines = (
                                ref[pl.ds(base, size, stride=2), :]
                                + ref[pl.ds(base + 1, size, stride=2), :]
                            )
                            term = split_dot(lines, joins[half])
                            total = term if total is None else total + term
                        to[comp, pl.ds(start, size), :] = total

                over(0, 1, (low, high), 64, join_body)
            def start_pairs(ks):
                for copy in down_copies(lv, tier, ks):
                    copy.start()
                    pending.append((copy, None))

            outer = tuple(k for k in sorted({0, pairs - 1}) if k in which)
            for k in outer:
                join_pair(k)
            if lv == 1:
                start_pairs(outer)
                join_halo(low, high)
            edge_sides = [side for side, k in ((0, 0), (1, pairs - 1)) if k in which]
            if lv > 1 and edge_sides:
                for side in edge_sides:
                    k = 0 if side == 0 else pairs - 1
                    three = slice(0, 3) if side == 0 else slice(SIDE - 3, SIDE)
                    lines = min(SIDE, tall // 2)
                    parts = []
                    for comp in range(2):
                        block_t = jnp.transpose(down_send[lv][comp, k, pl.ds(0, lines), :])
                        line = block_t[three]
                        if lines < SIDE:
                            line = jnp.concatenate([line, line], axis=1)
                        parts.append(line)
                    parts.append(jnp.zeros((2, SIDE), F32))
                    down_edge_send[tier, side] = jnp.concatenate(parts, axis=0)
                start_edges(down_edge, lv, tier, edge_sides)
            if lv > 1:
                start_pairs(outer)
            for k in range(1, pairs - 1):
                if k in which:
                    join_pair(k)
                    start_pairs((k,))

        def up(tier):
            low, high = SENT_UP[lv - 1][tier]
            if lv == 1:
                halo_up(tier)
            if lv > 1:
                for copy in up_copies(lv - 1, tier):
                    copy.wait_recv()
            prolong(tier, 0, columns // 2)
            rows = SMOOTH_ROWS[lv][tier]
            fine = (2 * low, 2 * high)
            if lv == 2 and tier == 3:
                copies = up_copies(lv, tier)

                def ready(col):
                    for copy in copies[2 * col - 2 : 2 * col]:
                        copy.start()

                shift(z_u, z_v, fine, 2, 2)
                for col in (2, 3):
                    over(col, 1, rows, 64, smooth_body)
                    ready(col)
                halo_up(tier)
                shift(z_u, z_v, fine, lambda i: 1 + 3 * i, 2)
                over(lambda i: 1 + 3 * i, 2, rows, 64, smooth_body, 2)
                fill_up_edges(tier)
                start_edges(up_edge, lv, tier)
                for col in (1, 4):
                    ready(col)
                pending.extend((copy, None) for copy in copies)
                return
            if lv > 1:
                halo_up(tier)
            shift(z_u, z_v, fine)
            over(1, columns, rows, 64, smooth_body, 2)

        def smooth_body(col, start, size):
            base = at_row(col, start)
            where = pl.ds(base, size)
            u, v, r_u, r_v = residual_at(z_u, z_v, base, size)
            u = u + half_u[where, :] * r_u
            v = v + half_v[where, :] * r_v
            if lv < levels - 1:
                y_u[where, :] = u
                y_v[where, :] = v
                return
            slot = col - 1
            lines = pl.ds(start, size)
            live = alive(0, own_rows)
            out_ref[slot, 0, lines, :] = u
            out_ref[slot, 1, lines, :] = v
            product = (
                velocity[slot, 0, lines, :].astype(F32) * u
                + velocity[slot, 1, lines, :].astype(F32) * v
            )
            grad_ref[slot, lines, :] = (
                -(friction[slot, lines, :].astype(F32) * product) * live
            ).astype(BF16)

        def up_last():
            tier = levels - 1
            rows = (0, tall)
            copies = up_copies(lv - 1, tier)
            def columns_done(first, count):
                shift(z_u, z_v, rows, first, count)
                over(first, count, rows, 64, smooth_body, 2)

            for k in (1, 2, 0, 3):
                for copy in copies[2 * k : 2 * k + 2]:
                    copy.wait_recv()
                prolong(tier, k, 1)
                if k == 2:
                    columns_done(4, 2)
                if k == 0:
                    columns_done(2, 2)
                    halo_up(tier)
                    columns_done(1, 1)
            columns_done(6, 3)

        def halo_up(tier, which=(0, 1)):
            low, high = SENT_UP[lv - 1][tier]
            if lv == 1:
                def halo_body(_, start, size):
                    limit = quarter * jnp.where(lane[:size] < quarter, east_rows, west_rows)
                    keep = lax.broadcasted_iota(jnp.int32, (size, SIDE), 0) + start < limit
                    for comp, (ref, to) in enumerate(((x_u, z_u), (x_v, z_v))):
                        lines = pl.ds(start, size)
                        wide = known_halo[comp, lines, :] * halo_sum[comp, lines, :]
                        wide = jnp.where(keep, wide, 0.0)
                        for col in (0, columns + 1):
                            for step in range(2):
                                where = pl.ds(at_row(col, 2 * start) + step, size, stride=2)
                                to[where, :] = ref[where, :] + wide

                over(0, 1, (low, high), 64, halo_body)
                return
            wait_edges(up_edge, lv - 1, tier, which)
            for side in which:
                col = columns + 1 if side == 0 else 0
                limit = quarter * (east_rows if side == 0 else west_rows)
                tile_t = jnp.transpose(up_edge_recv[tier, side])
                for part in range(2):
                    first, last = max(low, part * SIDE), min(high, (part + 1) * SIDE)
                    if first >= last:
                        continue
                    size = last - first
                    keep = below(first, size, limit)
                    for comp, (ref, to) in enumerate(((x_u, z_u), (x_v, z_v))):
                        wide = spread(tile_t, 2 * comp + part, first - part * SIDE, size)
                        wide = jnp.where(keep, wide, 0.0)
                        for step in range(2):
                            where = pl.ds(at_row(col, 2 * first) + step, size, stride=2)
                            to[where, :] = ref[where, :] + wide

        def prolong(tier, first, count):
            low, high = SENT_UP[lv - 1][tier]

            def prolong_body(k, start, size):
                keep = below(start, size, quarter * own_rows)
                for comp, (ref, to) in enumerate(((x_u, z_u), (x_v, z_v))):
                    coarse = up_recv[lv][comp, k, pl.ds(start, size), :]
                    if lv == 1:
                        coarse = coarse * down_send[1][comp, k, pl.ds(start, size), :]
                    coarse = jnp.where(keep, coarse, 0.0)
                    for half in range(2):
                        base = at_row(2 * k + half + 1, 2 * start)
                        wide = split_dot(coarse, spreads[half])
                        for step in range(2):
                            where = pl.ds(base + step, size, stride=2)
                            to[where, :] = ref[where, :] + wide

            over(first, count, (low, high), 64, prolong_body, 2)

        if lv == 2 and early:
            if early == 1:
                lax.fori_loop(2, 10, coefficients, 0)
                over(1, columns, START_ROWS[2][2], SIDE, start_body, 2)
                return
            shift(x_u, x_v, START_ROWS[2][2], 2, 2)
            over(2, 2, RESIDUAL_ROWS[2][2], 64, residual_body, 2)
            return
        if lv == levels - 1:
            if early:
                if early == 1:
                    lax.fori_loop(1, columns + 1, coefficients, 0)
                    over(1, columns, (0, tall), SIDE, start_body, 2)
                    shift(x_u, x_v, (0, tall), 2, columns - 2)
                    return
                over(3, columns - 4, (0, tall), 64, residual_body, 2)
                send_down(lv, (1, 2))
                over(lambda i: 2 + 5 * i, 2, (0, tall), 64, residual_body, 2)
                return

            def end_of_row(side):
                init_each(lambda copy: copy.wait_recv(), True, (lv,), (side,))
                unpack_halo(0, 0, (side,))
                own = columns if side == 0 else 1
                for col in (own, columns + 1 if side == 0 else 0):
                    coefficients(jnp.int32(col), 0)
                over(min(own, own + 1 - 2 * side), 2, (0, tall), SIDE, start_body, 2)
                shift(x_u, x_v, (0, tall), own, 1)
                over(own, 1, (0, tall), 64, residual_body, 2)
                send_down(lv, (3,) if side == 0 else (0,))

            for parity in range(2):

                @pl.when(patch % 2 == parity)
                def _(parity=parity):
                    for side in (parity, 1 - parity):
                        end_of_row(side)

            pending.clear()
            pending.extend((copy, None) for copy in down_copies(lv, lv))
            for side, there, _, dp in sides():
                pending.append((down_edge(lv, lv, side, dp), there))
            loads[3].wait()
            up_last()
        else:
            if lv == 0:
                for copy in known_copies():
                    copy.start()
                    pending.append((copy, None))
                for side, lines in enumerate(edges_of((half_u, half_v), 0, 2 * SIDE)):
                    lines.append(jnp.zeros((4, SIDE), F32))
                    base_edge_send[side] = jnp.concatenate(lines, axis=0)
                start_edges(base_edge, lv, 0)
            for word in ORDER[lv]:
                if word == "known0":
                    known()
                    continue
                {"down": down, "up": up, "send": send_up}[word[:-1]](int(word[-1]))
            loads[3].wait()

        finals = (x_u, x_v) if lv == 0 else (y_u, y_v)

        def finish(col, start, size):
            base = at_row(col, start)
            row = start // SIDE
            slot = row * columns + col - 1
            live = alive(row, own_rows)
            u = finals[0][pl.ds(base, size), :]
            v = finals[1][pl.ds(base, size), :]
            out_ref[slot, 0] = u
            out_ref[slot, 1] = v
            product = velocity[slot, 0].astype(F32) * u + velocity[slot, 1].astype(F32) * v
            grad_ref[slot] = (-(friction[slot].astype(F32) * product) * live).astype(BF16)

        if lv < levels - 1:
            over(1, columns, (0, tall), SIDE, finish)
        for copy, there in pending:
            if there is None:
                copy.wait_send()
            else:

                @pl.when(there)
                def _(copy=copy):
                    copy.wait_send()

    for lv in (2, 3):

        @pl.when(level == lv)
        def _(lv=lv):
            program(lv, 1)

    pl.semaphore_wait(barrier, count)
    init_each(lambda copy: copy.start(), False)

    for lv in (2, 3):

        @pl.when(level == lv)
        def _(lv=lv):
            program(lv, 2)

    @pl.when(jnp.logical_not(has_east))
    def _():
        init_recv[0] = jnp.ones((SLOTS, 16, SIDE), F32)

    @pl.when(jnp.logical_not(has_west))
    def _():
        init_recv[1] = jnp.ones((SLOTS, 16, SIDE), F32)

    init_each(lambda copy: copy.wait_recv(), True, range(levels - 1))

    def unpack_halo(row, carry, sides=(0, 1)):
        for side in sides:
            col = cols + 1 if side == 0 else 0
            base = base_of(jnp.int32(0) + col, row)
            live = alive(row, east_rows if side == 0 else west_rows)
            tile_t = columns_of(init_recv[side, row])

            def place(first, width, other):
                valid = lane < width if side == 0 else lane >= SIDE - width
                return jnp.where(valid, lanes_from(tile_t, side, first, width), other)

            mu[pl.ds(base, SIDE), :] = place(0, 4, 0.0) * live
            fric[pl.ds(base, SIDE), :] = place(4, 3, 1.0)
            b_u[pl.ds(base, SIDE), :] = place(7, 3, 0.0) * live
            b_v[pl.ds(base, SIDE), :] = place(10, 3, 0.0) * live
        return carry

    @pl.when(level < levels - 1)
    def _():
        lax.fori_loop(0, prows, unpack_halo, 0)

    @pl.when(level < 2)
    def _():
        first = jnp.where(level == 0, prows, 0)
        last = jnp.where(level == 0, 2 * prows, (cols + 2) * prows)
        lax.fori_loop(first, last, coefficients, 0)

    for lv in range(levels):

        @pl.when(level == lv)
        def _(lv=lv):
            program(lv, 0)

    init_each(lambda copy: copy.wait_send(), False)


def write_out(adjoint, gradient, adjoint_hbm, gradient_hbm, sem):
    copies = [
        pltpu.make_async_copy(adjoint, adjoint_hbm, sem.at[0]),
        pltpu.make_async_copy(gradient, gradient_hbm, sem.at[1]),
    ]
    for copy in copies:
        copy.start()
    for copy in copies:
        copy.wait()


def per_device(levels, patches, forcing, velocity, viscosity, friction, patch_rows):
    tall = pltpu.VMEM((TALL, SIDE), F32)
    vmem = pl.BlockSpec(memory_space=pltpu.VMEM)
    coarse = {
        sender: pltpu.VMEM((2, 2**sender // 2, SLOTS // 2**sender * SIDE // 2, SIDE), F32)
        for sender in range(1, levels)
    }
    adjoint, gradient = pl.pallas_call(
        functools.partial(kernel, levels, patches),
        out_shape=(
            jax.ShapeDtypeStruct((SLOTS, 2, SIDE, SIDE), F32),
            jax.ShapeDtypeStruct((SLOTS, SIDE, SIDE), BF16),
        ),
        in_specs=[pl.BlockSpec(memory_space=pltpu.HBM)] * 5,
        out_specs=(vmem, vmem),
        scratch_shapes=[
            pltpu.SMEM((levels, patches), jnp.int32),
            pltpu.VMEM((SLOTS, 2, SIDE, SIDE), BF16),
            pltpu.VMEM((SLOTS, 2, SIDE, SIDE), BF16),
            pltpu.VMEM((SLOTS, SIDE, SIDE), F32),
            pltpu.VMEM((SLOTS, SIDE, SIDE), BF16),
        ]
        + [tall] * 20
        + [
            pltpu.VMEM((2, SLOTS, 16, SIDE), F32),
            pltpu.VMEM((2, SLOTS, 16, SIDE), F32),
        ]
        + [coarse[sender] for sender in range(1, levels)] * 3
        + [pltpu.VMEM((4, 2, 8, SIDE), F32)] * 4
        + [pltpu.VMEM((2, 2 * SIDE, SIDE), F32)] * 2
        + [pltpu.VMEM((2, 8, SIDE), F32)] * 2
        + [
            pltpu.SemaphoreType.DMA((5,)),
            pltpu.SemaphoreType.DMA((4,)),
            pltpu.SemaphoreType.DMA((2, 16)),
            pltpu.SemaphoreType.DMA((2, 8)),
            pltpu.SemaphoreType.DMA((2, 32)),
            pltpu.SemaphoreType.DMA((2, 8)),
            pltpu.SemaphoreType.DMA((4,)),
        ],
        compiler_params=pltpu.CompilerParams(
            collective_id=0, has_side_effects=True, vmem_limit_bytes=44 << 20
        ),
    )(
        *(
            pltpu.with_memory_space_constraint(x, pltpu.HBM)
            for x in (patch_rows, forcing[0], velocity[0], viscosity[0], friction[0])
        )
    )
    adjoint, gradient = pl.pallas_call(
        write_out,
        out_shape=(
            jax.ShapeDtypeStruct(adjoint.shape, adjoint.dtype),
            jax.ShapeDtypeStruct(gradient.shape, gradient.dtype),
        ),
        in_specs=[vmem, vmem],
        out_specs=(pl.BlockSpec(memory_space=pltpu.HBM),) * 2,
        scratch_shapes=[pltpu.SemaphoreType.DMA((2,))],
        compiler_params=pltpu.CompilerParams(vmem_limit_bytes=4 << 20),
    )(adjoint, gradient)
    return adjoint[None], gradient[None]


def solution(mesh):
    in_specs = (
        P("level", "patch", None, None, None),
        P("level", "patch", None, None, None),
        P("level", "patch", None, None),
        P("level", "patch", None, None),
        P(),
    )
    out_specs = (P("level", "patch", None, None, None), P("level", "patch", None, None))
    return jax.shard_map(
        functools.partial(per_device, mesh.shape["level"], mesh.shape["patch"]),
        mesh=mesh,
        in_specs=in_specs,
        out_specs=out_specs,
        check_vma=False,
    )
```
